8 devices in a mesh: dp: 1 (over z), tp: 8 (over y, x, core).
Axes of the slice: x: 2, y: 2, z: 1, core: 2. Of those that a mesh axis runs over, the one named last changes fastest.
Arguments:
- x_in: bfloat16 [1, 128, 4096], P('dp', 'tp')
- start_pos: int32 [1], P('dp')
- k_cache: bfloat16 [1, 4096, 8, 128], P('dp', None, 'tp')
- v_cache: bfloat16 [1, 4096, 8, 128], P('dp', None, 'tp')
- attn_gain: bfloat16 [4096], replicated
- w_query: bfloat16 [4096, 32, 128], P(None, 'tp')
- w_key: bfloat16 [4096, 8, 128], P(None, 'tp')
- w_value: bfloat16 [4096, 8, 128], P(None, 'tp')
- w_out: bfloat16 [32, 128, 4096], P('tp')
- mlp_gain: bfloat16 [4096], replicated
- w_gate: bfloat16 [4096, 14336], P(None, 'tp')
- w_up: bfloat16 [4096, 14336], P(None, 'tp')
- w_down: bfloat16 [14336, 4096], P('tp')
Outputs:
- output 1: bfloat16 [1, 128, 4096], P('dp', 'tp')
- output 2: bfloat16 [1, 4096, 8, 128], P('dp', None, 'tp')
- output 3: bfloat16 [1, 4096, 8, 128], P('dp', None, 'tp')
All inputs are finite; a program needn't handle non-finite values.
Results may differ from the reference program's by a relative error of at most 0.0140087.
Values are sent between devices in bfloat16 or wider.
A program may use at most 1 GiB of HBM per device.

```python
import jax
import jax.numpy as jnp
from jax import lax

MODEL_DIM = 4096
Q_HEADS = 32
KV_HEADS = 8
HEAD_DIM = 128
FFN_DIM = 14336
WINDOW = 4096
BATCH_ROWS = 1
CHUNK_LEN = 128
ROPE_BASE = 10000.0
NORM_EPS = 1e-5
GROUP_SIZE = Q_HEADS // KV_HEADS
QUERY_BLOCK = min(CHUNK_LEN, 128)


def setup_inputs(seed: int = 0, part: int = 0) -> dict:
    part_keys = jax.random.split(jax.random.fold_in(jax.random.key(seed), part), 6)
    shared_keys = jax.random.split(jax.random.key(seed + 1), 9)
    cache_shape = (BATCH_ROWS, WINDOW, KV_HEADS, HEAD_DIM)
    x_in = jax.random.normal(part_keys[0], (BATCH_ROWS, CHUNK_LEN, MODEL_DIM), jnp.float32)
    row_starts = jax.random.randint(part_keys[1], (BATCH_ROWS,), 0, 3 * WINDOW)
    first_start = jax.random.randint(part_keys[2], (), WINDOW, 3 * WINDOW)
    start_pos = jnp.where(jnp.arange(BATCH_ROWS) == 0, first_start, row_starts)
    k_cache = 1.5 * jax.random.normal(part_keys[3], cache_shape, jnp.float32)
    v_mean = jax.random.normal(part_keys[4], (BATCH_ROWS, 1, KV_HEADS, HEAD_DIM), jnp.float32)
    v_cache = v_mean + jax.random.normal(part_keys[5], cache_shape, jnp.float32)
    attn_gain = 1.0 + 0.25 * jax.random.normal(shared_keys[0], (MODEL_DIM,), jnp.float32)
    w_query = (1.5 * MODEL_DIM ** -0.5) * jax.random.normal(shared_keys[1], (MODEL_DIM, Q_HEADS, HEAD_DIM), jnp.float32)
    w_key = (1.5 * MODEL_DIM ** -0.5) * jax.random.normal(shared_keys[2], (MODEL_DIM, KV_HEADS, HEAD_DIM), jnp.float32)
    w_value = MODEL_DIM ** -0.5 * jax.random.normal(shared_keys[3], (MODEL_DIM, KV_HEADS, HEAD_DIM), jnp.float32)
    w_out = (Q_HEADS * HEAD_DIM) ** -0.5 * jax.random.normal(shared_keys[4], (Q_HEADS, HEAD_DIM, MODEL_DIM), jnp.float32)
    mlp_gain = 1.0 + 0.25 * jax.random.normal(shared_keys[5], (MODEL_DIM,), jnp.float32)
    w_gate = MODEL_DIM ** -0.5 * jax.random.normal(shared_keys[6], (MODEL_DIM, FFN_DIM), jnp.float32)
    w_up = MODEL_DIM ** -0.5 * jax.random.normal(shared_keys[7], (MODEL_DIM, FFN_DIM), jnp.float32)
    w_down = FFN_DIM ** -0.5 * jax.random.normal(shared_keys[8], (FFN_DIM, MODEL_DIM), jnp.float32)
    return {
        'x_in': x_in.astype(jnp.bfloat16),
        'start_pos': start_pos.astype(jnp.int32),
        'k_cache': k_cache.astype(jnp.bfloat16),
        'v_cache': v_cache.astype(jnp.bfloat16),
        'attn_gain': attn_gain.astype(jnp.bfloat16),
        'w_query': w_query.astype(jnp.bfloat16),
        'w_key': w_key.astype(jnp.bfloat16),
        'w_value': w_value.astype(jnp.bfloat16),
        'w_out': w_out.astype(jnp.bfloat16),
        'mlp_gain': mlp_gain.astype(jnp.bfloat16),
        'w_gate': w_gate.astype(jnp.bfloat16),
        'w_up': w_up.astype(jnp.bfloat16),
        'w_down': w_down.astype(jnp.bfloat16),
    }


def rms_norm(rows, gain):
    rows32 = rows.astype(jnp.float32)
    inv_rms = lax.rsqrt(jnp.mean(rows32 * rows32, axis=-1, keepdims=True) + NORM_EPS)
    return (rows32 * inv_rms * gain.astype(jnp.float32)).astype(jnp.bfloat16)


def rotate(heads_in, positions):
    inv_freq = jnp.power(ROPE_BASE, -jnp.arange(0, HEAD_DIM, 2).astype(jnp.float32) / HEAD_DIM)
    angles = positions.astype(jnp.float32)[:, None] * inv_freq[None, :]
    cos_t = jnp.cos(angles)[:, None, :]
    sin_t = jnp.sin(angles)[:, None, :]
    pairs = heads_in.reshape(heads_in.shape[0], heads_in.shape[1], HEAD_DIM // 2, 2)
    even = pairs[..., 0]
    odd = pairs[..., 1]
    turned = jnp.stack([even * cos_t - odd * sin_t, even * sin_t + odd * cos_t], axis=-1)
    return turned.reshape(heads_in.shape)


def layer_row(x_row, start, k_old, v_old, attn_gain, w_query, w_key, w_value, w_out, mlp_gain, w_gate, w_up, w_down):
    positions = start + jnp.arange(CHUNK_LEN)
    normed = rms_norm(x_row, attn_gain)
    q_lin = jnp.dot(normed, w_query.reshape(MODEL_DIM, Q_HEADS * HEAD_DIM), preferred_element_type=jnp.float32)
    k_lin = jnp.dot(normed, w_key.reshape(MODEL_DIM, KV_HEADS * HEAD_DIM), preferred_element_type=jnp.float32)
    v_lin = jnp.dot(normed, w_value.reshape(MODEL_DIM, KV_HEADS * HEAD_DIM), preferred_element_type=jnp.float32)
    queries = rotate(q_lin.reshape(CHUNK_LEN, Q_HEADS, HEAD_DIM), positions).astype(jnp.bfloat16)
    k_chunk = rotate(k_lin.reshape(CHUNK_LEN, KV_HEADS, HEAD_DIM), positions).astype(jnp.bfloat16)
    v_chunk = v_lin.astype(jnp.bfloat16).reshape(CHUNK_LEN, KV_HEADS, HEAD_DIM)
    offsets = jnp.mod(jnp.arange(WINDOW) - start, WINDOW)
    cache_valid = (start - WINDOW + offsets) >= 0
    keys = jnp.concatenate([k_old, k_chunk], axis=0).astype(jnp.float32)
    values = jnp.concatenate([v_old, v_chunk], axis=0).astype(jnp.float32)
    n_blocks = CHUNK_LEN // QUERY_BLOCK
    q_tiles = queries.reshape(n_blocks, QUERY_BLOCK, KV_HEADS, GROUP_SIZE, HEAD_DIM)

    def attend_block(tile_pair):
        q_tile, block = tile_pair
        q_ids = block * QUERY_BLOCK + jnp.arange(QUERY_BLOCK)
        cache_mask = cache_valid[None, :] & (offsets[None, :] > q_ids[:, None])
        chunk_mask = jnp.arange(CHUNK_LEN)[None, :] <= q_ids[:, None]
        mask = jnp.concatenate([cache_mask, chunk_mask], axis=1)
        scores = jnp.einsum('qkge,ske->kgqs', q_tile.astype(jnp.float32), keys) * (HEAD_DIM ** -0.5)
        scores = jnp.where(mask[None, None], scores, -jnp.inf)
        attn_probs = jax.nn.softmax(scores, axis=-1).astype(jnp.bfloat16)
        mixed = jnp.einsum('kgqs,ske->qkge', attn_probs.astype(jnp.float32), values)
        return mixed.astype(jnp.bfloat16)

    mixed = lax.map(attend_block, (q_tiles, jnp.arange(n_blocks)))
    attn_out = jnp.dot(mixed.reshape(CHUNK_LEN, Q_HEADS * HEAD_DIM), w_out.reshape(Q_HEADS * HEAD_DIM, MODEL_DIM), preferred_element_type=jnp.float32)
    hidden = (x_row.astype(jnp.float32) + attn_out).astype(jnp.bfloat16)
    mlp_rows = rms_norm(hidden, mlp_gain)
    gate = jnp.dot(mlp_rows, w_gate, preferred_element_type=jnp.float32)
    up_proj = jnp.dot(mlp_rows, w_up, preferred_element_type=jnp.float32)
    activated = (jax.nn.silu(gate) * up_proj).astype(jnp.bfloat16)
    mlp_out = jnp.dot(activated, w_down, preferred_element_type=jnp.float32)
    x_out = (hidden.astype(jnp.float32) + mlp_out).astype(jnp.bfloat16)
    slots = jnp.mod(start + jnp.arange(CHUNK_LEN), WINDOW)
    k_new = k_old.at[slots].set(k_chunk)
    v_new = v_old.at[slots].set(v_chunk)
    return x_out, k_new, v_new


def reference(x_in, start_pos, k_cache, v_cache, attn_gain, w_query, w_key, w_value, w_out, mlp_gain, w_gate, w_up, w_down):
    def one_row(row_inputs):
        x_row, start, k_old, v_old = row_inputs
        return layer_row(x_row, start, k_old, v_old, attn_gain, w_query, w_key, w_value, w_out, mlp_gain, w_gate, w_up, w_down)

    x_out, k_new, v_new = lax.map(one_row, (x_in, start_pos, k_cache, v_cache))
    return x_out, k_new, v_new
```

```python
import functools

import jax
import jax.numpy as jnp
from jax import lax
from jax.experimental import pallas as pl
from jax.experimental.pallas import tpu as pltpu
from jax.sharding import PartitionSpec as P

ROPE_BASE = 10000.0
NORM_EPS = 1e-5
BF16 = jnp.bfloat16
F32 = jnp.float32
D = 4096
T = 128
FF = 1792
W = 4096
NP = 4
CW = D // NP
KB = 512
NKB = W // KB


def token_of_row(row):
    core = row // 64
    chip = (row // 16) % 4
    return 32 * chip + 16 * core + row % 16


def layer_kernel(start_ref, x_hbm, cos_hbm, sin_hbm, kc_hbm, vc_hbm, g1_hbm, wq_hbm, wk_hbm, wv_hbm, wo_hbm, g2_hbm, wg_hbm, wu_hbm, wd_hbm,
                 xo_ref, kch_ref, vch_ref,
                 xv, g1, g2, wg, wu, xg1, xg2, pbuf, ra, sb, rb, hb,
                 lsem, wsem, dsem, send_sem, recv_sem, fsend_sem, frecv_sem, asend_sem, arecv_sem, bsend_sem, brecv_sem):
    me = lax.axis_index("tp")
    core = me % 2
    chip = me // 2
    other = 1 - core
    partner = 2 * chip + other
    flip1 = chip + 1 - 2 * (chip % 2)
    flip2 = chip + 2 - 4 * (chip // 2)
    flip3 = 3 - chip
    chips = (chip, flip1, flip2, flip3)
    my_rows = pl.ds(pl.multiple_of(64 * core + 16 * chip, 16), 16)

    def rows_of(c, q):
        return pl.ds(pl.multiple_of(64 * c + 16 * q, 16), 16)

    def remote(src, dst, ssem, rsem, dev):
        return pltpu.make_async_remote_copy(src_ref=src, dst_ref=dst, send_sem=ssem, recv_sem=rsem, device_id={"tp": dev}, device_id_type=pl.DeviceIdType.MESH)

    def local(src, dst, sem):
        return pltpu.make_async_copy(src, dst, sem)

    def ag_direct(ph, xg, r, p):
        cols = pl.ds(p * CW, CW)
        return remote(xg.at[my_rows, cols], xg.at[my_rows, cols], send_sem.at[ph, r, p], recv_sem.at[ph, r, p], 2 * chips[r] + core)

    def ag_direct_in(ph, xg, r, p):
        ref = xg.at[rows_of(core, chips[r]), pl.ds(p * CW, CW)]
        return remote(ref, ref, send_sem.at[ph, r, p], recv_sem.at[ph, r, p], 2 * chips[r] + core)

    def ag_forward(ph, xg, r, p):
        ref = xg.at[rows_of(core, chips[r]), pl.ds(p * CW, CW)]
        return remote(ref, ref, fsend_sem.at[ph, r, p], frecv_sem.at[ph, r, p], partner)

    def ag_forward_in(ph, xg, r, p):
        ref = xg.at[rows_of(other, chips[r]), pl.ds(p * CW, CW)]
        return remote(ref, ref, fsend_sem.at[ph, r, p], frecv_sem.at[ph, r, p], partner)

    def ag_start(ph, xg):
        for p in range(NP):
            for r in (3, 1, 2):
                ag_direct(ph, xg, r, p).start()
            ag_forward(ph, xg, 0, p).start()

    def ag_relay(ph, xg, p):
        for r in (1, 2, 3):
            ag_direct_in(ph, xg, r, p).wait_recv()
            ag_forward(ph, xg, r, p).start()

    def ag_arrive(ph, xg, p):
        for r in (0, 1, 2, 3):
            ag_forward_in(ph, xg, r, p).wait_recv()

    def ag_finish(ph, xg):
        for p in range(NP):
            for r in (1, 2, 3):
                ag_direct(ph, xg, r, p).wait_send()
            for r in (0, 1, 2, 3):
                ag_forward(ph, xg, r, p).wait_send()

    def rs_a(ph, n):
        return remote(pbuf.at[ph, n, pl.ds(pl.multiple_of(64 * other, 64), 64), :], ra.at[ph, n], asend_sem.at[ph, n], arecv_sem.at[ph, n], partner)

    def rs_b(ph, n, r):
        return remote(sb.at[ph, n, pl.ds(pl.multiple_of(16 * chips[r], 16), 16), :], rb.at[ph, r - 1, n], bsend_sem.at[ph, r, n], brecv_sem.at[ph, r, n], 2 * chips[r] + core)

    def rs_put(ph, n, part):
        pbuf[ph, n] = part.astype(BF16)
        rs_a(ph, n).start()

    def rs_pair(ph, n):
        rs_a(ph, n).wait_recv()
        own = pbuf[ph, n, pl.ds(pl.multiple_of(64 * core, 64), 64), :].astype(F32)
        sb[ph, n] = (own + ra[ph, n].astype(F32)).astype(BF16)
        for r in (3, 1, 2):
            rs_b(ph, n, r).start()

    def rs_sum(ph, n):
        total = sb[ph, n, pl.ds(pl.multiple_of(16 * chip, 16), 16), :].astype(F32)
        for r in (1, 2, 3):
            rs_b(ph, n, r).wait_recv()
            total = total + rb[ph, r - 1, n].astype(F32)
        return total

    def rs_finish(ph):
        for n in range(NP):
            rs_a(ph, n).wait_send()
            for r in (1, 2, 3):
                rs_b(ph, n, r).wait_send()

    def normed(rows, gain):
        ms = jnp.zeros((16, 128), F32)
        for j in range(32):
            v = rows[:, 128 * j:128 * j + 128].astype(F32)
            ms = ms + v * v
        inv = lax.rsqrt(jnp.sum(ms, axis=-1, keepdims=True) * (1.0 / D) + NORM_EPS)
        return inv

    def store_normed(src, gain, dst):
        inv = normed(src, gain)
        for j in range(32):
            cols = slice(128 * j, 128 * j + 128)
            val = src[:, cols].astype(F32) * inv * gain[j:j + 1, :].astype(F32)
            dst[my_rows, cols] = val.astype(BF16)

    gate_loads = []
    for p in range(NP):
        gate_loads.append(local(wg_hbm.at[pl.ds(p * CW, CW), :], wg.at[pl.ds(p * CW, CW), :], wsem.at[0, p]))
        gate_loads.append(local(wu_hbm.at[pl.ds(p * CW, CW), :], wu.at[pl.ds(p * CW, CW), :], wsem.at[1, p]))

    def attention_phase(wq4, wqkv, kc, vc, vt, wo, cosv, sinv, qs, kch, vch, s_buf, o_buf):
        loads = {
            "x": local(x_hbm, xv, lsem.at[0]),
            "g1": local(g1_hbm, g1, lsem.at[1]),
            "wk": local(wk_hbm, wqkv.at[:, pl.ds(512, 128)], lsem.at[2]),
            "wv": local(wv_hbm, wqkv.at[:, pl.ds(640, 128)], lsem.at[3]),
            "vc": local(vc_hbm, vc, lsem.at[4]),
            "kc": local(kc_hbm, kc, lsem.at[5]),
            "cos": local(cos_hbm, cosv, lsem.at[6]),
            "sin": local(sin_hbm, sinv, lsem.at[7]),
            "wo": local(wo_hbm, wo, lsem.at[8]),
            "g2": local(g2_hbm, g2, lsem.at[9]),
        }
        loads["x"].start()
        loads["g1"].start()
        wq_loads = [local(wq_hbm.at[pl.ds(p * 4 * CW, 4 * CW), :], wq4.at[pl.ds(p * 4 * CW, 4 * CW), :], dsem.at[p]) for p in range(NP)]
        for ld in wq_loads:
            ld.start()
        for name in ("vc", "wk", "wv", "cos", "sin", "kc", "wo", "g2"):
            loads[name].start()

        barrier = pltpu.get_barrier_semaphore()
        for dev in (partner, 2 * flip1 + core, 2 * flip2 + core, 2 * flip3 + core):
            pl.semaphore_signal(barrier, inc=1, device_id={"tp": dev}, device_id_type=pl.DeviceIdType.MESH)

        loads["x"].wait()
        loads["g1"].wait()
        store_normed(xv, g1, xg1)
        pl.semaphore_wait(barrier, 4)
        ag_start(0, xg1)

        ri = lax.broadcasted_iota(jnp.int32, (256, 256), 0)
        ci = lax.broadcasted_iota(jnp.int32, (256, 256), 1)
        perm = (ci == 4 * (ri % 64) + ri // 64).astype(F32).astype(BF16)

        def split_heads(p):
            wq_loads[p].wait()

            def body(i, carry):
                base = p * (CW // 64) + i
                rows4 = wq4[pl.ds(pl.multiple_of(base * 256, 256), 256), :]
                out = jnp.dot(perm, rows4, preferred_element_type=F32).astype(BF16)
                for h in range(4):
                    wqkv[pl.ds(pl.multiple_of(base * 64, 64), 64), h * 128:h * 128 + 128] = out[64 * h:64 * h + 64, :]
                return carry

            lax.fori_loop(0, CW // 64, body, 0, unroll=4)

        split_heads(0)
        loads["vc"].wait()

        def flip_values(i, carry):
            ks = pl.ds(pl.multiple_of(i * KB, KB), KB)
            vt[:, ks] = vc[ks, :].astype(F32).T.astype(BF16)
            return carry

        lax.fori_loop(0, NKB, flip_values, 0)
        loads["wk"].wait()
        loads["wv"].wait()
        ag_relay(0, xg1, 0)
        acc = jnp.zeros((T, 768), F32)
        for p in range(NP):
            if p + 1 < NP:
                split_heads(p + 1)
            ag_arrive(0, xg1, p)
            cols = slice(p * CW, p * CW + CW)
            acc = acc + jnp.dot(xg1[:, cols], wqkv[cols, :], preferred_element_type=F32)
            if p + 1 < NP:
                ag_relay(0, xg1, p + 1)
        for ld in gate_loads:
            ld.start()
        loads["cos"].wait()
        loads["sin"].wait()

        lane = lax.broadcasted_iota(jnp.int32, (T, 128), 1)
        even = lane % 2 == 0
        cos_t = cosv[...]
        sin_t = sinv[...]

        def rotate(v):
            swapped = jnp.where(even, pltpu.roll(v, 127, 1), pltpu.roll(v, 1, 1))
            return v * cos_t + swapped * sin_t

        for h in range(4):
            qs[h * 128:h * 128 + 128, :] = rotate(acc[:, h * 128:h * 128 + 128]).astype(BF16)
        kch[...] = rotate(acc[:, 512:640]).astype(BF16)
        v_f32 = acc[:, 640:768]
        vch[...] = v_f32.astype(BF16)
        kch_ref[...] = kch[...]
        vch_ref[...] = vch[...]
        vt[:, W:W + T] = vch[...].astype(F32).T.astype(BF16)
        loads["kc"].wait()

        start = start_ref[0]
        tok_lane = token_of_row(lax.broadcasted_iota(jnp.int32, (1, 128), 1))
        factor = (128.0 ** -0.5) * 1.4426950408889634

        def half(hp, carry0):
            q2 = qs[pl.ds(pl.multiple_of(hp * 256, 256), 256), :]

            def scores(i, top):
                ks = pl.ds(pl.multiple_of(i * KB, KB), KB)
                st = lax.dot_general(kc[ks, :], q2, (((1,), (1,)), ((), ())), preferred_element_type=F32)
                slot = i * KB + lax.broadcasted_iota(jnp.int32, (KB, 128), 0)
                off = jnp.bitwise_and(slot - start, W - 1)
                thr = jnp.where(off >= W - start, off, -1)
                keep = thr > tok_lane
                for g in range(2):
                    part = jnp.where(keep, st[:, g * 128:g * 128 + 128], -jnp.inf)
                    s_buf[ks, g * 128:g * 128 + 128] = part
                    new = jnp.max(part.reshape(KB // 8, 8, 128), axis=0)
                    top = top[:g] + (jnp.maximum(top[g], new),) + top[g + 1:]
                return top

            st = lax.dot_general(kch[...], q2, (((1,), (1,)), ((), ())), preferred_element_type=F32)
            key_tok = token_of_row(lax.broadcasted_iota(jnp.int32, (T, 128), 0))
            keep = key_tok <= tok_lane
            top = ()
            for g in range(2):
                part = jnp.where(keep, st[:, g * 128:g * 128 + 128], -jnp.inf)
                s_buf[W:W + T, g * 128:g * 128 + 128] = part
                top = top + (jnp.max(part.reshape(T // 8, 8, 128), axis=0),)
            top = lax.fori_loop(0, NKB, scores, top)
            tops = tuple(jnp.max(t, axis=0, keepdims=True) for t in top)

            def expo(rows, n, mass):
                for g in range(2):
                    e = jnp.exp2((s_buf[rows, g * 128:g * 128 + 128] - tops[g]) * factor)
                    s_buf[rows, g * 128:g * 128 + 128] = e
                    mass = mass[:g] + (mass[g] + jnp.sum(e.reshape(n // 8, 8, 128), axis=0),) + mass[g + 1:]
                return mass

            mass = expo(slice(W, W + T), T, (jnp.zeros((8, 128), F32),) * 2)
            mass = lax.fori_loop(0, NKB, lambda i, m: expo(pl.ds(pl.multiple_of(i * KB, KB), KB), KB, m), mass)
            inv = jnp.concatenate([1.0 / jnp.sum(m, axis=0, keepdims=True) for m in mass], axis=1)

            def weigh(i, out):
                ks = pl.ds(pl.multiple_of(i * KB, KB), KB)
                probs = (s_buf[ks, :] * inv).astype(BF16)
                return out + jnp.dot(vt[:, ks], probs, preferred_element_type=F32)

            probs = (s_buf[W:W + T, :] * inv).astype(BF16)
            out = jnp.dot(vt[:, W:W + T], probs, preferred_element_type=F32)
            out = lax.fori_loop(0, NKB, weigh, out)
            for g in range(2):
                o_buf[hp, :, g * 128:g * 128 + 128] = out[:, g * 128:g * 128 + 128].T.astype(BF16)
            return carry0

        lax.fori_loop(0, 2, half, 0)
        loads["wo"].wait()
        for n in range(NP):
            cols = slice(n * CW, n * CW + CW)
            part = jnp.dot(o_buf[0], wo[0:256, cols], preferred_element_type=F32)
            part = part + jnp.dot(o_buf[1], wo[256:512, cols], preferred_element_type=F32)
            rs_put(0, n, part)
            if n > 0:
                rs_pair(0, n - 1)
        rs_pair(0, NP - 1)
        loads["g2"].wait()

    pl.run_scoped(
        attention_phase,
        pltpu.VMEM((4 * D, 128), BF16),
        pltpu.VMEM((D, 768), BF16),
        pltpu.VMEM((W, 128), BF16),
        pltpu.VMEM((W, 128), BF16),
        pltpu.VMEM((128, W + T), BF16),
        pltpu.VMEM((512, D), BF16),
        pltpu.VMEM((T, 128), F32),
        pltpu.VMEM((T, 128), F32),
        pltpu.VMEM((512, 128), BF16),
        pltpu.VMEM((T, 128), BF16),
        pltpu.VMEM((T, 128), BF16),
        pltpu.VMEM((W + T, 256), F32),
        pltpu.VMEM((2, T, 256), BF16),
    )

    def mlp_phase(wd, acc_g, acc_u, u_buf):
        down_loads = [local(wd_hbm.at[:, pl.ds(n * CW, CW)], wd.at[:, pl.ds(n * CW, CW)], dsem.at[n]) for n in range(NP)]
        for ld in down_loads:
            ld.start()
        for n in range(NP):
            cols = slice(n * CW, n * CW + CW)
            hb[:, cols] = (xv[:, cols].astype(F32) + rs_sum(0, n)).astype(BF16)
        store_normed(hb, g2, xg2)
        ag_start(1, xg2)
        ag_finish(0, xg1)
        rs_finish(0)
        ag_relay(1, xg2, 0)
        for p in range(NP):
            gate_loads[2 * p].wait()
            gate_loads[2 * p + 1].wait()
            ag_arrive(1, xg2, p)
            rows = slice(p * CW, p * CW + CW)
            m = xg2[:, rows]
            gate = jnp.dot(m, wg[rows, :], preferred_element_type=F32)
            up = jnp.dot(m, wu[rows, :], preferred_element_type=F32)
            if p == 0:
                acc_g[...] = gate
                acc_u[...] = up
            elif p + 1 < NP:
                acc_g[...] += gate
                acc_u[...] += up
            else:
                gate = acc_g[...] + gate
                u_buf[...] = (gate / (1.0 + jnp.exp(-gate)) * (acc_u[...] + up)).astype(BF16)
            if p + 1 < NP:
                ag_relay(1, xg2, p + 1)
        for n in range(NP):
            cols = slice(n * CW, n * CW + CW)
            down_loads[n].wait()
            rs_put(1, n, jnp.dot(u_buf[...], wd[:, cols], preferred_element_type=F32))
            if n > 0:
                rs_pair(1, n - 1)
        rs_pair(1, NP - 1)
        ag_finish(1, xg2)
        for n in range(NP):
            cols = slice(n * CW, n * CW + CW)
            xo_ref[:, cols] = (hb[:, cols].astype(F32) + rs_sum(1, n)).astype(BF16)
        rs_finish(1)

    pl.run_scoped(
        mlp_phase,
        pltpu.VMEM((FF, D), BF16),
        pltpu.VMEM((T, FF), F32),
        pltpu.VMEM((T, FF), F32),
        pltpu.VMEM((T, FF), BF16),
    )


def cache_kernel(start_ref, kch_ref, vch_ref, kc_ref, vc_ref, ko_ref, vo_ref):
    block = pl.program_id(0)
    start = start_ref[0]
    slot = block * KB + lax.broadcasted_iota(jnp.int32, (KB, 128), 0)
    off = jnp.bitwise_and(slot - start, W - 1)
    tok = token_of_row(lax.broadcasted_iota(jnp.int32, (1, 128), 1))
    pick = (off == tok).astype(F32).astype(BF16)
    fresh = off < T
    for chunk, old, new in ((kch_ref, kc_ref, ko_ref), (vch_ref, vc_ref, vo_ref)):
        placed = jnp.dot(pick, chunk[...], preferred_element_type=F32)
        new[...] = jnp.where(fresh, placed, old[...].astype(F32)).astype(BF16)


def solution(mesh):
    row_spec = P('dp', 'tp', None)
    cache_spec = P('dp', None, 'tp', None)
    head_cols = P(None, 'tp', None)
    in_specs = (row_spec, P('dp'), cache_spec, cache_spec, P(), head_cols, head_cols, head_cols, P('tp', None, None), P(), P(None, 'tp'), P(None, 'tp'), P('tp', None))
    out_specs = (row_spec, cache_spec, cache_spec)

    def local_layer(x_in, start_pos, k_cache, v_cache, attn_gain, w_query, w_key, w_value, w_out, mlp_gain, w_gate, w_up, w_down):
        inv_freq = jnp.power(ROPE_BASE, -jnp.arange(0, 128, 2).astype(F32) / 128)
        tokens = token_of_row(jnp.arange(T))
        angles = (start_pos[0] + tokens).astype(F32)[:, None] * jnp.repeat(inv_freq, 2)[None, :]
        cos_t = jnp.cos(angles)
        sin_t = jnp.sin(angles) * jnp.where(jnp.arange(128) % 2 == 0, -1.0, 1.0)[None, :]
        any_spec = pl.BlockSpec(memory_space=pl.ANY)
        vmem_spec = pl.BlockSpec(memory_space=pltpu.VMEM)
        dma = pltpu.SemaphoreType.DMA
        kc2 = k_cache.reshape(W, 128)
        vc2 = v_cache.reshape(W, 128)
        x_out, k_chunk, v_chunk = pl.pallas_call(
            layer_kernel,
            out_shape=(
                jax.ShapeDtypeStruct((16, D), BF16),
                jax.ShapeDtypeStruct((T, 128), BF16),
                jax.ShapeDtypeStruct((T, 128), BF16),
            ),
            in_specs=[pl.BlockSpec(memory_space=pltpu.SMEM)] + [any_spec] * 14,
            out_specs=(vmem_spec, vmem_spec, vmem_spec),
            scratch_shapes=[
                pltpu.VMEM((16, D), BF16),
                pltpu.VMEM((32, 128), BF16),
                pltpu.VMEM((32, 128), BF16),
                pltpu.VMEM((D, FF), BF16),
                pltpu.VMEM((D, FF), BF16),
                pltpu.VMEM((T, D), BF16),
                pltpu.VMEM((T, D), BF16),
                pltpu.VMEM((2, NP, T, CW), BF16),
                pltpu.VMEM((2, NP, 64, CW), BF16),
                pltpu.VMEM((2, NP, 64, CW), BF16),
                pltpu.VMEM((2, 3, NP, 16, CW), BF16),
                pltpu.VMEM((16, D), BF16),
                dma((10,)),
                dma((2, NP)),
                dma((NP,)),
                dma((2, 4, NP)),
                dma((2, 4, NP)),
                dma((2, 4, NP)),
                dma((2, 4, NP)),
                dma((2, NP)),
                dma((2, NP)),
                dma((2, 4, NP)),
                dma((2, 4, NP)),
            ],
            compiler_params=pltpu.CompilerParams(collective_id=0, has_side_effects=True, vmem_limit_bytes=67043328),
            name="layer",
        )(
            start_pos, x_in.reshape(16, D), cos_t, sin_t, kc2, vc2, attn_gain.reshape(32, 128), w_query.reshape(4 * D, 128),
            w_key.reshape(D, 128), w_value.reshape(D, 128), w_out.reshape(512, D), mlp_gain.reshape(32, 128), w_gate, w_up, w_down,
        )
        chunk_spec = pl.BlockSpec((T, 128), lambda i: (0, 0))
        block_spec = pl.BlockSpec((KB, 128), lambda i: (i, 0))
        k_new, v_new = pl.pallas_call(
            cache_kernel,
            grid=(NKB,),
            out_shape=(jax.ShapeDtypeStruct((W, 128), BF16),) * 2,
            in_specs=[pl.BlockSpec(memory_space=pltpu.SMEM), chunk_spec, chunk_spec, block_spec, block_spec],
            out_specs=(block_spec, block_spec),
            name="caches",
        )(start_pos, k_chunk, v_chunk, kc2, vc2)
        return x_out.reshape(x_in.shape), k_new.reshape(k_cache.shape), v_new.reshape(v_cache.shape)

    return jax.shard_map(local_layer, mesh=mesh, in_specs=in_specs, out_specs=out_specs, check_vma=False)
```

```python
import functools

import jax
import numpy as np
import jax.numpy as jnp
from jax import lax
from jax.experimental import pallas as pl
from jax.experimental.pallas import tpu as pltpu
from jax.sharding import PartitionSpec as P

ROPE_BASE = 10000.0
NORM_EPS = 1e-5
BF16 = jnp.bfloat16
F32 = jnp.float32
D = 4096
T = 128
FF = 1792
W = 4096
NP = 8
VMEM_LIMIT = 64000000
CW = D // NP
KB = 512
NKB = W // KB


def token_of_row(row):
    core = row // 64
    chip = (row // 16) % 4
    return 32 * chip + 16 * core + row % 16


def layer_kernel(start_ref, x_hbm, freq_hbm, kc_hbm, vc_hbm, g1_hbm, wq_hbm, wk_hbm, wv_hbm, wo_hbm, g2_hbm, wg_hbm, wu_hbm, wd_hbm,
                 xo_ref, kn_ref, vn_ref,
                 xv, g1, g2, wg, wu, xg1, xg2, pbuf, ra, sb, rb, hb,
                 lsem, wsem, dsem, send_sem, recv_sem, fsend_sem, frecv_sem, asend_sem, arecv_sem, bsend_sem, brecv_sem):
    me = lax.axis_index("tp")
    core = me % 2
    chip = me // 2
    other = 1 - core
    partner = 2 * chip + other
    flip1 = chip + 1 - 2 * (chip % 2)
    flip2 = chip + 2 - 4 * (chip // 2)
    flip3 = 3 - chip
    chips = (chip, flip1, flip2, flip3)
    my_rows = pl.ds(pl.multiple_of(64 * core + 16 * chip, 16), 16)

    def rows_of(c, q):
        return pl.ds(pl.multiple_of(64 * c + 16 * q, 16), 16)

    def remote(src, dst, ssem, rsem, dev):
        return pltpu.make_async_remote_copy(src_ref=src, dst_ref=dst, send_sem=ssem, recv_sem=rsem, device_id={"tp": dev}, device_id_type=pl.DeviceIdType.MESH)

    def local(src, dst, sem):
        return pltpu.make_async_copy(src, dst, sem)

    def ag_direct(ph, xg, r, p):
        cols = pl.ds(p * CW, CW)
        return remote(xg.at[my_rows, cols], xg.at[my_rows, cols], send_sem.at[ph, r, p], recv_sem.at[ph, r, p], 2 * chips[r] + core)

    def ag_direct_in(ph, xg, r, p):
        ref = xg.at[rows_of(core, chips[r]), pl.ds(p * CW, CW)]
        return remote(ref, ref, send_sem.at[ph, r, p], recv_sem.at[ph, r, p], 2 * chips[r] + core)

    def ag_forward(ph, xg, r, p):
        ref = xg.at[rows_of(core, chips[r]), pl.ds(p * CW, CW)]
        return remote(ref, ref, fsend_sem.at[ph, r, p], frecv_sem.at[ph, r, p], partner)

    def ag_forward_in(ph, xg, r, p):
        ref = xg.at[rows_of(other, chips[r]), pl.ds(p * CW, CW)]
        return remote(ref, ref, fsend_sem.at[ph, r, p], frecv_sem.at[ph, r, p], partner)

    def ag_start(ph, xg):
        for p in range(NP):
            for r in (3, 1, 2):
                ag_direct(ph, xg, r, p).start()
            ag_forward(ph, xg, 0, p).start()

    def ag_relay(ph, xg, p):
        for r in (1, 2, 3):
            ag_direct_in(ph, xg, r, p).wait_recv()
            ag_forward(ph, xg, r, p).start()

    def ag_arrive(ph, xg, p):
        for r in (0, 1, 2, 3):
            ag_forward_in(ph, xg, r, p).wait_recv()

    def ag_finish(ph, xg):
        for p in range(NP):
            for r in (1, 2, 3):
                ag_direct(ph, xg, r, p).wait_send()
            for r in (0, 1, 2, 3):
                ag_forward(ph, xg, r, p).wait_send()

    def rs_a(ph, n):
        return remote(pbuf.at[ph, n, pl.ds(pl.multiple_of(64 * other, 64), 64), :], ra.at[ph, n], asend_sem.at[ph, n], arecv_sem.at[ph, n], partner)

    def rs_b(ph, n, r):
        return remote(sb.at[ph, n, pl.ds(pl.multiple_of(16 * chips[r], 16), 16), :], rb.at[ph, r - 1, n], bsend_sem.at[ph, r, n], brecv_sem.at[ph, r, n], 2 * chips[r] + core)

    def rs_put(ph, n, part):
        pbuf[ph, n] = part.astype(BF16)
        rs_a(ph, n).start()

    def rs_pair(ph, n):
        rs_a(ph, n).wait_recv()
        own = pbuf[ph, n, pl.ds(pl.multiple_of(64 * core, 64), 64), :].astype(F32)
        sb[ph, n] = (own + ra[ph, n].astype(F32)).astype(BF16)
        for r in (3, 1, 2):
            rs_b(ph, n, r).start()

    def rs_sum(ph, n):
        total = sb[ph, n, pl.ds(pl.multiple_of(16 * chip, 16), 16), :].astype(F32)
        for r in (1, 2, 3):
            rs_b(ph, n, r).wait_recv()
            total = total + rb[ph, r - 1, n].astype(F32)
        return total

    def rs_finish(ph):
        for n in range(NP):
            rs_a(ph, n).wait_send()
            for r in (1, 2, 3):
                rs_b(ph, n, r).wait_send()

    def normed(rows, gain):
        ms = jnp.zeros((16, 128), F32)
        for j in range(32):
            v = rows[:, 128 * j:128 * j + 128].astype(F32)
            ms = ms + v * v
        inv = lax.rsqrt(jnp.sum(ms, axis=-1, keepdims=True) * (1.0 / D) + NORM_EPS)
        return inv

    def store_normed(src, gain, dst):
        inv = normed(src, gain)
        for j in range(32):
            cols = slice(128 * j, 128 * j + 128)
            val = src[:, cols].astype(F32) * inv * gain[j:j + 1, :].astype(F32)
            dst[my_rows, cols] = val.astype(BF16)

    gate_loads = []
    for p in range(NP):
        gate_loads.append(local(wg_hbm.at[pl.ds(p * CW, CW), :], wg.at[pl.ds(p * CW, CW), :], wsem.at[0, p]))
        gate_loads.append(local(wu_hbm.at[pl.ds(p * CW, CW), :], wu.at[pl.ds(p * CW, CW), :], wsem.at[1, p]))

    def attention_phase(kc, vc, vt, wo, freqv, qs, kch, vch, bias, o_buf):
        loads = {
            "x": local(x_hbm, xv, lsem.at[0]),
            "g1": local(g1_hbm, g1, lsem.at[1]),
            "freq": local(freq_hbm, freqv, lsem.at[6]),
            "vc": local(vc_hbm, vc, lsem.at[4]),
            "kc": local(kc_hbm, kc, lsem.at[5]),
            "wo": local(wo_hbm, wo, lsem.at[8]),
            "g2": local(g2_hbm, g2, lsem.at[9]),
        }
        loads["x"].start()
        loads["g1"].start()
        barrier = pltpu.get_barrier_semaphore()
        for dev in (partner, 2 * flip1 + core, 2 * flip2 + core, 2 * flip3 + core):
            pl.semaphore_signal(barrier, inc=1, device_id={"tp": dev}, device_id_type=pl.DeviceIdType.MESH)
        start = start_ref[0]
        tok_lane = token_of_row(lax.broadcasted_iota(jnp.int32, (1, 128), 1))

        def projection_phase(wq4, wqkv):
            wk_load = local(wk_hbm, wqkv.at[:, pl.ds(512, 128)], lsem.at[2])
            wv_load = local(wv_hbm, wqkv.at[:, pl.ds(640, 128)], lsem.at[3])
            wq_loads = [local(wq_hbm.at[pl.ds(p * 4 * CW, 4 * CW), :], wq4.at[pl.ds(p * 4 * CW, 4 * CW), :], dsem.at[p]) for p in range(NP)]
            for ld in wq_loads:
                ld.start()
            loads["vc"].start()
            loads["freq"].start()
            wk_load.start()
            wv_load.start()
            for name in ("kc", "wo", "g2"):
                loads[name].start()

            loads["x"].wait()
            loads["g1"].wait()
            store_normed(xv, g1, xg1)
            pl.semaphore_wait(barrier, 4)
            ag_start(0, xg1)

            ri = lax.broadcasted_iota(jnp.int32, (256, 256), 0)
            ci = lax.broadcasted_iota(jnp.int32, (256, 256), 1)
            perm = (ci == 4 * (ri % 64) + ri // 64).astype(F32).astype(BF16)

            def split_heads(p):
                wq_loads[p].wait()

                def body(i, carry):
                    base = p * (CW // 64) + 2 * i
                    rows4 = jnp.concatenate([wq4[pl.ds(pl.multiple_of((base + k) * 256, 256), 256), :] for k in range(2)], axis=1)
                    out = jnp.dot(perm, rows4, preferred_element_type=F32).astype(BF16)
                    for k in range(2):
                        for h in range(4):
                            wqkv[pl.ds(pl.multiple_of((base + k) * 64, 64), 64), h * 128:h * 128 + 128] = out[64 * h:64 * h + 64, k * 128:k * 128 + 128]
                    return carry

                for i in range(CW // 128):
                    body(i, 0)

            split_heads(0)
            ag_relay(0, xg1, 0)
            loads["vc"].wait()

            def flip_values(i, carry):
                ks = pl.ds(pl.multiple_of(i * KB, KB), KB)
                vt[:, ks] = vc[ks, :].astype(F32).T.astype(BF16)
                slot = i * KB + lax.broadcasted_iota(jnp.int32, (KB, 128), 0)
                off = jnp.bitwise_and(slot - start, W - 1)
                keep = jnp.where(off >= W - start, off, -1) > tok_lane
                bias[ks, :] = jnp.where(keep, 0.0, -jnp.inf)
                return carry

            loads["freq"].wait()
            tok_row = token_of_row(lax.broadcasted_iota(jnp.int32, (T, 128), 0))
            angles = (start + tok_row).astype(F32) * freqv[0:1, :]
            cos_t = jnp.cos(angles)
            lane = lax.broadcasted_iota(jnp.int32, (T, 128), 1)
            even = lane % 2 == 0
            sin_t = jnp.sin(angles)
            sin_t = jnp.where(even, -sin_t, sin_t)
            wk_load.wait()
            wv_load.wait()
            acc = jnp.zeros((T, 768), F32)
            for p in range(NP):
                if p + 1 < NP:
                    split_heads(p + 1)
                flip_values(p, 0)
                ag_arrive(0, xg1, p)
                cols = slice(p * CW, p * CW + CW)
                acc = acc + jnp.dot(xg1[:, cols], wqkv[cols, :], preferred_element_type=F32)
                if p + 1 < NP:
                    ag_relay(0, xg1, p + 1)
            for ld in gate_loads:
                ld.start()

            def rotate(v):
                swapped = jnp.where(even, pltpu.roll(v, 127, 1), pltpu.roll(v, 1, 1))
                return v * cos_t + swapped * sin_t

            for h in range(4):
                qs[h * 128:h * 128 + 128, :] = rotate(acc[:, h * 128:h * 128 + 128]).astype(BF16)
            kch[...] = rotate(acc[:, 512:640]).astype(BF16)
            v_new = acc[:, 640:768].astype(BF16)
            vch[...] = v_new
            vt[:, W:W + T] = v_new.astype(F32).T.astype(BF16)

        pl.run_scoped(
            projection_phase,
            pltpu.VMEM((4 * D, 128), BF16),
            pltpu.VMEM((D, 768), BF16),
        )
        loads["kc"].wait()
        factor = (128.0 ** -0.5) * 1.4426950408889634

        def softmax_phase(s_buf):
            queries = qs[...]
            tops, masses = [], []
            for b in range(NKB + 1):
                n = KB if b < NKB else T
                ks = slice(b * KB, b * KB + n)
                keys = kc[ks, :] if b < NKB else kch[...]
                st = lax.dot_general(keys, queries, (((1,), (1,)), ((), ())), preferred_element_type=F32)
                if b < NKB:
                    shift = bias[ks, :]
                else:
                    shift = jnp.where(token_of_row(lax.broadcasted_iota(jnp.int32, (T, 128), 0)) <= tok_lane, 0.0, -jnp.inf)
                top, mass = [], []
                for g in range(4):
                    gs = slice(g * 128, g * 128 + 128)
                    part = st[:, gs] + shift
                    s_buf[ks, gs] = part
                    t = jnp.max(jnp.max(part.reshape(n // 8, 8, 128), axis=0), axis=0, keepdims=True)
                    t = jnp.maximum(t, jnp.finfo(F32).min)
                    e = jnp.exp2((s_buf[ks, gs] - t) * factor)
                    s_buf[ks, gs] = e
                    mass.append(jnp.sum(jnp.sum(e.reshape(n // 8, 8, 128), axis=0), axis=0, keepdims=True))
                    top.append(t)
                tops.append(jnp.concatenate(top, axis=1))
                masses.append(jnp.concatenate(mass, axis=1))
            best = functools.reduce(jnp.maximum, tops)
            scales = [jnp.exp2((t - best) * factor) for t in tops]
            total = sum(m * sc for m, sc in zip(masses, scales))
            inv = 1.0 / total
            out = None
            for b in range(NKB + 1):
                n = KB if b < NKB else T
                ks = slice(b * KB, b * KB + n)
                probs = (s_buf[ks, :] * (scales[b] * inv)).astype(BF16)
                part = jnp.dot(vt[:, ks], probs, preferred_element_type=F32)
                out = part if out is None else out + part
            for g in range(4):
                o_buf[:, g * 128:g * 128 + 128] = out[:, g * 128:g * 128 + 128].T.astype(BF16)

        pl.run_scoped(softmax_phase, pltpu.VMEM((W + T, 512), F32))
        loads["wo"].wait()
        for n in range(NP):
            cols = slice(n * CW, n * CW + CW)
            rs_put(0, n, jnp.dot(o_buf[...], wo[:, cols], preferred_element_type=F32))
            if n > 0:
                rs_pair(0, n - 1)
        rs_pair(0, NP - 1)
        loads["g2"].wait()

        chunk = jnp.concatenate([kch[...], vch[...]], axis=1)

        def merge(i, carry):
            ks = pl.ds(pl.multiple_of(i * KB, KB), KB)
            slot = i * KB + lax.broadcasted_iota(jnp.int32, (KB, 128), 0)
            off = jnp.bitwise_and(slot - start, W - 1)
            pick = (off == tok_lane).astype(F32).astype(BF16)
            placed = jnp.dot(pick, chunk, preferred_element_type=F32)
            fresh = off < T
            kn_ref[ks, :] = jnp.where(fresh, placed[:, 0:128], kc[ks, :].astype(F32)).astype(BF16)
            vn_ref[ks, :] = jnp.where(fresh, placed[:, 128:256], vc[ks, :].astype(F32)).astype(BF16)
            return carry

        lax.fori_loop(0, NKB, merge, 0)

    pl.run_scoped(
        attention_phase,
        pltpu.VMEM((W, 128), BF16),
        pltpu.VMEM((W, 128), BF16),
        pltpu.VMEM((128, W + T), BF16),
        pltpu.VMEM((512, D), BF16),
        pltpu.VMEM((8, 128), F32),
        pltpu.VMEM((512, 128), BF16),
        pltpu.VMEM((T, 128), BF16),
        pltpu.VMEM((T, 128), BF16),
        pltpu.VMEM((W, 128), F32),
        pltpu.VMEM((T, 512), BF16),
    )

    def mlp_phase(wd, acc_g, acc_u, u_buf):
        down_loads = [local(wd_hbm.at[:, pl.ds(n * CW, CW)], wd.at[:, pl.ds(n * CW, CW)], dsem.at[n]) for n in range(NP)]
        for ld in down_loads:
            ld.start()
        for n in range(NP):
            cols = slice(n * CW, n * CW + CW)
            hb[:, cols] = (xv[:, cols].astype(F32) + rs_sum(0, n)).astype(BF16)
        store_normed(hb, g2, xg2)
        ag_start(1, xg2)
        ag_finish(0, xg1)
        rs_finish(0)
        ag_relay(1, xg2, 0)
        for p in range(NP):
            gate_loads[2 * p].wait()
            gate_loads[2 * p + 1].wait()
            ag_arrive(1, xg2, p)
            rows = slice(p * CW, p * CW + CW)
            m = xg2[:, rows]
            gate = jnp.dot(m, wg[rows, :], preferred_element_type=F32)
            up = jnp.dot(m, wu[rows, :], preferred_element_type=F32)
            if p == 0:
                acc_g[...] = gate
                acc_u[...] = up
            elif p + 1 < NP:
                acc_g[...] += gate
                acc_u[...] += up
            else:
                gate = acc_g[...] + gate
                u_buf[...] = (gate / (1.0 + jnp.exp(-gate)) * (acc_u[...] + up)).astype(BF16)
            if p + 1 < NP:
                ag_relay(1, xg2, p + 1)
        for n in range(NP):
            cols = slice(n * CW, n * CW + CW)
            down_loads[n].wait()
            rs_put(1, n, jnp.dot(u_buf[...], wd[:, cols], preferred_element_type=F32))
            if n > 0:
                rs_pair(1, n - 1)
        rs_pair(1, NP - 1)
        ag_finish(1, xg2)
        for n in range(NP):
            cols = slice(n * CW, n * CW + CW)
            xo_ref[:, cols] = (hb[:, cols].astype(F32) + rs_sum(1, n)).astype(BF16)
        rs_finish(1)

    pl.run_scoped(
        mlp_phase,
        pltpu.VMEM((FF, D), BF16),
        pltpu.VMEM((T, FF), F32),
        pltpu.VMEM((T, FF), F32),
        pltpu.VMEM((T, FF), BF16),
    )


def solution(mesh):
    row_spec = P('dp', 'tp', None)
    cache_spec = P('dp', None, 'tp', None)
    head_cols = P(None, 'tp', None)
    in_specs = (row_spec, P('dp'), cache_spec, cache_spec, P(), head_cols, head_cols, head_cols, P('tp', None, None), P(), P(None, 'tp'), P(None, 'tp'), P('tp', None))
    out_specs = (row_spec, cache_spec, cache_spec)

    def local_layer(x_in, start_pos, k_cache, v_cache, attn_gain, w_query, w_key, w_value, w_out, mlp_gain, w_gate, w_up, w_down):
        freq = np.repeat(ROPE_BASE ** (-np.arange(0, 128, 2) / 128.0), 2).astype(np.float32)
        freq = jnp.asarray(np.tile(freq[None, :], (8, 1)))
        any_spec = pl.BlockSpec(memory_space=pl.ANY)
        vmem_spec = pl.BlockSpec(memory_space=pltpu.VMEM)
        dma = pltpu.SemaphoreType.DMA
        kc2 = k_cache.reshape(W, 128)
        vc2 = v_cache.reshape(W, 128)
        x_out, k_new, v_new = pl.pallas_call(
            layer_kernel,
            out_shape=(pltpu.VMEM((16, D), BF16), pltpu.VMEM((W, 128), BF16), pltpu.VMEM((W, 128), BF16)),
            in_specs=[pl.BlockSpec(memory_space=pltpu.SMEM)] + [any_spec] * 13,
            out_specs=(vmem_spec, vmem_spec, vmem_spec),
            scratch_shapes=[
                pltpu.VMEM((16, D), BF16),
                pltpu.VMEM((32, 128), BF16),
                pltpu.VMEM((32, 128), BF16),
                pltpu.VMEM((D, FF), BF16),
                pltpu.VMEM((D, FF), BF16),
                pltpu.VMEM((T, D), BF16),
                pltpu.VMEM((T, D), BF16),
                pltpu.VMEM((2, NP, T, CW), BF16),
                pltpu.VMEM((2, NP, 64, CW), BF16),
                pltpu.VMEM((2, NP, 64, CW), BF16),
                pltpu.VMEM((2, 3, NP, 16, CW), BF16),
                pltpu.VMEM((16, D), BF16),
                dma((10,)),
                dma((2, NP)),
                dma((NP,)),
                dma((2, 4, NP)),
                dma((2, 4, NP)),
                dma((2, 4, NP)),
                dma((2, 4, NP)),
                dma((2, NP)),
                dma((2, NP)),
                dma((2, 4, NP)),
                dma((2, 4, NP)),
            ],
            compiler_params=pltpu.CompilerParams(collective_id=0, has_side_effects=True, vmem_limit_bytes=VMEM_LIMIT),
            name="layer",
        )(
            start_pos, x_in.reshape(16, D), freq, kc2, vc2, attn_gain.reshape(32, 128), w_query.reshape(4 * D, 128),
            w_key.reshape(D, 128), w_value.reshape(D, 128), w_out.reshape(512, D), mlp_gain.reshape(32, 128), w_gate, w_up, w_down,
        )
        return x_out.reshape(x_in.shape), k_new.reshape(k_cache.shape), v_new.reshape(v_cache.shape)

    return jax.shard_map(local_layer, mesh=mesh, in_specs=in_specs, out_specs=out_specs, check_vma=False)
```

```python
import functools

import jax
import numpy as np
import jax.numpy as jnp
from jax import lax
from jax.experimental import pallas as pl
from jax.experimental.pallas import tpu as pltpu
from jax.sharding import PartitionSpec as P

ROPE_BASE = 10000.0
NORM_EPS = 1e-5
BF16 = jnp.bfloat16
F32 = jnp.float32
D = 4096
T = 128
FF = 1792
W = 4096
NP = 8
VMEM_LIMIT = 64000000
CW = D // NP
KB = 512
NKB = W // KB


def token_of_row(row):
    core = row // 64
    chip = (row // 16) % 4
    return 32 * chip + 16 * core + row % 16


def layer_kernel(start_hbm, x_hbm, freq_hbm, kc_hbm, vc_hbm, g1_hbm, wq_hbm, wk_hbm, wv_hbm, wo_hbm, g2_hbm, wg_hbm, wu_hbm, wd_hbm,
                 xo_ref, kn_ref, vn_ref,
                 start_ref, xv, g1, g2, wg, wu, xg1, xg2, pbuf, ra, sb, rb, hb,
                 lsem, wsem, dsem, send_sem, recv_sem, fsend_sem, frecv_sem, asend_sem, arecv_sem, bsend_sem, brecv_sem):
    me = lax.axis_index("tp")
    core = me % 2
    chip = me // 2
    other = 1 - core
    partner = 2 * chip + other
    flip1 = chip + 1 - 2 * (chip % 2)
    flip2 = chip + 2 - 4 * (chip // 2)
    flip3 = 3 - chip
    chips = (chip, flip1, flip2, flip3)
    my_rows = pl.ds(pl.multiple_of(64 * core + 16 * chip, 16), 16)

    def rows_of(c, q):
        return pl.ds(pl.multiple_of(64 * c + 16 * q, 16), 16)

    def remote(src, dst, ssem, rsem, dev):
        return pltpu.make_async_remote_copy(src_ref=src, dst_ref=dst, send_sem=ssem, recv_sem=rsem, device_id={"tp": dev}, device_id_type=pl.DeviceIdType.MESH)

    def local(src, dst, sem):
        return pltpu.make_async_copy(src, dst, sem)

    def ag_direct(ph, xg, r, p):
        cols = pl.ds(p * CW, CW)
        return remote(xg.at[my_rows, cols], xg.at[my_rows, cols], send_sem.at[ph, r, p], recv_sem.at[ph, r, p], 2 * chips[r] + core)

    def ag_direct_in(ph, xg, r, p):
        ref = xg.at[rows_of(core, chips[r]), pl.ds(p * CW, CW)]
        return remote(ref, ref, send_sem.at[ph, r, p], recv_sem.at[ph, r, p], 2 * chips[r] + core)

    def ag_forward(ph, xg, r, p):
        ref = xg.at[rows_of(core, chips[r]), pl.ds(p * CW, CW)]
        return remote(ref, ref, fsend_sem.at[ph, r, p], frecv_sem.at[ph, r, p], partner)

    def ag_forward_in(ph, xg, r, p):
        ref = xg.at[rows_of(other, chips[r]), pl.ds(p * CW, CW)]
        return remote(ref, ref, fsend_sem.at[ph, r, p], frecv_sem.at[ph, r, p], partner)

    def ag_start(ph, xg):
        for p in range(NP):
            for r in (3, 1, 2):
                ag_direct(ph, xg, r, p).start()
            ag_forward(ph, xg, 0, p).start()

    def ag_relay(ph, xg, p):
        for r in (1, 2, 3):
            ag_direct_in(ph, xg, r, p).wait_recv()
            ag_forward(ph, xg, r, p).start()

    def ag_arrive(ph, xg, p):
        for r in (0, 1, 2, 3):
            ag_forward_in(ph, xg, r, p).wait_recv()

    def ag_finish(ph, xg):
        for p in range(NP):
            for r in (1, 2, 3):
                ag_direct(ph, xg, r, p).wait_send()
            for r in (0, 1, 2, 3):
                ag_forward(ph, xg, r, p).wait_send()

    def rs_a(ph, n):
        return remote(pbuf.at[ph, n, pl.ds(pl.multiple_of(64 * other, 64), 64), :], ra.at[ph, n], asend_sem.at[ph, n], arecv_sem.at[ph, n], partner)

    def rs_b(ph, n, r):
        return remote(sb.at[ph, n, pl.ds(pl.multiple_of(16 * chips[r], 16), 16), :], rb.at[ph, r - 1, n], bsend_sem.at[ph, r, n], brecv_sem.at[ph, r, n], 2 * chips[r] + core)

    def rs_put(ph, n, part):
        pbuf[ph, n] = part.astype(BF16)
        rs_a(ph, n).start()

    def rs_pair(ph, n):
        rs_a(ph, n).wait_recv()
        own = pbuf[ph, n, pl.ds(pl.multiple_of(64 * core, 64), 64), :].astype(F32)
        sb[ph, n] = (own + ra[ph, n].astype(F32)).astype(BF16)
        for r in (3, 1, 2):
            rs_b(ph, n, r).start()

    def rs_sum(ph, n):
        total = sb[ph, n, pl.ds(pl.multiple_of(16 * chip, 16), 16), :].astype(F32)
        for r in (1, 2, 3):
            rs_b(ph, n, r).wait_recv()
            total = total + rb[ph, r - 1, n].astype(F32)
        return total

    def rs_finish(ph):
        for n in range(NP):
            rs_a(ph, n).wait_send()
            for r in (1, 2, 3):
                rs_b(ph, n, r).wait_send()

    def normed(rows, gain):
        ms = jnp.zeros((16, 128), F32)
        for j in range(32):
            v = rows[:, 128 * j:128 * j + 128].astype(F32)
            ms = ms + v * v
        inv = lax.rsqrt(jnp.sum(ms, axis=-1, keepdims=True) * (1.0 / D) + NORM_EPS)
        return inv

    def store_normed(src, gain, dst):
        inv = normed(src, gain)
        for j in range(32):
            cols = slice(128 * j, 128 * j + 128)
            val = src[:, cols].astype(F32) * inv * gain[j:j + 1, :].astype(F32)
            dst[my_rows, cols] = val.astype(BF16)

    gate_loads = []
    for p in range(NP):
        gate_loads.append(local(wg_hbm.at[pl.ds(p * CW, CW), :], wg.at[pl.ds(p * CW, CW), :], wsem.at[0, p]))
        gate_loads.append(local(wu_hbm.at[pl.ds(p * CW, CW), :], wu.at[pl.ds(p * CW, CW), :], wsem.at[1, p]))

    def attention_phase(kc, vc, vt, wo, freqv, qs, kch, vch, bias, o_buf):
        loads = {
            "x": local(x_hbm, xv, lsem.at[0]),
            "g1": local(g1_hbm, g1, lsem.at[1]),
            "freq": local(freq_hbm, freqv, lsem.at[6]),
            "vc": local(vc_hbm, vc, lsem.at[4]),
            "kc": local(kc_hbm, kc, lsem.at[5]),
            "wo": local(wo_hbm, wo, lsem.at[8]),
            "g2": local(g2_hbm, g2, lsem.at[9]),
            "start": local(start_hbm, start_ref, lsem.at[7]),
        }
        loads["x"].start()
        loads["g1"].start()
        barrier = pltpu.get_barrier_semaphore()
        for dev in (partner, 2 * flip1 + core, 2 * flip2 + core, 2 * flip3 + core):
            pl.semaphore_signal(barrier, inc=1, device_id={"tp": dev}, device_id_type=pl.DeviceIdType.MESH)
        tok_lane = token_of_row(lax.broadcasted_iota(jnp.int32, (1, 128), 1))

        def projection_phase(wq4, wqkv):
            wk_load = local(wk_hbm, wqkv.at[:, pl.ds(512, 128)], lsem.at[2])
            wv_load = local(wv_hbm, wqkv.at[:, pl.ds(640, 128)], lsem.at[3])
            wq_loads = [local(wq_hbm.at[pl.ds(p * 4 * CW, 4 * CW), :], wq4.at[pl.ds(p * 4 * CW, 4 * CW), :], dsem.at[p]) for p in range(NP)]
            for ld in wq_loads:
                ld.start()
            loads["vc"].start()
            loads["freq"].start()
            loads["start"].start()
            wk_load.start()
            wv_load.start()
            for name in ("kc", "wo", "g2"):
                loads[name].start()

            loads["x"].wait()
            loads["g1"].wait()
            store_normed(xv, g1, xg1)
            pl.semaphore_wait(barrier, 4)
            ag_start(0, xg1)

            ri = lax.broadcasted_iota(jnp.int32, (256, 256), 0)
            ci = lax.broadcasted_iota(jnp.int32, (256, 256), 1)
            perm = (ci == 4 * (ri % 64) + ri // 64).astype(F32).astype(BF16)

            def split_heads(p):
                wq_loads[p].wait()

                def body(i, carry):
                    base = p * (CW // 64) + 2 * i
                    rows4 = jnp.concatenate([wq4[pl.ds(pl.multiple_of((base + k) * 256, 256), 256), :] for k in range(2)], axis=1)
                    out = jnp.dot(perm, rows4, preferred_element_type=F32).astype(BF16)
                    for k in range(2):
                        for h in range(4):
                            wqkv[pl.ds(pl.multiple_of((base + k) * 64, 64), 64), h * 128:h * 128 + 128] = out[64 * h:64 * h + 64, k * 128:k * 128 + 128]
                    return carry

                for i in range(CW // 128):
                    body(i, 0)

            loads["vc"].wait()

            def flip_values(i, carry):
                ks = pl.ds(pl.multiple_of(i * KB, KB), KB)
                vt[:, ks] = vc[ks, :].astype(F32).T.astype(BF16)
                slot = i * KB + lax.broadcasted_iota(jnp.int32, (KB, 128), 0)
                off = jnp.bitwise_and(slot - start, W - 1)
                keep = jnp.where(off >= W - start, off, -1) > tok_lane
                bias[ks, :] = jnp.where(keep, 0.0, -jnp.inf)
                return carry

            loads["start"].wait()
            start = start_ref[0]
            for p in range(4):
                split_heads(p)
            for p in range(6):
                flip_values(p, 0)
            loads["freq"].wait()
            tok_row = token_of_row(lax.broadcasted_iota(jnp.int32, (T, 128), 0))
            angles = (start + tok_row).astype(F32) * freqv[0:1, :]
            cos_t = jnp.cos(angles)
            lane = lax.broadcasted_iota(jnp.int32, (T, 128), 1)
            even = lane % 2 == 0
            sin_t = jnp.sin(angles)
            sin_t = jnp.where(even, -sin_t, sin_t)
            wk_load.wait()
            wv_load.wait()
            acc = jnp.zeros((T, 768), F32)
            ag_relay(0, xg1, 0)
            ag_relay(0, xg1, 1)
            for p in range(NP):
                if p + 2 < NP:
                    ag_relay(0, xg1, p + 2)
                if p + 4 < NP:
                    split_heads(p + 4)
                if p < 2:
                    flip_values(p + 6, 0)
                ag_arrive(0, xg1, p)
                cols = slice(p * CW, p * CW + CW)
                acc = acc + jnp.dot(xg1[:, cols], wqkv[cols, :], preferred_element_type=F32)
            for ld in gate_loads:
                ld.start()

            def rotate(v):
                swapped = jnp.where(even, pltpu.roll(v, 127, 1), pltpu.roll(v, 1, 1))
                return v * cos_t + swapped * sin_t

            for h in range(4):
                qs[h * 128:h * 128 + 128, :] = rotate(acc[:, h * 128:h * 128 + 128]).astype(BF16)
            kch[...] = rotate(acc[:, 512:640]).astype(BF16)
            v_new = acc[:, 640:768].astype(BF16)
            vch[...] = v_new
            vt[:, W:W + T] = v_new.astype(F32).T.astype(BF16)

        pl.run_scoped(
            projection_phase,
            pltpu.VMEM((4 * D, 128), BF16),
            pltpu.VMEM((D, 768), BF16),
        )
        loads["kc"].wait()
        factor = (128.0 ** -0.5) * 1.4426950408889634

        def softmax_phase(s_buf):
            queries = qs[...]
            tops, masses = [], []
            for b in range(NKB + 1):
                n = KB if b < NKB else T
                ks = slice(b * KB, b * KB + n)
                keys = kc[ks, :] if b < NKB else kch[...]
                st = lax.dot_general(keys, queries, (((1,), (1,)), ((), ())), preferred_element_type=F32)
                if b < NKB:
                    shift = bias[ks, :]
                else:
                    shift = jnp.where(token_of_row(lax.broadcasted_iota(jnp.int32, (T, 128), 0)) <= tok_lane, 0.0, -jnp.inf)
                top, mass = [], []
                for g in range(4):
                    gs = slice(g * 128, g * 128 + 128)
                    part = st[:, gs] + shift
                    s_buf[ks, gs] = part
                    t = jnp.max(jnp.max(part.reshape(n // 8, 8, 128), axis=0), axis=0, keepdims=True)
                    t = jnp.maximum(t, jnp.finfo(F32).min)
                    e = jnp.exp2((s_buf[ks, gs] - t) * factor)
                    s_buf[ks, gs] = e
                    mass.append(jnp.sum(jnp.sum(e.reshape(n // 8, 8, 128), axis=0), axis=0, keepdims=True))
                    top.append(t)
                tops.append(jnp.concatenate(top, axis=1))
                masses.append(jnp.concatenate(mass, axis=1))
            best = functools.reduce(jnp.maximum, tops)
            scales = [jnp.exp2((t - best) * factor) for t in tops]
            total = sum(m * sc for m, sc in zip(masses, scales))
            inv = 1.0 / total
            out = None
            for b in range(NKB + 1):
                n = KB if b < NKB else T
                ks = slice(b * KB, b * KB + n)
                probs = (s_buf[ks, :] * (scales[b] * inv)).astype(BF16)
                part = jnp.dot(vt[:, ks], probs, preferred_element_type=F32)
                out = part if out is None else out + part
            for g in range(4):
                o_buf[:, g * 128:g * 128 + 128] = out[:, g * 128:g * 128 + 128].T.astype(BF16)

        pl.run_scoped(softmax_phase, pltpu.VMEM((W + T, 512), F32))
        loads["wo"].wait()
        for n in range(NP):
            cols = slice(n * CW, n * CW + CW)
            rs_put(0, n, jnp.dot(o_buf[...], wo[:, cols], preferred_element_type=F32))
            if n > 0:
                rs_pair(0, n - 1)
        rs_pair(0, NP - 1)
        loads["g2"].wait()

        chunk = jnp.concatenate([kch[...], vch[...]], axis=1)

        def merge(i, carry):
            ks = pl.ds(pl.multiple_of(i * KB, KB), KB)
            slot = i * KB + lax.broadcasted_iota(jnp.int32, (KB, 128), 0)
            off = jnp.bitwise_and(slot - start, W - 1)
            pick = (off == tok_lane).astype(F32).astype(BF16)
            placed = jnp.dot(pick, chunk, preferred_element_type=F32)
            fresh = off < T
            kn_ref[ks, :] = jnp.where(fresh, placed[:, 0:128], kc[ks, :].astype(F32)).astype(BF16)
            vn_ref[ks, :] = jnp.where(fresh, placed[:, 128:256], vc[ks, :].astype(F32)).astype(BF16)
            return carry

        start = start_ref[0]
        lax.fori_loop(0, NKB, merge, 0)

    pl.run_scoped(
        attention_phase,
        pltpu.VMEM((W, 128), BF16),
        pltpu.VMEM((W, 128), BF16),
        pltpu.VMEM((128, W + T), BF16),
        pltpu.VMEM((512, D), BF16),
        pltpu.VMEM((8, 128), F32),
        pltpu.VMEM((512, 128), BF16),
        pltpu.VMEM((T, 128), BF16),
        pltpu.VMEM((T, 128), BF16),
        pltpu.VMEM((W, 128), F32),
        pltpu.VMEM((T, 512), BF16),
    )

    def mlp_phase(wd, acc_g, acc_u, u_buf):
        down_loads = [local(wd_hbm.at[:, pl.ds(n * CW, CW)], wd.at[:, pl.ds(n * CW, CW)], dsem.at[n]) for n in range(NP)]
        for ld in down_loads:
            ld.start()
        for n in range(NP):
            cols = slice(n * CW, n * CW + CW)
            hb[:, cols] = (xv[:, cols].astype(F32) + rs_sum(0, n)).astype(BF16)
        store_normed(hb, g2, xg2)
        ag_start(1, xg2)
        ag_finish(0, xg1)
        rs_finish(0)
        ag_relay(1, xg2, 0)
        ag_relay(1, xg2, 1)
        for p in range(NP):
            if p + 2 < NP:
                ag_relay(1, xg2, p + 2)
            gate_loads[2 * p].wait()
            gate_loads[2 * p + 1].wait()
            ag_arrive(1, xg2, p)
            rows = slice(p * CW, p * CW + CW)
            m = xg2[:, rows]
            gate = jnp.dot(m, wg[rows, :], preferred_element_type=F32)
            up = jnp.dot(m, wu[rows, :], preferred_element_type=F32)
            if p == 0:
                acc_g[...] = gate
                acc_u[...] = up
            elif p + 1 < NP:
                acc_g[...] += gate
                acc_u[...] += up
            else:
                gate = acc_g[...] + gate
                u_buf[...] = (gate / (1.0 + jnp.exp(-gate)) * (acc_u[...] + up)).astype(BF16)
        for n in range(NP):
            cols = slice(n * CW, n * CW + CW)
            down_loads[n].wait()
            rs_put(1, n, jnp.dot(u_buf[...], wd[:, cols], preferred_element_type=F32))
            if n > 0:
                rs_pair(1, n - 1)
        rs_pair(1, NP - 1)
        ag_finish(1, xg2)
        for n in range(NP):
            cols = slice(n * CW, n * CW + CW)
            xo_ref[:, cols] = (hb[:, cols].astype(F32) + rs_sum(1, n)).astype(BF16)
        rs_finish(1)

    pl.run_scoped(
        mlp_phase,
        pltpu.VMEM((FF, D), BF16),
        pltpu.VMEM((T, FF), F32),
        pltpu.VMEM((T, FF), F32),
        pltpu.VMEM((T, FF), BF16),
    )


def solution(mesh):
    row_spec = P('dp', 'tp', None)
    cache_spec = P('dp', None, 'tp', None)
    head_cols = P(None, 'tp', None)
    in_specs = (row_spec, P('dp'), cache_spec, cache_spec, P(), head_cols, head_cols, head_cols, P('tp', None, None), P(), P(None, 'tp'), P(None, 'tp'), P('tp', None))
    out_specs = (row_spec, cache_spec, cache_spec)

    def local_layer(x_in, start_pos, k_cache, v_cache, attn_gain, w_query, w_key, w_value, w_out, mlp_gain, w_gate, w_up, w_down):
        freq = np.repeat(ROPE_BASE ** (-np.arange(0, 128, 2) / 128.0), 2).astype(np.float32)
        freq = jnp.asarray(np.tile(freq[None, :], (8, 1)))
        any_spec = pl.BlockSpec(memory_space=pl.ANY)
        vmem_spec = pl.BlockSpec(memory_space=pltpu.VMEM)
        dma = pltpu.SemaphoreType.DMA
        kc2 = k_cache.reshape(W, 128)
        vc2 = v_cache.reshape(W, 128)
        x_out, k_new, v_new = pl.pallas_call(
            layer_kernel,
            out_shape=(pltpu.VMEM((16, D), BF16), pltpu.VMEM((W, 128), BF16), pltpu.VMEM((W, 128), BF16)),
            in_specs=[any_spec] * 14,
            out_specs=(vmem_spec, vmem_spec, vmem_spec),
            scratch_shapes=[
                pltpu.SMEM((1,), jnp.int32),
                pltpu.VMEM((16, D), BF16),
                pltpu.VMEM((32, 128), BF16),
                pltpu.VMEM((32, 128), BF16),
                pltpu.VMEM((D, FF), BF16),
                pltpu.VMEM((D, FF), BF16),
                pltpu.VMEM((T, D), BF16),
                pltpu.VMEM((T, D), BF16),
                pltpu.VMEM((2, NP, T, CW), BF16),
                pltpu.VMEM((2, NP, 64, CW), BF16),
                pltpu.VMEM((2, NP, 64, CW), BF16),
                pltpu.VMEM((2, 3, NP, 16, CW), BF16),
                pltpu.VMEM((16, D), BF16),
                dma((10,)),
                dma((2, NP)),
                dma((NP,)),
                dma((2, 4, NP)),
                dma((2, 4, NP)),
                dma((2, 4, NP)),
                dma((2, 4, NP)),
                dma((2, NP)),
                dma((2, NP)),
                dma((2, 4, NP)),
                dma((2, 4, NP)),
            ],
            compiler_params=pltpu.CompilerParams(collective_id=0, has_side_effects=True, vmem_limit_bytes=VMEM_LIMIT),
            name="layer",
        )(
            start_pos, x_in.reshape(16, D), freq, kc2, vc2, attn_gain.reshape(32, 128), w_query.reshape(4 * D, 128),
            w_key.reshape(D, 128), w_value.reshape(D, 128), w_out.reshape(512, D), mlp_gain.reshape(32, 128), w_gate, w_up, w_down,
        )
        return x_out.reshape(x_in.shape), k_new.reshape(k_cache.shape), v_new.reshape(v_cache.shape)

    return jax.shard_map(local_layer, mesh=mesh, in_specs=in_specs, out_specs=out_specs, check_vma=False)
```

```python
import functools

import jax
import numpy as np
import jax.numpy as jnp
from jax import lax
from jax.experimental import pallas as pl
from jax.experimental.pallas import tpu as pltpu
from jax.sharding import PartitionSpec as P

ROPE_BASE = 10000.0
NORM_EPS = 1e-5
BF16 = jnp.bfloat16
F32 = jnp.float32
D = 4096
T = 128
FF = 1792
W = 4096
NP = 8
VMEM_LIMIT = 64000000
CW = D // NP
NQ = 4
CQ = D // NQ
AHEAD = 1
KB = 512
NKB = W // KB


def token_of_row(row):
    core = 1 - row // 64
    chip = (row // 16) % 4
    return 32 * chip + 16 * core + row % 16


def layer_kernel(start_hbm, x_hbm, freq_hbm, kc_hbm, vc_hbm, g1_hbm, wq_hbm, wk_hbm, wv_hbm, wo_hbm, g2_hbm, wg_hbm, wu_hbm, wd_hbm,
                 xo_ref, kn_ref, vn_ref,
                 start_ref, xv, g1, g2, wg, wu, xg1, xg2, pbuf, ra, sb, rb, hb,
                 lsem, wsem, dsem, send_sem, recv_sem, fsend_sem, frecv_sem, asend_sem, arecv_sem, bsend_sem, brecv_sem):
    me = lax.axis_index("tp")
    core = me % 2
    chip = me // 2
    other = 1 - core
    partner = 2 * chip + other
    flip1 = chip + 1 - 2 * (chip % 2)
    flip2 = chip + 2 - 4 * (chip // 2)
    flip3 = 3 - chip
    chips = (chip, flip1, flip2, flip3)
    my_rows = pl.ds(pl.multiple_of(64 * other + 16 * chip, 16), 16)

    def rows_of(c, q):
        return pl.ds(pl.multiple_of(64 * (1 - c) + 16 * q, 16), 16)

    def remote(src, dst, ssem, rsem, dev):
        return pltpu.make_async_remote_copy(src_ref=src, dst_ref=dst, send_sem=ssem, recv_sem=rsem, device_id={"tp": dev}, device_id_type=pl.DeviceIdType.MESH)

    def local(src, dst, sem):
        return pltpu.make_async_copy(src, dst, sem)

    widths = (CW, CQ)

    def piece(ph, xg, c, r, p):
        return xg.at[rows_of(c, chips[r]), pl.ds(p * widths[ph], widths[ph])]

    def ag_direct(ph, xg, r, p):
        ref = piece(ph, xg, core, 0, p)
        return remote(ref, ref, send_sem.at[ph, r, p], recv_sem.at[ph, r, p], 2 * chips[r] + core)

    def ag_direct_in(ph, xg, r, p):
        ref = piece(ph, xg, core, r, p)
        return remote(ref, ref, send_sem.at[ph, r, p], recv_sem.at[ph, r, p], 2 * chips[r] + core)

    def ag_forward(ph, xg, r, p):
        ref = piece(ph, xg, core, r, p)
        return remote(ref, ref, fsend_sem.at[ph, r, p], frecv_sem.at[ph, r, p], partner)

    def ag_forward_in(ph, xg, r, p):
        ref = piece(ph, xg, other, r, p)
        return remote(ref, ref, fsend_sem.at[ph, r, p], frecv_sem.at[ph, r, p], partner)

    def ag_start(ph, xg):
        for p in range(D // widths[ph]):
            for r in (3, 1, 2):
                ag_direct(ph, xg, r, p).start()
            ag_forward(ph, xg, 0, p).start()

    def ag_relay(ph, xg, p):
        for r in (1, 2, 3):
            ag_direct_in(ph, xg, r, p).wait_recv()
            ag_forward(ph, xg, r, p).start()

    def ag_arrive(ph, xg, p):
        for r in (0, 1, 2, 3):
            ag_forward_in(ph, xg, r, p).wait_recv()

    def ag_finish(ph, xg):
        for p in range(D // widths[ph]):
            for r in (1, 2, 3):
                ag_direct(ph, xg, r, p).wait_send()
            for r in (0, 1, 2, 3):
                ag_forward(ph, xg, r, p).wait_send()

    def owner(half):
        return pl.when(core == 1 - half)

    def helper(half):
        return pl.when(core == half)

    def rs_a(ph, half, n):
        return remote(pbuf.at[ph, half, n], ra.at[ph, n], asend_sem.at[ph, n], arecv_sem.at[ph, n], partner)

    def rs_b(ph, n, r):
        return remote(sb.at[ph, n, pl.ds(pl.multiple_of(16 * chips[r], 16), 16), :], rb.at[ph, r - 1, n], bsend_sem.at[ph, r, n], brecv_sem.at[ph, r, n], 2 * chips[r] + core)

    def rs_put(ph, half, n, part):
        pbuf[ph, half, n] = part.astype(BF16)

        @helper(half)
        def _():
            rs_a(ph, half, n).start()

    def rs_pairs(ph, half, pieces):
        @owner(half)
        def _():
            for n in pieces:
                rs_a(ph, half, n).wait_recv()
                sb[ph, n] = (pbuf[ph, half, n].astype(F32) + ra[ph, n].astype(F32)).astype(BF16)
                for r in (3, 1, 2):
                    rs_b(ph, n, r).start()

    def rs_sum(ph, n):
        total = sb[ph, n, pl.ds(pl.multiple_of(16 * chip, 16), 16), :].astype(F32)
        for r in (1, 2, 3):
            rs_b(ph, n, r).wait_recv()
            total = total + rb[ph, r - 1, n].astype(F32)
        return total

    def rs_finish(ph):
        for n in range(NQ):
            for half in range(2):
                @helper(half)
                def _():
                    rs_a(ph, half, n).wait_send()
            for r in (1, 2, 3):
                rs_b(ph, n, r).wait_send()

    def normed(rows, gain):
        ms = jnp.zeros((16, 128), F32)
        for j in range(32):
            v = rows[:, 128 * j:128 * j + 128].astype(F32)
            ms = ms + v * v
        inv = lax.rsqrt(jnp.sum(ms, axis=-1, keepdims=True) * (1.0 / D) + NORM_EPS)
        return inv

    def store_normed(src, gain, dst):
        inv = normed(src, gain)
        for j in range(32):
            cols = slice(128 * j, 128 * j + 128)
            val = src[:, cols].astype(F32) * inv * gain[j:j + 1, :].astype(F32)
            dst[my_rows, cols] = val.astype(BF16)

    gate_loads = []
    for p in range(NQ):
        gate_loads.append(local(wg_hbm.at[pl.ds(p * CQ, CQ), :], wg.at[pl.ds(p * CQ, CQ), :], wsem.at[0, p]))
        gate_loads.append(local(wu_hbm.at[pl.ds(p * CQ, CQ), :], wu.at[pl.ds(p * CQ, CQ), :], wsem.at[1, p]))

    def start_mlp_rows():
        for n in range(NQ):
            cols = slice(n * CQ, n * CQ + CQ)
            hb[:, cols] = (xv[:, cols].astype(F32) + rs_sum(0, n)).astype(BF16)
        store_normed(hb, g2, xg2)
        ag_start(1, xg2)

    def attention_phase(kc, vc, vt, wo, freqv, qs, kch, vch, bias, o_buf):
        loads = {
            "x": local(x_hbm, xv, lsem.at[0]),
            "g1": local(g1_hbm, g1, lsem.at[1]),
            "freq": local(freq_hbm, freqv, lsem.at[6]),
            "vc": local(vc_hbm, vc, lsem.at[4]),
            "kc": local(kc_hbm, kc, lsem.at[5]),
            "wo": local(wo_hbm, wo, lsem.at[8]),
            "g2": local(g2_hbm, g2, lsem.at[9]),
            "start": local(start_hbm, start_ref, lsem.at[7]),
        }
        loads["x"].start()
        loads["g1"].start()
        barrier = pltpu.get_barrier_semaphore()
        for dev in (partner, 2 * flip1 + core, 2 * flip2 + core, 2 * flip3 + core):
            pl.semaphore_signal(barrier, inc=1, device_id={"tp": dev}, device_id_type=pl.DeviceIdType.MESH)
        lane1 = lax.broadcasted_iota(jnp.int32, (1, 128), 1)
        tok_lane = token_of_row(lane1)
        tok_half = [token_of_row(64 * half + lane1 % 64) for half in range(2)]

        def projection_phase(wq4, wqkv):
            wk_load = local(wk_hbm, wqkv.at[:, pl.ds(512, 128)], lsem.at[2])
            wv_load = local(wv_hbm, wqkv.at[:, pl.ds(640, 128)], lsem.at[3])
            wq_loads = [local(wq_hbm.at[pl.ds(p * 4 * CW, 4 * CW), :], wq4.at[pl.ds(p * 4 * CW, 4 * CW), :], dsem.at[p]) for p in range(NP)]
            for ld in wq_loads:
                ld.start()
            loads["vc"].start()
            loads["freq"].start()
            loads["start"].start()
            wk_load.start()
            wv_load.start()
            for name in ("kc", "wo", "g2"):
                loads[name].start()

            loads["x"].wait()
            loads["g1"].wait()
            store_normed(xv, g1, xg1)
            pl.semaphore_wait(barrier, 4)
            ag_start(0, xg1)

            ri = lax.broadcasted_iota(jnp.int32, (256, 256), 0)
            ci = lax.broadcasted_iota(jnp.int32, (256, 256), 1)
            perm = (ci == 4 * (ri % 64) + ri // 64).astype(F32).astype(BF16)

            def split_heads(p):
                wq_loads[p].wait()

                def body(i, carry):
                    base = p * (CW // 64) + 2 * i
                    rows4 = jnp.concatenate([wq4[pl.ds(pl.multiple_of((base + k) * 256, 256), 256), :] for k in range(2)], axis=1)
                    out = jnp.dot(perm, rows4, preferred_element_type=F32).astype(BF16)
                    for k in range(2):
                        for h in range(4):
                            wqkv[pl.ds(pl.multiple_of((base + k) * 64, 64), 64), h * 128:h * 128 + 128] = out[64 * h:64 * h + 64, k * 128:k * 128 + 128]
                    return carry

                for i in range(CW // 128):
                    body(i, 0)

            loads["vc"].wait()

            def flip_values(i, carry):
                ks = pl.ds(pl.multiple_of(i * KB, KB), KB)
                vt[:, ks] = vc[ks, :].astype(F32).T.astype(BF16)
                slot = i * KB + lax.broadcasted_iota(jnp.int32, (KB, 128), 0)
                off = jnp.bitwise_and(slot - start, W - 1)
                limit = jnp.where(off >= W - start, off, -1)
                for half in range(2):
                    bias[half, ks, :] = jnp.where(limit > tok_half[half], 0.0, -jnp.inf)
                return carry

            loads["start"].wait()
            start = start_ref[0]
            for p in range(4):
                split_heads(p)
            for p in range(4):
                flip_values(p, 0)
            loads["freq"].wait()
            tok_row = token_of_row(lax.broadcasted_iota(jnp.int32, (T, 128), 0))
            angles = (start + tok_row).astype(F32) * freqv[0:1, :]
            cos_t = jnp.cos(angles)
            lane = lax.broadcasted_iota(jnp.int32, (T, 128), 1)
            even = lane % 2 == 0
            sin_t = jnp.sin(angles)
            sin_t = jnp.where(even, -sin_t, sin_t)
            wk_load.wait()
            wv_load.wait()
            acc = jnp.zeros((T, 768), F32)
            ag_relay(0, xg1, 0)
            ag_relay(0, xg1, 1)
            for p in range(NP):
                if p + 2 < NP:
                    ag_relay(0, xg1, p + 2)
                if p + 4 < NP:
                    split_heads(p + 4)
                if p < 4:
                    flip_values(p + 4, 0)
                ag_arrive(0, xg1, p)
                cols = slice(p * CW, p * CW + CW)
                acc = acc + jnp.dot(xg1[:, cols], wqkv[cols, :], preferred_element_type=F32)
            for ld in gate_loads:
                ld.start()

            def rotate(v):
                swapped = jnp.where(even, pltpu.roll(v, 127, 1), pltpu.roll(v, 1, 1))
                return v * cos_t + swapped * sin_t

            for h in range(4):
                turned = rotate(acc[:, h * 128:h * 128 + 128]).astype(BF16)
                for half in range(2):
                    qs[half, h * 64:h * 64 + 64, :] = turned[64 * half:64 * half + 64, :]
            kch[...] = rotate(acc[:, 512:640]).astype(BF16)
            v_new = acc[:, 640:768].astype(BF16)
            vch[...] = v_new
            vt[:, W:W + T] = v_new.astype(F32).T.astype(BF16)

        pl.run_scoped(
            projection_phase,
            pltpu.VMEM((4 * D, 128), BF16),
            pltpu.VMEM((D, 768), BF16),
        )
        loads["kc"].wait()
        factor = (128.0 ** -0.5) * 1.4426950408889634

        def softmax(half, s_buf, hook):
            queries = qs[half]
            tops, masses = [], []
            for b in range(NKB + 1):
                n = KB if b < NKB else T
                ks = slice(b * KB, b * KB + n)
                keys = kc[ks, :] if b < NKB else kch[...]
                st = lax.dot_general(keys, queries, (((1,), (1,)), ((), ())), preferred_element_type=F32)
                if b < NKB:
                    shift = bias[half, ks, :]
                else:
                    shift = jnp.where(token_of_row(lax.broadcasted_iota(jnp.int32, (T, 128), 0)) <= tok_half[half], 0.0, -jnp.inf)
                top, mass = [], []
                for g in range(2):
                    gs = slice(g * 128, g * 128 + 128)
                    part = st[:, gs] + shift
                    s_buf[ks, gs] = part
                    t = jnp.max(jnp.max(part.reshape(n // 8, 8, 128), axis=0), axis=0, keepdims=True)
                    t = jnp.maximum(t, jnp.finfo(F32).min)
                    e = jnp.exp2((s_buf[ks, gs] - t) * factor)
                    s_buf[ks, gs] = e
                    mass.append(jnp.sum(jnp.sum(e.reshape(n // 8, 8, 128), axis=0), axis=0, keepdims=True))
                    top.append(t)
                tops.append(jnp.concatenate(top, axis=1))
                masses.append(jnp.concatenate(mass, axis=1))
                if b == 1:
                    hook()
            best = functools.reduce(jnp.maximum, tops)
            scales = [jnp.exp2((t - best) * factor) for t in tops]
            total = sum(m * sc for m, sc in zip(masses, scales))
            inv = 1.0 / total
            out = None
            for b in range(NKB + 1):
                n = KB if b < NKB else T
                ks = slice(b * KB, b * KB + n)
                probs = (s_buf[ks, :] * (scales[b] * inv)).astype(BF16)
                part = jnp.dot(vt[:, ks], probs, preferred_element_type=F32)
                out = part if out is None else out + part
            for g in range(2):
                flipped = out[:, g * 128:g * 128 + 128].T.astype(BF16)
                for j in range(2):
                    h = 2 * g + j
                    o_buf[half, :, h * 128:h * 128 + 128] = flipped[64 * j:64 * j + 64, :]

        def project_out(half):
            for n in range(NQ):
                cols = slice(n * CQ, n * CQ + CQ)
                rs_put(0, half, n, jnp.dot(o_buf[half], wo[:, cols], preferred_element_type=F32))

        def softmax_phase(s_buf):
            softmax(0, s_buf, lambda: None)
            loads["wo"].wait()
            project_out(0)
            rs_pairs(0, 0, range(NQ // 2))
            softmax(1, s_buf, lambda: rs_pairs(0, 0, range(NQ // 2, NQ)))

        pl.run_scoped(softmax_phase, pltpu.VMEM((W + T, 256), F32))
        project_out(1)
        rs_pairs(0, 1, range(NQ))
        loads["g2"].wait()
        owner(0)(start_mlp_rows)

        chunk = jnp.concatenate([kch[...], vch[...]], axis=1)

        def merge(i, carry):
            ks = pl.ds(pl.multiple_of(i * KB, KB), KB)
            slot = i * KB + lax.broadcasted_iota(jnp.int32, (KB, 128), 0)
            off = jnp.bitwise_and(slot - start, W - 1)
            pick = (off == tok_lane).astype(F32).astype(BF16)
            placed = jnp.dot(pick, chunk, preferred_element_type=F32)
            fresh = off < T
            kn_ref[ks, :] = jnp.where(fresh, placed[:, 0:128], kc[ks, :].astype(F32)).astype(BF16)
            vn_ref[ks, :] = jnp.where(fresh, placed[:, 128:256], vc[ks, :].astype(F32)).astype(BF16)
            return carry

        start = start_ref[0]
        lax.fori_loop(0, NKB, merge, 0)

    pl.run_scoped(
        attention_phase,
        pltpu.VMEM((W, 128), BF16),
        pltpu.VMEM((W, 128), BF16),
        pltpu.VMEM((128, W + T), BF16),
        pltpu.VMEM((512, D), BF16),
        pltpu.VMEM((8, 128), F32),
        pltpu.VMEM((2, 256, 128), BF16),
        pltpu.VMEM((T, 128), BF16),
        pltpu.VMEM((T, 128), BF16),
        pltpu.VMEM((2, W, 128), F32),
        pltpu.VMEM((2, 64, 512), BF16),
    )

    def mlp_phase(wd, acc_g, acc_u, u_buf):
        down_loads = [local(wd_hbm.at[:, pl.ds(n * CQ, CQ)], wd.at[:, pl.ds(n * CQ, CQ)], dsem.at[n]) for n in range(NQ)]
        for ld in down_loads:
            ld.start()

        def relay(half, p):
            @owner(half)
            def _():
                ag_relay(1, xg2, p)

        def arrive(half, p):
            @helper(half)
            def _():
                ag_arrive(1, xg2, p)

        def gate_up(half, p):
            if half == 0:
                gate_loads[2 * p].wait()
                gate_loads[2 * p + 1].wait()
            arrive(half, p)
            rows = slice(p * CQ, p * CQ + CQ)
            m = xg2[64 * half:64 * half + 64, rows]
            gate = jnp.dot(m, wg[rows, :], preferred_element_type=F32)
            up = jnp.dot(m, wu[rows, :], preferred_element_type=F32)
            if p == 0:
                acc_g[...] = gate
                acc_u[...] = up
            elif p + 1 < NQ:
                acc_g[...] += gate
                acc_u[...] += up
            else:
                gate = acc_g[...] + gate
                u_buf[...] = (gate / (1.0 + jnp.exp(-gate)) * (acc_u[...] + up)).astype(BF16)

        def down(half, n):
            cols = slice(n * CQ, n * CQ + CQ)
            if half == 0:
                down_loads[n].wait()
            rs_put(1, half, n, jnp.dot(u_buf[...], wd[:, cols], preferred_element_type=F32))

        for p in range(AHEAD):
            relay(0, p)
        for p in range(NQ):
            if p + AHEAD < NQ:
                relay(0, p + AHEAD)
            gate_up(0, p)
            if p == NQ // 4:
                owner(1)(start_mlp_rows)
        for n in range(NQ):
            down(0, n)
            if n > 0:
                rs_pairs(1, 0, [n - 1])
            if n + 1 < NQ:
                relay(1, n)
        rs_pairs(1, 0, [NQ - 1])
        for p in range(NQ):
            if p == 0:
                relay(1, NQ - 1)
            gate_up(1, p)
        for n in range(NQ):
            down(1, n)
            if n > 0:
                rs_pairs(1, 1, [n - 1])
        rs_pairs(1, 1, [NQ - 1])
        ag_finish(0, xg1)
        rs_finish(0)
        ag_finish(1, xg2)
        for n in range(NQ):
            cols = slice(n * CQ, n * CQ + CQ)
            xo_ref[:, cols] = (hb[:, cols].astype(F32) + rs_sum(1, n)).astype(BF16)
        rs_finish(1)

    pl.run_scoped(
        mlp_phase,
        pltpu.VMEM((FF, D), BF16),
        pltpu.VMEM((64, FF), F32),
        pltpu.VMEM((64, FF), F32),
        pltpu.VMEM((64, FF), BF16),
    )


def solution(mesh):
    row_spec = P('dp', 'tp', None)
    cache_spec = P('dp', None, 'tp', None)
    head_cols = P(None, 'tp', None)
    in_specs = (row_spec, P('dp'), cache_spec, cache_spec, P(), head_cols, head_cols, head_cols, P('tp', None, None), P(), P(None, 'tp'), P(None, 'tp'), P('tp', None))
    out_specs = (row_spec, cache_spec, cache_spec)

    def local_layer(x_in, start_pos, k_cache, v_cache, attn_gain, w_query, w_key, w_value, w_out, mlp_gain, w_gate, w_up, w_down):
        freq = np.repeat(ROPE_BASE ** (-np.arange(0, 128, 2) / 128.0), 2).astype(np.float32)
        freq = jnp.asarray(np.tile(freq[None, :], (8, 1)))
        any_spec = pl.BlockSpec(memory_space=pl.ANY)
        vmem_spec = pl.BlockSpec(memory_space=pltpu.VMEM)
        dma = pltpu.SemaphoreType.DMA
        kc2 = k_cache.reshape(W, 128)
        vc2 = v_cache.reshape(W, 128)
        x_out, k_new, v_new = pl.pallas_call(
            layer_kernel,
            out_shape=(pltpu.VMEM((16, D), BF16), pltpu.VMEM((W, 128), BF16), pltpu.VMEM((W, 128), BF16)),
            in_specs=[any_spec] * 14,
            out_specs=(vmem_spec, vmem_spec, vmem_spec),
            scratch_shapes=[
                pltpu.SMEM((1,), jnp.int32),
                pltpu.VMEM((16, D), BF16),
                pltpu.VMEM((32, 128), BF16),
                pltpu.VMEM((32, 128), BF16),
                pltpu.VMEM((D, FF), BF16),
                pltpu.VMEM((D, FF), BF16),
                pltpu.VMEM((T, D), BF16),
                pltpu.VMEM((T, D), BF16),
                pltpu.VMEM((2, 2, NQ, 64, CQ), BF16),
                pltpu.VMEM((2, NQ, 64, CQ), BF16),
                pltpu.VMEM((2, NQ, 64, CQ), BF16),
                pltpu.VMEM((2, 3, NQ, 16, CQ), BF16),
                pltpu.VMEM((16, D), BF16),
                dma((10,)),
                dma((2, NP)),
                dma((NP,)),
                dma((2, 4, NP)),
                dma((2, 4, NP)),
                dma((2, 4, NP)),
                dma((2, 4, NP)),
                dma((2, NP)),
                dma((2, NP)),
                dma((2, 4, NP)),
                dma((2, 4, NP)),
            ],
            compiler_params=pltpu.CompilerParams(collective_id=0, has_side_effects=True, vmem_limit_bytes=VMEM_LIMIT),
            name="layer",
        )(
            start_pos, x_in.reshape(16, D), freq, kc2, vc2, attn_gain.reshape(32, 128), w_query.reshape(4 * D, 128),
            w_key.reshape(D, 128), w_value.reshape(D, 128), w_out.reshape(512, D), mlp_gain.reshape(32, 128), w_gate, w_up, w_down,
        )
        return x_out.reshape(x_in.shape), k_new.reshape(k_cache.shape), v_new.reshape(v_cache.shape)

    return jax.shard_map(local_layer, mesh=mesh, in_specs=in_specs, out_specs=out_specs, check_vma=False)
```

```python
import functools

import jax
import numpy as np
import jax.numpy as jnp
from jax import lax
from jax.experimental import pallas as pl
from jax.experimental.pallas import tpu as pltpu
from jax.sharding import PartitionSpec as P

ROPE_BASE = 10000.0
NORM_EPS = 1e-5
BF16 = jnp.bfloat16
F32 = jnp.float32
D = 4096
T = 128
FF = 1792
W = 4096
NP = 8
CW = D // NP
GATHER = [(512 * p, 512) for p in range(7)] + [(3584, 256), (3840, 256)]
SCATTER = [(512 * p, 512) for p in range(8)]
NA = len(GATHER)
NR = len(SCATTER)
LAG = 3
VMEM_LIMIT = 64000000
KB = 512
NKB = W // KB


def token_of_row(row):
    core = row // 64
    chip = (row // 16) % 4
    return 32 * chip + 16 * core + row % 16


def layer_kernel(start_hbm, x_hbm, freq_hbm, kc_hbm, vc_hbm, g1_hbm, wq_hbm, wk_hbm, wv_hbm, wo_hbm, g2_hbm, wg_hbm, wu_hbm, wd_hbm,
                 xo_ref, kn_ref, vn_ref,
                 start_ref, xv, g1, g2, wg, wu, xg1, xg2, pbuf, ra, sb, rb, hb,
                 lsem, wsem, dsem, send_sem, recv_sem, fsend_sem, frecv_sem, asend_sem, arecv_sem, bsend_sem, brecv_sem):
    me = lax.axis_index("tp")
    core = me % 2
    chip = me // 2
    other = 1 - core
    partner = 2 * chip + other
    flip1 = chip + 1 - 2 * (chip % 2)
    flip2 = chip + 2 - 4 * (chip // 2)
    flip3 = 3 - chip
    chips = (chip, flip1, flip2, flip3)
    my_rows = pl.ds(pl.multiple_of(64 * core + 16 * chip, 16), 16)

    def rows_of(c, q):
        return pl.ds(pl.multiple_of(64 * c + 16 * q, 16), 16)

    def remote(src, dst, ssem, rsem, dev):
        return pltpu.make_async_remote_copy(src_ref=src, dst_ref=dst, send_sem=ssem, recv_sem=rsem, device_id={"tp": dev}, device_id_type=pl.DeviceIdType.MESH)

    def local(src, dst, sem):
        return pltpu.make_async_copy(src, dst, sem)

    def ag_direct(ph, xg, r, p):
        cols = pl.ds(*GATHER[p])
        return remote(xg.at[my_rows, cols], xg.at[my_rows, cols], send_sem.at[ph, r, p], recv_sem.at[ph, r, p], 2 * chips[r] + core)

    def ag_direct_in(ph, xg, r, p):
        ref = xg.at[rows_of(core, chips[r]), pl.ds(*GATHER[p])]
        return remote(ref, ref, send_sem.at[ph, r, p], recv_sem.at[ph, r, p], 2 * chips[r] + core)

    def ag_forward(ph, xg, r, p):
        ref = xg.at[rows_of(core, chips[r]), pl.ds(*GATHER[p])]
        return remote(ref, ref, fsend_sem.at[ph, r, p], frecv_sem.at[ph, r, p], partner)

    def ag_forward_in(ph, xg, r, p):
        ref = xg.at[rows_of(other, chips[r]), pl.ds(*GATHER[p])]
        return remote(ref, ref, fsend_sem.at[ph, r, p], frecv_sem.at[ph, r, p], partner)

    def ag_start(ph, xg):
        for p in range(NA):
            for r in (3, 1, 2):
                ag_direct(ph, xg, r, p).start()
            ag_forward(ph, xg, 0, p).start()

    def ag_relay(ph, xg, p):
        for r in (1, 2, 3):
            ag_direct_in(ph, xg, r, p).wait_recv()
            ag_forward(ph, xg, r, p).start()

    def ag_arrive(ph, xg, p):
        for r in (0, 1, 2, 3):
            ag_forward_in(ph, xg, r, p).wait_recv()

    def ag_finish(ph, xg):
        for p in range(NA):
            for r in (1, 2, 3):
                ag_direct(ph, xg, r, p).wait_send()
            for r in (0, 1, 2, 3):
                ag_forward(ph, xg, r, p).wait_send()

    def rs_a(ph, n):
        cols = pl.ds(*SCATTER[n])
        return remote(pbuf.at[ph, pl.ds(pl.multiple_of(64 * other, 64), 64), cols], ra.at[ph, :, cols], asend_sem.at[ph, n], arecv_sem.at[ph, n], partner)

    def rs_b(ph, n, r):
        cols = pl.ds(*SCATTER[n])
        return remote(sb.at[ph, pl.ds(pl.multiple_of(16 * chips[r], 16), 16), cols], rb.at[ph, r - 1, :, cols], bsend_sem.at[ph, r, n], brecv_sem.at[ph, r, n], 2 * chips[r] + core)

    def rs_put(ph, n, part):
        pbuf[ph, :, pl.ds(*SCATTER[n])] = part.astype(BF16)
        rs_a(ph, n).start()

    def rs_pair(ph, n):
        cols = pl.ds(*SCATTER[n])
        rs_a(ph, n).wait_recv()
        own = pbuf[ph, pl.ds(pl.multiple_of(64 * core, 64), 64), cols].astype(F32)
        sb[ph, :, cols] = (own + ra[ph, :, cols].astype(F32)).astype(BF16)
        for r in (3, 1, 2):
            rs_b(ph, n, r).start()

    def rs_all(ph, product, group):
        for n in range(0, NR, group):
            part = product(n, pl.ds(SCATTER[n][0], group * CW))
            for k in range(group):
                rs_put(ph, n + k, part[:, k * CW:k * CW + CW])
            for k in range(n - LAG, n - LAG + group):
                if k >= 0:
                    rs_pair(ph, k)
        for n in range(NR - LAG, NR):
            rs_pair(ph, n)

    def rs_sum(ph, n):
        cols = pl.ds(*SCATTER[n])
        total = sb[ph, pl.ds(pl.multiple_of(16 * chip, 16), 16), cols].astype(F32)
        for r in (1, 2, 3):
            rs_b(ph, n, r).wait_recv()
            total = total + rb[ph, r - 1, :, cols].astype(F32)
        return total

    def rs_finish(ph):
        for n in range(NR):
            rs_a(ph, n).wait_send()
            for r in (1, 2, 3):
                rs_b(ph, n, r).wait_send()

    def normed(rows, gain):
        ms = jnp.zeros((16, 128), F32)
        for j in range(32):
            v = rows[:, 128 * j:128 * j + 128].astype(F32)
            ms = ms + v * v
        inv = lax.rsqrt(jnp.sum(ms, axis=-1, keepdims=True) * (1.0 / D) + NORM_EPS)
        return inv

    def store_normed(src, gain, dst):
        inv = normed(src, gain)
        for j in range(32):
            cols = slice(128 * j, 128 * j + 128)
            val = src[:, cols].astype(F32) * inv * gain[j:j + 1, :].astype(F32)
            dst[my_rows, cols] = val.astype(BF16)

    gate_loads = []
    for p in range(NA):
        rows = pl.ds(*GATHER[p])
        gate_loads.append(local(wg_hbm.at[rows, :], wg.at[rows, :], wsem.at[0, p]))
        gate_loads.append(local(wu_hbm.at[rows, :], wu.at[rows, :], wsem.at[1, p]))

    def attention_phase(kc, vc, vt, wo, freqv, qt, kch, vch, bias, o_buf):
        loads = {
            "x": local(x_hbm, xv, lsem.at[0]),
            "g1": local(g1_hbm, g1, lsem.at[1]),
            "freq": local(freq_hbm, freqv, lsem.at[6]),
            "vc": local(vc_hbm, vc, lsem.at[4]),
            "kc": local(kc_hbm, kc, lsem.at[5]),
            "wo": local(wo_hbm, wo, lsem.at[8]),
            "g2": local(g2_hbm, g2, lsem.at[9]),
            "start": local(start_hbm, start_ref, lsem.at[7]),
        }
        loads["x"].start()
        loads["g1"].start()
        barrier = pltpu.get_barrier_semaphore()
        for dev in (partner, 2 * flip1 + core, 2 * flip2 + core, 2 * flip3 + core):
            pl.semaphore_signal(barrier, inc=1, device_id={"tp": dev}, device_id_type=pl.DeviceIdType.MESH)
        tok_lane = token_of_row(lax.broadcasted_iota(jnp.int32, (1, 128), 1))

        def projection_phase(wq4, wqkv):
            wk_load = local(wk_hbm, wqkv.at[:, pl.ds(512, 128)], lsem.at[2])
            wv_load = local(wv_hbm, wqkv.at[:, pl.ds(640, 128)], lsem.at[3])
            wq_loads = [local(wq_hbm.at[pl.ds(p * 4 * CW, 4 * CW), :], wq4.at[pl.ds(p * 4 * CW, 4 * CW), :], dsem.at[p]) for p in range(NP)]
            for ld in wq_loads:
                ld.start()
            loads["vc"].start()
            loads["freq"].start()
            loads["start"].start()
            wk_load.start()
            wv_load.start()
            for name in ("kc", "wo", "g2"):
                loads[name].start()

            loads["x"].wait()
            loads["g1"].wait()
            store_normed(xv, g1, xg1)
            pl.semaphore_wait(barrier, 4)
            ag_start(0, xg1)

            ri = lax.broadcasted_iota(jnp.int32, (256, 256), 0)
            ci = lax.broadcasted_iota(jnp.int32, (256, 256), 1)
            perm = (ci == 4 * (ri % 64) + ri // 64).astype(F32).astype(BF16)

            def split_heads(p):
                wq_loads[p].wait()

                def body(i, carry):
                    base = p * (CW // 64) + 2 * i
                    rows4 = jnp.concatenate([wq4[pl.ds(pl.multiple_of((base + k) * 256, 256), 256), :] for k in range(2)], axis=1)
                    out = jnp.dot(perm, rows4, preferred_element_type=F32).astype(BF16)
                    for k in range(2):
                        for h in range(4):
                            wqkv[pl.ds(pl.multiple_of((base + k) * 64, 64), 64), h * 128:h * 128 + 128] = out[64 * h:64 * h + 64, k * 128:k * 128 + 128]
                    return carry

                for i in range(CW // 128):
                    body(i, 0)

            loads["vc"].wait()

            def flip_values(i, carry):
                ks = pl.ds(pl.multiple_of(i * KB, KB), KB)
                vt[:, ks] = vc[ks, :].astype(F32).T.astype(BF16)
                slot = i * KB + lax.broadcasted_iota(jnp.int32, (KB, 128), 0)
                off = jnp.bitwise_and(slot - start, W - 1)
                keep = jnp.where(off >= W - start, off, -1) > tok_lane
                bias[ks, :] = jnp.where(keep, 0.0, -jnp.inf)
                return carry

            loads["start"].wait()
            start = start_ref[0]
            for p in range(4):
                split_heads(p)
            for p in range(6):
                flip_values(p, 0)
            loads["freq"].wait()
            tok_row = token_of_row(lax.broadcasted_iota(jnp.int32, (T, 128), 0))
            angles = (start + tok_row).astype(F32) * freqv[0:1, :]
            cos_t = jnp.cos(angles)
            lane = lax.broadcasted_iota(jnp.int32, (T, 128), 1)
            even = lane % 2 == 0
            sin_t = jnp.sin(angles)
            sin_t = jnp.where(even, -sin_t, sin_t)
            wk_load.wait()
            wv_load.wait()
            acc = jnp.zeros((T, 768), F32)
            ag_relay(0, xg1, 0)
            ag_relay(0, xg1, 1)
            for p in range(NA):
                if p + 2 < NA:
                    ag_relay(0, xg1, p + 2)
                if p + 4 < NP:
                    split_heads(p + 4)
                if p < 2:
                    flip_values(p + 6, 0)
                ag_arrive(0, xg1, p)
                cols = pl.ds(*GATHER[p])
                acc = acc + jnp.dot(xg1[:, cols], wqkv[cols, :], preferred_element_type=F32)
            for ld in gate_loads:
                ld.start()

            def rotate(v):
                swapped = jnp.where(even, pltpu.roll(v, 127, 1), pltpu.roll(v, 1, 1))
                return v * cos_t + swapped * sin_t

            for h in range(4):
                qt[:, h * 128:h * 128 + 128] = rotate(acc[:, h * 128:h * 128 + 128]).T.astype(BF16)
            kch[...] = rotate(acc[:, 512:640]).astype(BF16)
            v_new = acc[:, 640:768].astype(BF16)
            vch[...] = v_new
            vt[:, W:W + T] = v_new.astype(F32).T.astype(BF16)

        pl.run_scoped(
            projection_phase,
            pltpu.VMEM((4 * D, 128), BF16),
            pltpu.VMEM((D, 768), BF16),
        )
        loads["kc"].wait()
        factor = (128.0 ** -0.5) * 1.4426950408889634

        def softmax_phase(e_buf):
            queries = qt[...]
            tops, masses = [], []
            for b in range(NKB + 1):
                keys = kc[b * KB:b * KB + KB, :] if b < NKB else kch[...]
                scores = jnp.dot(keys, queries, preferred_element_type=F32)
                for i in range(KB // 128 if b < NKB else 1):
                    ks = slice(b * KB + i * 128, b * KB + i * 128 + 128)
                    if b < NKB:
                        shift = bias[ks, :]
                    else:
                        shift = jnp.where(token_of_row(lax.broadcasted_iota(jnp.int32, (T, 128), 0)) <= tok_lane, 0.0, -jnp.inf)
                    top, mass = [], []
                    for g in range(4):
                        gs = slice(g * 128, g * 128 + 128)
                        part = (scores[i * 128:i * 128 + 128, gs] + shift).reshape(16, 8, 128)
                        t = jnp.maximum(jnp.max(part, axis=0), jnp.finfo(F32).min)
                        e = jnp.exp2((part - t[None]) * factor)
                        e_buf[ks, gs] = e.reshape(128, 128)
                        mass.append(jnp.sum(e, axis=0))
                        top.append(t)
                    tops.append(top)
                    masses.append(mass)
            blocks = len(tops)
            weights = []
            for g in range(4):
                best = jnp.max(functools.reduce(jnp.maximum, [tops[b][g] for b in range(blocks)]), axis=0, keepdims=True)
                scales = [jnp.exp2((tops[b][g] - best) * factor) for b in range(blocks)]
                total = functools.reduce(jnp.add, [masses[b][g] * scales[b] for b in range(blocks)])
                inv = 1.0 / jnp.sum(total, axis=0, keepdims=True)
                weights.append([sc * inv for sc in scales])
            out = None
            for b in range(NKB + 1):
                n = KB if b < NKB else T
                ks = slice(b * KB, b * KB + n)
                rows = []
                for i in range(n // 128):
                    r0 = b * KB + i * 128
                    cols = [(e_buf[r0:r0 + 128, g * 128:g * 128 + 128].reshape(16, 8, 128) * weights[g][b * (KB // 128) + i][None]).reshape(128, 128) for g in range(4)]
                    rows.append(jnp.concatenate(cols, axis=1))
                probs = jnp.concatenate(rows, axis=0).astype(BF16)
                part = jnp.dot(vt[:, ks], probs, preferred_element_type=F32)
                out = part if out is None else out + part
            for g in range(4):
                o_buf[:, g * 128:g * 128 + 128] = out[:, g * 128:g * 128 + 128].T.astype(BF16)

        pl.run_scoped(softmax_phase, pltpu.VMEM((W + T, 512), F32))
        loads["wo"].wait()
        rs_all(0, lambda n, cols: jnp.dot(o_buf[...], wo[:, cols], preferred_element_type=F32), 2)
        loads["g2"].wait()

        chunk = jnp.concatenate([kch[...], vch[...]], axis=1)

        def merge(i, carry):
            ks = pl.ds(pl.multiple_of(i * KB, KB), KB)
            slot = i * KB + lax.broadcasted_iota(jnp.int32, (KB, 128), 0)
            off = jnp.bitwise_and(slot - start, W - 1)
            pick = (off == tok_lane).astype(F32).astype(BF16)
            placed = jnp.dot(pick, chunk, preferred_element_type=F32)
            fresh = off < T
            kn_ref[ks, :] = jnp.where(fresh, placed[:, 0:128], kc[ks, :].astype(F32)).astype(BF16)
            vn_ref[ks, :] = jnp.where(fresh, placed[:, 128:256], vc[ks, :].astype(F32)).astype(BF16)
            return carry

        start = start_ref[0]
        lax.fori_loop(0, NKB, merge, 0)

    pl.run_scoped(
        attention_phase,
        pltpu.VMEM((W, 128), BF16),
        pltpu.VMEM((W, 128), BF16),
        pltpu.VMEM((128, W + T), BF16),
        pltpu.VMEM((512, D), BF16),
        pltpu.VMEM((8, 128), F32),
        pltpu.VMEM((128, 512), BF16),
        pltpu.VMEM((T, 128), BF16),
        pltpu.VMEM((T, 128), BF16),
        pltpu.VMEM((W, 128), F32),
        pltpu.VMEM((T, 512), BF16),
    )

    def mlp_phase(wd, acc_g, acc_u, u_buf):
        down_loads = [local(wd_hbm.at[:, pl.ds(n * CW, CW)], wd.at[:, pl.ds(n * CW, CW)], dsem.at[n]) for n in range(NP)]
        for ld in down_loads:
            ld.start()
        for n in range(NR):
            cols = pl.ds(*SCATTER[n])
            hb[:, cols] = (xv[:, cols].astype(F32) + rs_sum(0, n)).astype(BF16)
        store_normed(hb, g2, xg2)
        ag_start(1, xg2)
        ag_finish(0, xg1)
        rs_finish(0)
        ag_relay(1, xg2, 0)
        ag_relay(1, xg2, 1)
        for p in range(NA):
            if p + 2 < NA:
                ag_relay(1, xg2, p + 2)
            gate_loads[2 * p].wait()
            gate_loads[2 * p + 1].wait()
            ag_arrive(1, xg2, p)
            rows = pl.ds(*GATHER[p])
            m = xg2[:, rows]
            gate = jnp.dot(m, wg[rows, :], preferred_element_type=F32)
            up = jnp.dot(m, wu[rows, :], preferred_element_type=F32)
            if p == 0:
                acc_g[...] = gate
                acc_u[...] = up
            elif p + 1 < NA:
                acc_g[...] += gate
                acc_u[...] += up
            else:
                gate = acc_g[...] + gate
                u_buf[...] = (gate / (1.0 + jnp.exp(-gate)) * (acc_u[...] + up)).astype(BF16)
        def down(n, cols):
            down_loads[n].wait()
            return jnp.dot(u_buf[...], wd[:, cols], preferred_element_type=F32)

        rs_all(1, down, 1)
        ag_finish(1, xg2)
        for n in range(NR):
            cols = pl.ds(*SCATTER[n])
            xo_ref[:, cols] = (hb[:, cols].astype(F32) + rs_sum(1, n)).astype(BF16)
        rs_finish(1)

    pl.run_scoped(
        mlp_phase,
        pltpu.VMEM((FF, D), BF16),
        pltpu.VMEM((T, FF), F32),
        pltpu.VMEM((T, FF), F32),
        pltpu.VMEM((T, FF), BF16),
    )


def write_kernel(x_ref, k_ref, v_ref, xo_hbm, ko_hbm, vo_hbm, sem):
    copies = [pltpu.make_async_copy(src, dst, sem.at[i]) for i, (src, dst) in enumerate(((k_ref, ko_hbm), (v_ref, vo_hbm), (x_ref, xo_hbm)))]
    for copy in copies:
        copy.start()
    for copy in copies:
        copy.wait()


def solution(mesh):
    row_spec = P('dp', 'tp', None)
    cache_spec = P('dp', None, 'tp', None)
    head_cols = P(None, 'tp', None)
    in_specs = (row_spec, P('dp'), cache_spec, cache_spec, P(), head_cols, head_cols, head_cols, P('tp', None, None), P(), P(None, 'tp'), P(None, 'tp'), P('tp', None))
    out_specs = (row_spec, cache_spec, cache_spec)

    def local_layer(x_in, start_pos, k_cache, v_cache, attn_gain, w_query, w_key, w_value, w_out, mlp_gain, w_gate, w_up, w_down):
        freq = np.repeat(ROPE_BASE ** (-np.arange(0, 128, 2) / 128.0), 2).astype(np.float32)
        freq = jnp.asarray(np.tile(freq[None, :], (8, 1)))
        any_spec = pl.BlockSpec(memory_space=pl.ANY)
        vmem_spec = pl.BlockSpec(memory_space=pltpu.VMEM)
        dma = pltpu.SemaphoreType.DMA
        kc2 = k_cache.reshape(W, 128)
        vc2 = v_cache.reshape(W, 128)
        results = pl.pallas_call(
            layer_kernel,
            out_shape=(pltpu.VMEM((16, D), BF16), pltpu.VMEM((W, 128), BF16), pltpu.VMEM((W, 128), BF16)),
            in_specs=[pl.BlockSpec(memory_space=pltpu.HBM)] + [any_spec] * 13,
            out_specs=(vmem_spec, vmem_spec, vmem_spec),
            scratch_shapes=[
                pltpu.SMEM((1,), jnp.int32),
                pltpu.VMEM((16, D), BF16),
                pltpu.VMEM((32, 128), BF16),
                pltpu.VMEM((32, 128), BF16),
                pltpu.VMEM((D, FF), BF16),
                pltpu.VMEM((D, FF), BF16),
                pltpu.VMEM((T, D), BF16),
                pltpu.VMEM((T, D), BF16),
                pltpu.VMEM((2, T, D), BF16),
                pltpu.VMEM((2, 64, D), BF16),
                pltpu.VMEM((2, 64, D), BF16),
                pltpu.VMEM((2, 3, 16, D), BF16),
                pltpu.VMEM((16, D), BF16),
                dma((10,)),
                dma((2, NA)),
                dma((NP,)),
                dma((2, 4, NA)),
                dma((2, 4, NA)),
                dma((2, 4, NA)),
                dma((2, 4, NA)),
                dma((2, NR)),
                dma((2, NR)),
                dma((2, 4, NR)),
                dma((2, 4, NR)),
            ],
            compiler_params=pltpu.CompilerParams(collective_id=0, has_side_effects=True, vmem_limit_bytes=VMEM_LIMIT),
            name="layer",
        )(
            start_pos, x_in.reshape(16, D), freq, kc2, vc2, attn_gain.reshape(32, 128), w_query.reshape(4 * D, 128),
            w_key.reshape(D, 128), w_value.reshape(D, 128), w_out.reshape(512, D), mlp_gain.reshape(32, 128), w_gate, w_up, w_down,
        )
        x_out, k_new, v_new = pl.pallas_call(
            write_kernel,
            out_shape=(jax.ShapeDtypeStruct((16, D), BF16), jax.ShapeDtypeStruct((W, 128), BF16), jax.ShapeDtypeStruct((W, 128), BF16)),
            in_specs=[vmem_spec] * 3,
            out_specs=(pl.BlockSpec(memory_space=pltpu.HBM),) * 3,
            scratch_shapes=[dma((3,))],
            compiler_params=pltpu.CompilerParams(vmem_limit_bytes=1 << 20),
            name="write",
        )(*[pltpu.with_memory_space_constraint(r, pltpu.VMEM) for r in results])
        return x_out.reshape(x_in.shape), k_new.reshape(k_cache.shape), v_new.reshape(v_cache.shape)

    return jax.shard_map(local_layer, mesh=mesh, in_specs=in_specs, out_specs=out_specs, check_vma=False)
```

```python
import functools

import jax
import numpy as np
import jax.numpy as jnp
from jax import lax
from jax.experimental import pallas as pl
from jax.experimental.pallas import tpu as pltpu
from jax.sharding import PartitionSpec as P

ROPE_BASE = 10000.0
NORM_EPS = 1e-5
BF16 = jnp.bfloat16
F32 = jnp.float32
D = 4096
T = 128
FF = 1792
W = 4096
NP = 8
CW = D // NP
GATHER = [(512 * p, 512) for p in range(7)] + [(3584, 256), (3840, 256)]
SCATTER = [(512 * p, 512) for p in range(8)]
NA = len(GATHER)
NR = len(SCATTER)
LAG = 2
VIA = 4
VMEM_LIMIT = 64000000
KB = 512
NKB = W // KB


def token_of_row(row):
    core = row // 64
    chip = (row // 16) % 4
    return 32 * chip + 16 * core + row % 16


def layer_kernel(start_hbm, x_hbm, freq_hbm, kc_hbm, vc_hbm, g1_hbm, wq_hbm, wk_hbm, wv_hbm, wo_hbm, g2_hbm, wg_hbm, wu_hbm, wd_hbm,
                 xo_ref, kn_ref, vn_ref,
                 start_ref, xv, g1, g2, wg, wu, xg1, xg2, pbuf, ra, sb, rb, tb, hb,
                 lsem, wsem, dsem, send_sem, recv_sem, fsend_sem, frecv_sem, asend_sem, arecv_sem, bsend_sem, brecv_sem):
    me = lax.axis_index("tp")
    core = me % 2
    chip = me // 2
    other = 1 - core
    partner = 2 * chip + other
    flip1 = chip + 1 - 2 * (chip % 2)
    flip2 = chip + 2 - 4 * (chip // 2)
    flip3 = 3 - chip
    chips = (chip, flip1, flip2, flip3)
    my_rows = pl.ds(pl.multiple_of(64 * core + 16 * chip, 16), 16)

    def rows_of(c, q):
        return pl.ds(pl.multiple_of(64 * c + 16 * q, 16), 16)

    def remote(src, dst, ssem, rsem, dev):
        return pltpu.make_async_remote_copy(src_ref=src, dst_ref=dst, send_sem=ssem, recv_sem=rsem, device_id={"tp": dev}, device_id_type=pl.DeviceIdType.MESH)

    def local(src, dst, sem):
        return pltpu.make_async_copy(src, dst, sem)

    def ag_direct(ph, xg, r, p):
        cols = pl.ds(*GATHER[p])
        return remote(xg.at[my_rows, cols], xg.at[my_rows, cols], send_sem.at[ph, r, p], recv_sem.at[ph, r, p], 2 * chips[r] + core)

    def ag_direct_in(ph, xg, r, p):
        ref = xg.at[rows_of(core, chips[r]), pl.ds(*GATHER[p])]
        return remote(ref, ref, send_sem.at[ph, r, p], recv_sem.at[ph, r, p], 2 * chips[r] + core)

    def ag_forward(ph, xg, r, p):
        ref = xg.at[rows_of(core, chips[r]), pl.ds(*GATHER[p])]
        return remote(ref, ref, fsend_sem.at[ph, r, p], frecv_sem.at[ph, r, p], partner)

    def ag_forward_in(ph, xg, r, p):
        ref = xg.at[rows_of(other, chips[r]), pl.ds(*GATHER[p])]
        return remote(ref, ref, fsend_sem.at[ph, r, p], frecv_sem.at[ph, r, p], partner)

    def ag_start(ph, xg):
        for p in range(NA):
            for r in (3, 1, 2):
                ag_direct(ph, xg, r, p).start()
            ag_forward(ph, xg, 0, p).start()

    def ag_relay(ph, xg, p):
        for r in (1, 2, 3):
            ag_direct_in(ph, xg, r, p).wait_recv()
            ag_forward(ph, xg, r, p).start()

    def ag_arrive(ph, xg, p):
        for r in (0, 1, 2, 3):
            ag_forward_in(ph, xg, r, p).wait_recv()

    def ag_finish(ph, xg):
        for p in range(NA):
            for r in (1, 2, 3):
                ag_direct(ph, xg, r, p).wait_send()
            for r in (0, 1, 2, 3):
                ag_forward(ph, xg, r, p).wait_send()

    def rs_a(ph, n):
        cols = pl.ds(*SCATTER[n])
        return remote(pbuf.at[ph, pl.ds(pl.multiple_of(64 * other, 64), 64), cols], ra.at[ph, :, cols], asend_sem.at[ph, n], arecv_sem.at[ph, n], partner)

    def rs_b(ph, n, r):
        cols = pl.ds(*SCATTER[n])
        return remote(sb.at[ph, pl.ds(pl.multiple_of(16 * chips[r], 16), 16), cols], rb.at[ph, r - 1, :, cols], bsend_sem.at[ph, r, n], brecv_sem.at[ph, r, n], 2 * chips[r] + core)

    def rs_put(ph, n, part):
        pbuf[ph, :, pl.ds(*SCATTER[n])] = part.astype(BF16)
        rs_a(ph, n).start()

    def rs_first(n):
        return 1 + n % 2

    def rs_transit(ph, n):
        cols = pl.ds(*SCATTER[n])
        src = sb.at[ph, pl.ds(pl.multiple_of(16 * chips[3], 16), 16), cols]
        return remote(src, tb.at[ph, :, cols], bsend_sem.at[ph, 3, n], brecv_sem.at[ph, 3, n], 2 * chips[rs_first(n)] + core)

    def rs_pair(ph, n):
        cols = pl.ds(*SCATTER[n])
        rs_a(ph, n).wait_recv()
        own = pbuf[ph, pl.ds(pl.multiple_of(64 * core, 64), 64), cols].astype(F32)
        sb[ph, :, cols] = (own + ra[ph, :, cols].astype(F32)).astype(BF16)
        if n < VIA:
            rs_transit(ph, n).start()
            rs_b(ph, n, rs_first(n)).start()
        else:
            for r in (3, 1, 2):
                rs_b(ph, n, r).start()

    def rs_cross(ph, n):
        cols = pl.ds(*SCATTER[n])
        second = 3 - rs_first(n)
        rows = pl.ds(pl.multiple_of(16 * chips[second], 16), 16)
        rs_transit(ph, n).wait_recv()
        sb[ph, rows, cols] = (sb[ph, rows, cols].astype(F32) + tb[ph, :, cols].astype(F32)).astype(BF16)
        rs_b(ph, n, second).start()

    def rs_all(ph, product, group):
        for n in range(0, NR, group):
            part = product(n, pl.ds(SCATTER[n][0], group * CW))
            for k in range(group):
                rs_put(ph, n + k, part[:, k * CW:k * CW + CW])
            for k in range(n - LAG, n - LAG + group):
                if k >= 0:
                    rs_pair(ph, k)
        for n in range(NR - LAG, NR):
            rs_pair(ph, n)
        for n in range(VIA):
            rs_cross(ph, n)

    def rs_sum(ph, n):
        cols = pl.ds(*SCATTER[n])
        total = sb[ph, pl.ds(pl.multiple_of(16 * chip, 16), 16), cols].astype(F32)
        for r in (1, 2) if n < VIA else (1, 2, 3):
            rs_b(ph, n, r).wait_recv()
            total = total + rb[ph, r - 1, :, cols].astype(F32)
        return total

    def rs_finish(ph):
        for n in range(NR):
            rs_a(ph, n).wait_send()
            for r in (1, 2):
                rs_b(ph, n, r).wait_send()
            (rs_transit(ph, n) if n < VIA else rs_b(ph, n, 3)).wait_send()

    def normed(rows, gain):
        ms = jnp.zeros((16, 128), F32)
        for j in range(32):
            v = rows[:, 128 * j:128 * j + 128].astype(F32)
            ms = ms + v * v
        inv = lax.rsqrt(jnp.sum(ms, axis=-1, keepdims=True) * (1.0 / D) + NORM_EPS)
        return inv

    def store_normed(src, gain, dst):
        inv = normed(src, gain)
        for j in range(32):
            cols = slice(128 * j, 128 * j + 128)
            val = src[:, cols].astype(F32) * inv * gain[j:j + 1, :].astype(F32)
            dst[my_rows, cols] = val.astype(BF16)

    gate_loads = []
    for p in range(NA):
        rows = pl.ds(*GATHER[p])
        gate_loads.append(local(wg_hbm.at[rows, :], wg.at[rows, :], wsem.at[0, p]))
        gate_loads.append(local(wu_hbm.at[rows, :], wu.at[rows, :], wsem.at[1, p]))

    def attention_phase(kc, vc, vt, wo, freqv, qt, kch, vch, bias, o_buf):
        loads = {
            "x": local(x_hbm, xv, lsem.at[0]),
            "g1": local(g1_hbm, g1, lsem.at[1]),
            "freq": local(freq_hbm, freqv, lsem.at[6]),
            "vc": local(vc_hbm, vc, lsem.at[4]),
            "kc": local(kc_hbm, kc, lsem.at[5]),
            "wo": local(wo_hbm, wo, lsem.at[8]),
            "g2": local(g2_hbm, g2, lsem.at[9]),
            "start": local(start_hbm, start_ref, lsem.at[7]),
        }
        loads["x"].start()
        loads["g1"].start()
        barrier = pltpu.get_barrier_semaphore()
        for dev in (partner, 2 * flip1 + core, 2 * flip2 + core, 2 * flip3 + core):
            pl.semaphore_signal(barrier, inc=1, device_id={"tp": dev}, device_id_type=pl.DeviceIdType.MESH)
        tok_lane = token_of_row(lax.broadcasted_iota(jnp.int32, (1, 128), 1))

        def projection_phase(wq4, wqkv):
            wk_load = local(wk_hbm, wqkv.at[:, pl.ds(512, 128)], lsem.at[2])
            wv_load = local(wv_hbm, wqkv.at[:, pl.ds(640, 128)], lsem.at[3])
            wq_loads = [local(wq_hbm.at[pl.ds(p * 4 * CW, 4 * CW), :], wq4.at[pl.ds(p * 4 * CW, 4 * CW), :], dsem.at[p]) for p in range(NP)]
            for ld in wq_loads:
                ld.start()
            loads["vc"].start()
            loads["freq"].start()
            loads["start"].start()
            wk_load.start()
            wv_load.start()
            for name in ("kc", "wo", "g2"):
                loads[name].start()

            loads["x"].wait()
            loads["g1"].wait()
            store_normed(xv, g1, xg1)
            pl.semaphore_wait(barrier, 4)
            ag_start(0, xg1)

            ri = lax.broadcasted_iota(jnp.int32, (256, 256), 0)
            ci = lax.broadcasted_iota(jnp.int32, (256, 256), 1)
            perm = (ci == 4 * (ri % 64) + ri // 64).astype(F32).astype(BF16)

            def split_heads(p):
                wq_loads[p].wait()

                def body(i, carry):
                    base = p * (CW // 64) + 2 * i
                    rows4 = jnp.concatenate([wq4[pl.ds(pl.multiple_of((base + k) * 256, 256), 256), :] for k in range(2)], axis=1)
                    out = jnp.dot(perm, rows4, preferred_element_type=F32).astype(BF16)
                    for k in range(2):
                        for h in range(4):
                            wqkv[pl.ds(pl.multiple_of((base + k) * 64, 64), 64), h * 128:h * 128 + 128] = out[64 * h:64 * h + 64, k * 128:k * 128 + 128]
                    return carry

                for i in range(CW // 128):
                    body(i, 0)

            loads["vc"].wait()

            def flip_values(i, carry):
                ks = pl.ds(pl.multiple_of(i * KB, KB), KB)
                vt[:, ks] = vc[ks, :].astype(F32).T.astype(BF16)
                slot = i * KB + lax.broadcasted_iota(jnp.int32, (KB, 128), 0)
                off = jnp.bitwise_and(slot - start, W - 1)
                keep = jnp.where(off >= W - start, off, -1) > tok_lane
                bias[ks, :] = jnp.where(keep, 0.0, -jnp.inf)
                return carry

            loads["start"].wait()
            start = start_ref[0:1, :]
            for p in range(4):
                split_heads(p)
            for p in range(6):
                flip_values(p, 0)
            loads["freq"].wait()
            tok_row = token_of_row(lax.broadcasted_iota(jnp.int32, (T, 128), 0))
            angles = (start + tok_row).astype(F32) * freqv[0:1, :]
            cos_t = jnp.cos(angles)
            lane = lax.broadcasted_iota(jnp.int32, (T, 128), 1)
            even = lane % 2 == 0
            sin_t = jnp.sin(angles)
            sin_t = jnp.where(even, -sin_t, sin_t)
            wk_load.wait()
            wv_load.wait()
            acc = jnp.zeros((T, 768), F32)
            ag_relay(0, xg1, 0)
            ag_relay(0, xg1, 1)
            for p in range(NA):
                if p + 2 < NA:
                    ag_relay(0, xg1, p + 2)
                if p + 4 < NP:
                    split_heads(p + 4)
                if p < 2:
                    flip_values(p + 6, 0)
                ag_arrive(0, xg1, p)
                cols = pl.ds(*GATHER[p])
                acc = acc + jnp.dot(xg1[:, cols], wqkv[cols, :], preferred_element_type=F32)
            for ld in gate_loads:
                ld.start()

            def rotate(v):
                swapped = jnp.where(even, pltpu.roll(v, 127, 1), pltpu.roll(v, 1, 1))
                return v * cos_t + swapped * sin_t

            for h in range(4):
                qt[:, h * 128:h * 128 + 128] = rotate(acc[:, h * 128:h * 128 + 128]).T.astype(BF16)
            kch[...] = rotate(acc[:, 512:640]).astype(BF16)
            v_new = acc[:, 640:768].astype(BF16)
            vch[...] = v_new
            vt[:, W:W + T] = v_new.astype(F32).T.astype(BF16)

        pl.run_scoped(
            projection_phase,
            pltpu.VMEM((4 * D, 128), BF16),
            pltpu.VMEM((D, 768), BF16),
        )
        loads["kc"].wait()
        factor = (128.0 ** -0.5) * 1.4426950408889634

        def softmax_phase(e_buf):
            queries = qt[...]
            tops, masses = [], []
            for b in range(NKB + 1):
                keys = kc[b * KB:b * KB + KB, :] if b < NKB else kch[...]
                scores = jnp.dot(keys, queries, preferred_element_type=F32)
                for i in range(KB // 128 if b < NKB else 1):
                    ks = slice(b * KB + i * 128, b * KB + i * 128 + 128)
                    if b < NKB:
                        shift = bias[ks, :]
                    else:
                        shift = jnp.where(token_of_row(lax.broadcasted_iota(jnp.int32, (T, 128), 0)) <= tok_lane, 0.0, -jnp.inf)
                    top, mass = [], []
                    for g in range(4):
                        gs = slice(g * 128, g * 128 + 128)
                        part = (scores[i * 128:i * 128 + 128, gs] + shift).reshape(16, 8, 128)
                        t = jnp.maximum(jnp.max(part, axis=0), jnp.finfo(F32).min)
                        e = jnp.exp2((part - t[None]) * factor)
                        e_buf[ks, gs] = e.reshape(128, 128)
                        mass.append(jnp.sum(e, axis=0))
                        top.append(t)
                    tops.append(top)
                    masses.append(mass)
            blocks = len(tops)
            weights = []
            for g in range(4):
                best = jnp.max(functools.reduce(jnp.maximum, [tops[b][g] for b in range(blocks)]), axis=0, keepdims=True)
                scales = [jnp.exp2((tops[b][g] - best) * factor) for b in range(blocks)]
                total = functools.reduce(jnp.add, [masses[b][g] * scales[b] for b in range(blocks)])
                inv = 1.0 / jnp.sum(total, axis=0, keepdims=True)
                weights.append([sc * inv for sc in scales])
            out = None
            for b in range(NKB + 1):
                n = KB if b < NKB else T
                ks = slice(b * KB, b * KB + n)
                rows = []
                for i in range(n // 128):
                    r0 = b * KB + i * 128
                    cols = [(e_buf[r0:r0 + 128, g * 128:g * 128 + 128].reshape(16, 8, 128) * weights[g][b * (KB // 128) + i][None]).reshape(128, 128) for g in range(4)]
                    rows.append(jnp.concatenate(cols, axis=1))
                probs = jnp.concatenate(rows, axis=0).astype(BF16)
                part = jnp.dot(vt[:, ks], probs, preferred_element_type=F32)
                out = part if out is None else out + part
            for g in range(4):
                o_buf[:, g * 128:g * 128 + 128] = out[:, g * 128:g * 128 + 128].T.astype(BF16)

        pl.run_scoped(softmax_phase, pltpu.VMEM((W + T, 512), F32))
        loads["wo"].wait()
        rs_all(0, lambda n, cols: jnp.dot(o_buf[...], wo[:, cols], preferred_element_type=F32), 2)
        loads["g2"].wait()

        chunk = jnp.concatenate([kch[...], vch[...]], axis=1)

        def merge(i, carry):
            ks = pl.ds(pl.multiple_of(i * KB, KB), KB)
            slot = i * KB + lax.broadcasted_iota(jnp.int32, (KB, 128), 0)
            off = jnp.bitwise_and(slot - start, W - 1)
            pick = (off == tok_lane).astype(F32).astype(BF16)
            placed = jnp.dot(pick, chunk, preferred_element_type=F32)
            fresh = off < T
            kn_ref[ks, :] = jnp.where(fresh, placed[:, 0:128], kc[ks, :].astype(F32)).astype(BF16)
            vn_ref[ks, :] = jnp.where(fresh, placed[:, 128:256], vc[ks, :].astype(F32)).astype(BF16)
            return carry

        start = start_ref[0:1, :]
        lax.fori_loop(0, NKB, merge, 0)

    pl.run_scoped(
        attention_phase,
        pltpu.VMEM((W, 128), BF16),
        pltpu.VMEM((W, 128), BF16),
        pltpu.VMEM((128, W + T), BF16),
        pltpu.VMEM((512, D), BF16),
        pltpu.VMEM((8, 128), F32),
        pltpu.VMEM((128, 512), BF16),
        pltpu.VMEM((T, 128), BF16),
        pltpu.VMEM((T, 128), BF16),
        pltpu.VMEM((W, 128), F32),
        pltpu.VMEM((T, 512), BF16),
    )

    def mlp_phase(wd, acc_g, acc_u, u_buf):
        down_loads = [local(wd_hbm.at[:, pl.ds(n * CW, CW)], wd.at[:, pl.ds(n * CW, CW)], dsem.at[n]) for n in range(NP)]
        for ld in down_loads:
            ld.start()
        for n in range(NR):
            cols = pl.ds(*SCATTER[n])
            hb[:, cols] = (xv[:, cols].astype(F32) + rs_sum(0, n)).astype(BF16)
        store_normed(hb, g2, xg2)
        ag_start(1, xg2)
        ag_finish(0, xg1)
        rs_finish(0)
        ag_relay(1, xg2, 0)
        ag_relay(1, xg2, 1)
        for p in range(NA):
            if p + 2 < NA:
                ag_relay(1, xg2, p + 2)
            gate_loads[2 * p].wait()
            gate_loads[2 * p + 1].wait()
            ag_arrive(1, xg2, p)
            rows = pl.ds(*GATHER[p])
            m = xg2[:, rows]
            gate = jnp.dot(m, wg[rows, :], preferred_element_type=F32)
            up = jnp.dot(m, wu[rows, :], preferred_element_type=F32)
            if p == 0:
                acc_g[...] = gate
                acc_u[...] = up
            elif p + 1 < NA:
                acc_g[...] += gate
                acc_u[...] += up
            else:
                gate = acc_g[...] + gate
                u_buf[...] = (gate / (1.0 + jnp.exp(-gate)) * (acc_u[...] + up)).astype(BF16)
        def down(n, cols):
            down_loads[n].wait()
            return jnp.dot(u_buf[...], wd[:, cols], preferred_element_type=F32)

        rs_all(1, down, 1)
        ag_finish(1, xg2)
        for n in range(NR):
            cols = pl.ds(*SCATTER[n])
            xo_ref[:, cols] = (hb[:, cols].astype(F32) + rs_sum(1, n)).astype(BF16)
        rs_finish(1)

    pl.run_scoped(
        mlp_phase,
        pltpu.VMEM((FF, D), BF16),
        pltpu.VMEM((T, FF), F32),
        pltpu.VMEM((T, FF), F32),
        pltpu.VMEM((T, FF), BF16),
    )


def write_kernel(x_ref, k_ref, v_ref, xo_hbm, ko_hbm, vo_hbm, sem):
    copies = [pltpu.make_async_copy(src, dst, sem.at[i]) for i, (src, dst) in enumerate(((k_ref, ko_hbm), (v_ref, vo_hbm), (x_ref, xo_hbm)))]
    for copy in copies:
        copy.start()
    for copy in copies:
        copy.wait()


def solution(mesh):
    row_spec = P('dp', 'tp', None)
    cache_spec = P('dp', None, 'tp', None)
    head_cols = P(None, 'tp', None)
    in_specs = (row_spec, P('dp'), cache_spec, cache_spec, P(), head_cols, head_cols, head_cols, P('tp', None, None), P(), P(None, 'tp'), P(None, 'tp'), P('tp', None))
    out_specs = (row_spec, cache_spec, cache_spec)

    def local_layer(x_in, start_pos, k_cache, v_cache, attn_gain, w_query, w_key, w_value, w_out, mlp_gain, w_gate, w_up, w_down):
        freq = np.repeat(ROPE_BASE ** (-np.arange(0, 128, 2) / 128.0), 2).astype(np.float32)
        freq = jnp.asarray(np.tile(freq[None, :], (8, 1)))
        any_spec = pl.BlockSpec(memory_space=pl.ANY)
        vmem_spec = pl.BlockSpec(memory_space=pltpu.VMEM)
        dma = pltpu.SemaphoreType.DMA
        kc2 = k_cache.reshape(W, 128)
        vc2 = v_cache.reshape(W, 128)
        results = pl.pallas_call(
            layer_kernel,
            out_shape=(pltpu.VMEM((16, D), BF16), pltpu.VMEM((W, 128), BF16), pltpu.VMEM((W, 128), BF16)),
            in_specs=[any_spec] * 14,
            out_specs=(vmem_spec, vmem_spec, vmem_spec),
            scratch_shapes=[
                pltpu.VMEM((8, 128), jnp.int32),
                pltpu.VMEM((16, D), BF16),
                pltpu.VMEM((32, 128), BF16),
                pltpu.VMEM((32, 128), BF16),
                pltpu.VMEM((D, FF), BF16),
                pltpu.VMEM((D, FF), BF16),
                pltpu.VMEM((T, D), BF16),
                pltpu.VMEM((T, D), BF16),
                pltpu.VMEM((2, T, D), BF16),
                pltpu.VMEM((2, 64, D), BF16),
                pltpu.VMEM((2, 64, D), BF16),
                pltpu.VMEM((2, 3, 16, D), BF16),
                pltpu.VMEM((2, 16, VIA * CW), BF16),
                pltpu.VMEM((16, D), BF16),
                dma((10,)),
                dma((2, NA)),
                dma((NP,)),
                dma((2, 4, NA)),
                dma((2, 4, NA)),
                dma((2, 4, NA)),
                dma((2, 4, NA)),
                dma((2, NR)),
                dma((2, NR)),
                dma((2, 4, NR)),
                dma((2, 4, NR)),
            ],
            compiler_params=pltpu.CompilerParams(collective_id=0, has_side_effects=True, vmem_limit_bytes=VMEM_LIMIT),
            name="layer",
        )(
            jnp.broadcast_to(start_pos[:, None], (8, 128)), x_in.reshape(16, D), freq, kc2, vc2, attn_gain.reshape(32, 128), w_query.reshape(4 * D, 128),
            w_key.reshape(D, 128), w_value.reshape(D, 128), w_out.reshape(512, D), mlp_gain.reshape(32, 128), w_gate, w_up, w_down,
        )
        x_out, k_new, v_new = pl.pallas_call(
            write_kernel,
            out_shape=(jax.ShapeDtypeStruct((16, D), BF16), jax.ShapeDtypeStruct((W, 128), BF16), jax.ShapeDtypeStruct((W, 128), BF16)),
            in_specs=[vmem_spec] * 3,
            out_specs=(pl.BlockSpec(memory_space=pltpu.HBM),) * 3,
            scratch_shapes=[dma((3,))],
            compiler_params=pltpu.CompilerParams(vmem_limit_bytes=1 << 20),
            name="write",
        )(*[pltpu.with_memory_space_constraint(r, pltpu.VMEM) for r in results])
        return x_out.reshape(x_in.shape), k_new.reshape(k_cache.shape), v_new.reshape(v_cache.shape)

    return jax.shard_map(local_layer, mesh=mesh, in_specs=in_specs, out_specs=out_specs, check_vma=False)
```

```python
import functools

import jax
import numpy as np
import jax.numpy as jnp
from jax import lax
from jax.experimental import pallas as pl
from jax.experimental.pallas import tpu as pltpu
from jax.sharding import PartitionSpec as P

ROPE_BASE = 10000.0
NORM_EPS = 1e-5
BF16 = jnp.bfloat16
F32 = jnp.float32
D = 4096
T = 128
FF = 1792
W = 4096
NP = 8
CW = D // NP
GATHER = [(512 * p, 512) for p in range(7)] + [(3584, 256), (3840, 256)]
SCATTER = [(512 * p, 512) for p in range(8)]
NA = len(GATHER)
HAND = (6, 7, 8)
NR = len(SCATTER)
LAG = 2
VIA = 6
VMEM_LIMIT = 64000000
KB = 512
NKB = W // KB


def token_of_row(row):
    core = row // 64
    chip = (row // 16) % 4
    return 32 * chip + 16 * core + row % 16


def layer_kernel(start_hbm, x_hbm, freq_hbm, kc_hbm, vc_hbm, g1_hbm, wq_hbm, wk_hbm, wv_hbm, wo_hbm, g2_hbm, wg_hbm, wu_hbm, wd_hbm,
                 xo_ref, kn_ref, vn_ref,
                 start_ref, xv, g1, g2, wg, wu, xg1, xg2, pbuf, ra, sb, rb, tb, hb,
                 lsem, wsem, dsem, send_sem, recv_sem, fsend_sem, frecv_sem, asend_sem, arecv_sem, bsend_sem, brecv_sem, hsend_sem, hrecv_sem, gsend_sem, grecv_sem):
    me = lax.axis_index("tp")
    core = me % 2
    chip = me // 2
    other = 1 - core
    partner = 2 * chip + other
    flip1 = chip + 1 - 2 * (chip % 2)
    flip2 = chip + 2 - 4 * (chip // 2)
    flip3 = 3 - chip
    chips = (chip, flip1, flip2, flip3)
    my_rows = pl.ds(pl.multiple_of(64 * core + 16 * chip, 16), 16)

    def rows_of(c, q):
        return pl.ds(pl.multiple_of(64 * c + 16 * q, 16), 16)

    def remote(src, dst, ssem, rsem, dev):
        return pltpu.make_async_remote_copy(src_ref=src, dst_ref=dst, send_sem=ssem, recv_sem=rsem, device_id={"tp": dev}, device_id_type=pl.DeviceIdType.MESH)

    def local(src, dst, sem):
        return pltpu.make_async_copy(src, dst, sem)

    def piece(xg, c, r, p):
        return xg.at[rows_of(c, chips[r]), pl.ds(*GATHER[p])]

    def ag_direct(ph, xg, r, p):
        ref = piece(xg, core, 0, p)
        return remote(ref, ref, send_sem.at[ph, r, p], recv_sem.at[ph, r, p], 2 * chips[r] + core)

    def ag_direct_in(ph, xg, r, p):
        ref = piece(xg, core, r, p)
        return remote(ref, ref, send_sem.at[ph, r, p], recv_sem.at[ph, r, p], 2 * chips[r] + core)

    def ag_forward(ph, xg, r, p):
        ref = piece(xg, core, r, p)
        return remote(ref, ref, fsend_sem.at[ph, r, p], frecv_sem.at[ph, r, p], partner)

    def ag_forward_in(ph, xg, r, p):
        ref = piece(xg, other, r, p)
        return remote(ref, ref, fsend_sem.at[ph, r, p], frecv_sem.at[ph, r, p], partner)

    def ag_hand(ph, xg, r, p):
        ref = piece(xg, 0, 0, p)
        return remote(ref, ref, hsend_sem.at[ph, r, p - HAND[0]], hrecv_sem.at[ph, r, p - HAND[0]], 2 * chips[r] + 1)

    def ag_hand_in(ph, xg, r, p):
        ref = piece(xg, 0, r, p)
        return remote(ref, ref, hsend_sem.at[ph, r, p - HAND[0]], hrecv_sem.at[ph, r, p - HAND[0]], 2 * chips[r] + 1)

    def ag_hand_forward(ph, xg, r, p):
        ref = piece(xg, 0, r, p)
        return remote(ref, ref, gsend_sem.at[ph, r, p - HAND[0]], grecv_sem.at[ph, r, p - HAND[0]], partner)

    def on_core(c):
        return pl.when(core == c)

    def ag_start(ph, xg):
        for p in range(NA):
            ag_forward(ph, xg, 0, p).start()
            if p not in HAND:
                for r in (3, 1, 2):
                    ag_direct(ph, xg, r, p).start()

    def ag_start_last(ph, xg):
        @on_core(1)
        def _():
            for p in HAND:
                for r in (3, 1, 2):
                    ag_direct(ph, xg, r, p).start()
                ag_forward_in(ph, xg, 0, p).wait_recv()
                for r in (3, 1, 2):
                    ag_hand(ph, xg, r, p).start()

    def ag_relay(ph, xg, p):
        def pass_on():
            for r in (1, 2, 3):
                ag_direct_in(ph, xg, r, p).wait_recv()
                ag_forward(ph, xg, r, p).start()

        if p not in HAND:
            pass_on()
        else:
            @on_core(1)
            def _():
                pass_on()
                for r in (1, 2, 3):
                    ag_hand_in(ph, xg, r, p).wait_recv()
                    ag_hand_forward(ph, xg, r, p).start()

    def ag_arrive(ph, xg, p):
        def wait_all():
            for r in (0, 1, 2, 3):
                ag_forward_in(ph, xg, r, p).wait_recv()

        if p not in HAND:
            wait_all()
        else:
            @on_core(0)
            def _():
                wait_all()
                for r in (1, 2, 3):
                    ag_hand_forward(ph, xg, r, p).wait_recv()

    def ag_finish(ph, xg):
        for p in range(NA):
            ag_forward(ph, xg, 0, p).wait_send()
            if p not in HAND:
                for r in (1, 2, 3):
                    ag_direct(ph, xg, r, p).wait_send()
                    ag_forward(ph, xg, r, p).wait_send()

        @on_core(1)
        def _():
            for p in HAND:
                for r in (1, 2, 3):
                    ag_direct(ph, xg, r, p).wait_send()
                    ag_forward(ph, xg, r, p).wait_send()
                    ag_hand(ph, xg, r, p).wait_send()
                    ag_hand_forward(ph, xg, r, p).wait_send()

    def rs_a(ph, n):
        cols = pl.ds(*SCATTER[n])
        return remote(pbuf.at[ph, pl.ds(pl.multiple_of(64 * other, 64), 64), cols], ra.at[ph, :, cols], asend_sem.at[ph, n], arecv_sem.at[ph, n], partner)

    def rs_b(ph, n, r):
        cols = pl.ds(*SCATTER[n])
        return remote(sb.at[ph, pl.ds(pl.multiple_of(16 * chips[r], 16), 16), cols], rb.at[ph, r - 1, :, cols], bsend_sem.at[ph, r, n], brecv_sem.at[ph, r, n], 2 * chips[r] + core)

    def rs_put(ph, n, part):
        pbuf[ph, :, pl.ds(*SCATTER[n])] = part.astype(BF16)
        rs_a(ph, n).start()

    def rs_first(n):
        return 1 + n % 2

    def rs_transit(ph, n):
        cols = pl.ds(*SCATTER[n])
        src = sb.at[ph, pl.ds(pl.multiple_of(16 * chips[3], 16), 16), cols]
        return remote(src, tb.at[ph, :, cols], bsend_sem.at[ph, 3, n], brecv_sem.at[ph, 3, n], 2 * chips[rs_first(n)] + core)

    def rs_pair(ph, n):
        cols = pl.ds(*SCATTER[n])
        rs_a(ph, n).wait_recv()
        own = pbuf[ph, pl.ds(pl.multiple_of(64 * core, 64), 64), cols].astype(F32)
        sb[ph, :, cols] = (own + ra[ph, :, cols].astype(F32)).astype(BF16)
        if n < VIA:
            rs_transit(ph, n).start()
            rs_b(ph, n, rs_first(n)).start()
        else:
            for r in (3, 1, 2):
                rs_b(ph, n, r).start()

    def rs_cross(ph, n):
        cols = pl.ds(*SCATTER[n])
        second = 3 - rs_first(n)
        rows = pl.ds(pl.multiple_of(16 * chips[second], 16), 16)
        rs_transit(ph, n).wait_recv()
        sb[ph, rows, cols] = (sb[ph, rows, cols].astype(F32) + tb[ph, :, cols].astype(F32)).astype(BF16)
        rs_b(ph, n, second).start()

    def rs_all(ph, product, group):
        for n in range(0, NR, group):
            part = product(n, pl.ds(SCATTER[n][0], group * CW))
            for k in range(group):
                rs_put(ph, n + k, part[:, k * CW:k * CW + CW])
            for k in range(n - LAG, n - LAG + group):
                if k >= 0:
                    rs_pair(ph, k)
        for n in range(NR - LAG, NR):
            rs_pair(ph, n)
        for n in range(VIA):
            rs_cross(ph, n)

    def rs_sum(ph, n):
        cols = pl.ds(*SCATTER[n])
        total = sb[ph, pl.ds(pl.multiple_of(16 * chip, 16), 16), cols].astype(F32)
        for r in (1, 2) if n < VIA else (1, 2, 3):
            rs_b(ph, n, r).wait_recv()
            total = total + rb[ph, r - 1, :, cols].astype(F32)
        return total

    def rs_finish(ph):
        for n in range(NR):
            rs_a(ph, n).wait_send()
            for r in (1, 2):
                rs_b(ph, n, r).wait_send()
            (rs_transit(ph, n) if n < VIA else rs_b(ph, n, 3)).wait_send()

    def normed(rows, gain):
        ms = jnp.zeros((16, 128), F32)
        for j in range(32):
            v = rows[:, 128 * j:128 * j + 128].astype(F32)
            ms = ms + v * v
        inv = lax.rsqrt(jnp.sum(ms, axis=-1, keepdims=True) * (1.0 / D) + NORM_EPS)
        return inv

    def store_normed(src, gain, dst):
        inv = normed(src, gain)
        for j in range(32):
            cols = slice(128 * j, 128 * j + 128)
            val = src[:, cols].astype(F32) * inv * gain[j:j + 1, :].astype(F32)
            dst[my_rows, cols] = val.astype(BF16)

    gate_loads = []
    for p in range(NA):
        rows = pl.ds(*GATHER[p])
        gate_loads.append(local(wg_hbm.at[rows, :], wg.at[rows, :], wsem.at[0, p]))
        gate_loads.append(local(wu_hbm.at[rows, :], wu.at[rows, :], wsem.at[1, p]))

    def attention_phase(kc, vc, vt, wo, freqv, qt, kch, vch, bias, o_buf):
        loads = {
            "x": local(x_hbm, xv, lsem.at[0]),
            "g1": local(g1_hbm, g1, lsem.at[1]),
            "freq": local(freq_hbm, freqv, lsem.at[6]),
            "vc": local(vc_hbm, vc, lsem.at[4]),
            "kc": local(kc_hbm, kc, lsem.at[5]),
            "wo": local(wo_hbm, wo, lsem.at[8]),
            "g2": local(g2_hbm, g2, lsem.at[9]),
            "start": local(start_hbm, start_ref, lsem.at[7]),
        }
        loads["x"].start()
        loads["g1"].start()
        barrier = pltpu.get_barrier_semaphore()
        for dev in (partner, 2 * flip1 + core, 2 * flip2 + core, 2 * flip3 + core):
            pl.semaphore_signal(barrier, inc=1, device_id={"tp": dev}, device_id_type=pl.DeviceIdType.MESH)
        tok_lane = token_of_row(lax.broadcasted_iota(jnp.int32, (1, 128), 1))

        def projection_phase(wq4, wqkv):
            wk_load = local(wk_hbm, wqkv.at[:, pl.ds(512, 128)], lsem.at[2])
            wv_load = local(wv_hbm, wqkv.at[:, pl.ds(640, 128)], lsem.at[3])
            wq_loads = [local(wq_hbm.at[pl.ds(p * 4 * CW, 4 * CW), :], wq4.at[pl.ds(p * 4 * CW, 4 * CW), :], dsem.at[p]) for p in range(NP)]
            for ld in wq_loads:
                ld.start()
            loads["vc"].start()
            loads["freq"].start()
            loads["start"].start()
            wk_load.start()
            wv_load.start()
            for name in ("kc", "wo", "g2"):
                loads[name].start()

            loads["x"].wait()
            loads["g1"].wait()
            store_normed(xv, g1, xg1)
            pl.semaphore_wait(barrier, 4)
            ag_start(0, xg1)

            ri = lax.broadcasted_iota(jnp.int32, (256, 256), 0)
            ci = lax.broadcasted_iota(jnp.int32, (256, 256), 1)
            perm = (ci == 4 * (ri % 64) + ri // 64).astype(F32).astype(BF16)

            def split_heads(p):
                wq_loads[p].wait()

                def body(i, carry):
                    base = p * (CW // 64) + 2 * i
                    rows4 = jnp.concatenate([wq4[pl.ds(pl.multiple_of((base + k) * 256, 256), 256), :] for k in range(2)], axis=1)
                    out = jnp.dot(perm, rows4, preferred_element_type=F32).astype(BF16)
                    for k in range(2):
                        for h in range(4):
                            wqkv[pl.ds(pl.multiple_of((base + k) * 64, 64), 64), h * 128:h * 128 + 128] = out[64 * h:64 * h + 64, k * 128:k * 128 + 128]
                    return carry

                for i in range(CW // 128):
                    body(i, 0)

            loads["vc"].wait()

            def flip_values(i, carry):
                ks = pl.ds(pl.multiple_of(i * KB, KB), KB)
                vt[:, ks] = vc[ks, :].astype(F32).T.astype(BF16)
                slot = i * KB + lax.broadcasted_iota(jnp.int32, (KB, 128), 0)
                off = jnp.bitwise_and(slot - start, W - 1)
                keep = jnp.where(off >= W - start, off, -1) > tok_lane
                bias[ks, :] = jnp.where(keep, 0.0, -jnp.inf)
                return carry

            loads["start"].wait()
            start = start_ref[0]
            for p in range(4):
                split_heads(p)
            for p in range(6):
                flip_values(p, 0)
            loads["freq"].wait()
            tok_row = token_of_row(lax.broadcasted_iota(jnp.int32, (T, 128), 0))
            angles = (start + tok_row).astype(F32) * freqv[0:1, :]
            cos_t = jnp.cos(angles)
            lane = lax.broadcasted_iota(jnp.int32, (T, 128), 1)
            even = lane % 2 == 0
            sin_t = jnp.sin(angles)
            sin_t = jnp.where(even, -sin_t, sin_t)
            wk_load.wait()
            wv_load.wait()
            acc = jnp.zeros((T, 768), F32)
            ag_start_last(0, xg1)
            ag_relay(0, xg1, 0)
            ag_relay(0, xg1, 1)
            for p in range(NA):
                if p + 2 < NA:
                    ag_relay(0, xg1, p + 2)
                if p + 4 < NP:
                    split_heads(p + 4)
                if p < 2:
                    flip_values(p + 6, 0)
                ag_arrive(0, xg1, p)
                cols = pl.ds(*GATHER[p])
                acc = acc + jnp.dot(xg1[:, cols], wqkv[cols, :], preferred_element_type=F32)
            for ld in gate_loads:
                ld.start()

            def rotate(v):
                swapped = jnp.where(even, pltpu.roll(v, 127, 1), pltpu.roll(v, 1, 1))
                return v * cos_t + swapped * sin_t

            for h in range(4):
                qt[:, h * 128:h * 128 + 128] = rotate(acc[:, h * 128:h * 128 + 128]).T.astype(BF16)
            kch[...] = rotate(acc[:, 512:640]).astype(BF16)
            v_new = acc[:, 640:768].astype(BF16)
            vch[...] = v_new
            vt[:, W:W + T] = v_new.astype(F32).T.astype(BF16)

        pl.run_scoped(
            projection_phase,
            pltpu.VMEM((4 * D, 128), BF16),
            pltpu.VMEM((D, 768), BF16),
        )
        loads["kc"].wait()
        factor = (128.0 ** -0.5) * 1.4426950408889634

        def softmax_phase(e_buf):
            queries = qt[...]
            tops, masses = [], []
            for b in range(NKB + 1):
                keys = kc[b * KB:b * KB + KB, :] if b < NKB else kch[...]
                scores = jnp.dot(keys, queries, preferred_element_type=F32)
                for i in range(KB // 128 if b < NKB else 1):
                    ks = slice(b * KB + i * 128, b * KB + i * 128 + 128)
                    if b < NKB:
                        shift = bias[ks, :]
                    else:
                        shift = jnp.where(token_of_row(lax.broadcasted_iota(jnp.int32, (T, 128), 0)) <= tok_lane, 0.0, -jnp.inf)
                    top, mass = [], []
                    for g in range(4):
                        gs = slice(g * 128, g * 128 + 128)
                        part = (scores[i * 128:i * 128 + 128, gs] + shift).reshape(16, 8, 128)
                        t = jnp.maximum(jnp.max(part, axis=0), jnp.finfo(F32).min)
                        e = jnp.exp2((part - t[None]) * factor)
                        e_buf[ks, gs] = e.reshape(128, 128)
                        mass.append(jnp.sum(e, axis=0))
                        top.append(t)
                    tops.append(top)
                    masses.append(mass)
            blocks = len(tops)
            weights = []
            for g in range(4):
                best = jnp.max(functools.reduce(jnp.maximum, [tops[b][g] for b in range(blocks)]), axis=0, keepdims=True)
                scales = [jnp.exp2((tops[b][g] - best) * factor) for b in range(blocks)]
                total = functools.reduce(jnp.add, [masses[b][g] * scales[b] for b in range(blocks)])
                inv = 1.0 / jnp.sum(total, axis=0, keepdims=True)
                weights.append([sc * inv for sc in scales])
            out = None
            for b in range(NKB + 1):
                n = KB if b < NKB else T
                ks = slice(b * KB, b * KB + n)
                rows = []
                for i in range(n // 128):
                    r0 = b * KB + i * 128
                    cols = [(e_buf[r0:r0 + 128, g * 128:g * 128 + 128].reshape(16, 8, 128) * weights[g][b * (KB // 128) + i][None]).reshape(128, 128) for g in range(4)]
                    rows.append(jnp.concatenate(cols, axis=1))
                probs = jnp.concatenate(rows, axis=0).astype(BF16)
                part = jnp.dot(vt[:, ks], probs, preferred_element_type=F32)
                out = part if out is None else out + part
            for g in range(4):
                o_buf[:, g * 128:g * 128 + 128] = out[:, g * 128:g * 128 + 128].T.astype(BF16)

        pl.run_scoped(softmax_phase, pltpu.VMEM((W + T, 512), F32))
        loads["wo"].wait()
        rs_all(0, lambda n, cols: jnp.dot(o_buf[...], wo[:, cols], preferred_element_type=F32), 2)
        loads["g2"].wait()

        chunk = jnp.concatenate([kch[...], vch[...]], axis=1)

        def merge(i, carry):
            ks = pl.ds(pl.multiple_of(i * KB, KB), KB)
            slot = i * KB + lax.broadcasted_iota(jnp.int32, (KB, 128), 0)
            off = jnp.bitwise_and(slot - start, W - 1)
            pick = (off == tok_lane).astype(F32).astype(BF16)
            placed = jnp.dot(pick, chunk, preferred_element_type=F32)
            fresh = off < T
            kn_ref[ks, :] = jnp.where(fresh, placed[:, 0:128], kc[ks, :].astype(F32)).astype(BF16)
            vn_ref[ks, :] = jnp.where(fresh, placed[:, 128:256], vc[ks, :].astype(F32)).astype(BF16)
            return carry

        start = start_ref[0]
        lax.fori_loop(0, NKB, merge, 0)

    pl.run_scoped(
        attention_phase,
        pltpu.VMEM((W, 128), BF16),
        pltpu.VMEM((W, 128), BF16),
        pltpu.VMEM((128, W + T), BF16),
        pltpu.VMEM((512, D), BF16),
        pltpu.VMEM((8, 128), F32),
        pltpu.VMEM((128, 512), BF16),
        pltpu.VMEM((T, 128), BF16),
        pltpu.VMEM((T, 128), BF16),
        pltpu.VMEM((W, 128), F32),
        pltpu.VMEM((T, 512), BF16),
    )

    def mlp_phase(wd, acc_g, acc_u, u_buf):
        down_loads = [local(wd_hbm.at[:, pl.ds(n * CW, CW)], wd.at[:, pl.ds(n * CW, CW)], dsem.at[n]) for n in range(NP)]
        for ld in down_loads:
            ld.start()
        for n in range(NR):
            cols = pl.ds(*SCATTER[n])
            hb[:, cols] = (xv[:, cols].astype(F32) + rs_sum(0, n)).astype(BF16)
        store_normed(hb, g2, xg2)
        ag_start(1, xg2)
        ag_finish(0, xg1)
        rs_finish(0)
        ag_start_last(1, xg2)
        ag_relay(1, xg2, 0)
        ag_relay(1, xg2, 1)
        for p in range(NA):
            if p + 2 < NA:
                ag_relay(1, xg2, p + 2)
            gate_loads[2 * p].wait()
            gate_loads[2 * p + 1].wait()
            ag_arrive(1, xg2, p)
            rows = pl.ds(*GATHER[p])
            m = xg2[:, rows]
            gate = jnp.dot(m, wg[rows, :], preferred_element_type=F32)
            up = jnp.dot(m, wu[rows, :], preferred_element_type=F32)
            if p == 0:
                acc_g[...] = gate
                acc_u[...] = up
            elif p + 1 < NA:
                acc_g[...] += gate
                acc_u[...] += up
            else:
                gate = acc_g[...] + gate
                u_buf[...] = (gate / (1.0 + jnp.exp(-gate)) * (acc_u[...] + up)).astype(BF16)
        def down(n, cols):
            down_loads[n].wait()
            return jnp.dot(u_buf[...], wd[:, cols], preferred_element_type=F32)

        rs_all(1, down, 1)
        ag_finish(1, xg2)
        for n in range(NR):
            cols = pl.ds(*SCATTER[n])
            xo_ref[:, cols] = (hb[:, cols].astype(F32) + rs_sum(1, n)).astype(BF16)
        rs_finish(1)

    pl.run_scoped(
        mlp_phase,
        pltpu.VMEM((FF, D), BF16),
        pltpu.VMEM((T, FF), F32),
        pltpu.VMEM((T, FF), F32),
        pltpu.VMEM((T, FF), BF16),
    )


def write_kernel(x_ref, k_ref, v_ref, xo_hbm, ko_hbm, vo_hbm, sem):
    copies = [pltpu.make_async_copy(src, dst, sem.at[i]) for i, (src, dst) in enumerate(((k_ref, ko_hbm), (v_ref, vo_hbm), (x_ref, xo_hbm)))]
    for copy in copies:
        copy.start()
    for copy in copies:
        copy.wait()


def solution(mesh):
    row_spec = P('dp', 'tp', None)
    cache_spec = P('dp', None, 'tp', None)
    head_cols = P(None, 'tp', None)
    in_specs = (row_spec, P('dp'), cache_spec, cache_spec, P(), head_cols, head_cols, head_cols, P('tp', None, None), P(), P(None, 'tp'), P(None, 'tp'), P('tp', None))
    out_specs = (row_spec, cache_spec, cache_spec)

    def local_layer(x_in, start_pos, k_cache, v_cache, attn_gain, w_query, w_key, w_value, w_out, mlp_gain, w_gate, w_up, w_down):
        freq = np.repeat(ROPE_BASE ** (-np.arange(0, 128, 2) / 128.0), 2).astype(np.float32)
        freq = jnp.asarray(np.tile(freq[None, :], (8, 1)))
        any_spec = pl.BlockSpec(memory_space=pl.ANY)
        vmem_spec = pl.BlockSpec(memory_space=pltpu.VMEM)
        dma = pltpu.SemaphoreType.DMA
        kc2 = k_cache.reshape(W, 128)
        vc2 = v_cache.reshape(W, 128)
        results = pl.pallas_call(
            layer_kernel,
            out_shape=(pltpu.VMEM((16, D), BF16), pltpu.VMEM((W, 128), BF16), pltpu.VMEM((W, 128), BF16)),
            in_specs=[any_spec] * 14,
            out_specs=(vmem_spec, vmem_spec, vmem_spec),
            scratch_shapes=[
                pltpu.SMEM((1,), jnp.int32),
                pltpu.VMEM((16, D), BF16),
                pltpu.VMEM((32, 128), BF16),
                pltpu.VMEM((32, 128), BF16),
                pltpu.VMEM((D, FF), BF16),
                pltpu.VMEM((D, FF), BF16),
                pltpu.VMEM((T, D), BF16),
                pltpu.VMEM((T, D), BF16),
                pltpu.VMEM((2, T, D), BF16),
                pltpu.VMEM((2, 64, D), BF16),
                pltpu.VMEM((2, 64, D), BF16),
                pltpu.VMEM((2, 3, 16, D), BF16),
                pltpu.VMEM((2, 16, VIA * CW), BF16),
                pltpu.VMEM((16, D), BF16),
                dma((10,)),
                dma((2, NA)),
                dma((NP,)),
                dma((2, 4, NA)),
                dma((2, 4, NA)),
                dma((2, 4, NA)),
                dma((2, 4, NA)),
                dma((2, NR)),
                dma((2, NR)),
                dma((2, 4, NR)),
                dma((2, 4, NR)),
                dma((2, 4, len(HAND))),
                dma((2, 4, len(HAND))),
                dma((2, 4, len(HAND))),
                dma((2, 4, len(HAND))),
            ],
            compiler_params=pltpu.CompilerParams(collective_id=0, has_side_effects=True, vmem_limit_bytes=VMEM_LIMIT),
            name="layer",
        )(
            start_pos, x_in.reshape(16, D), freq, kc2, vc2, attn_gain.reshape(32, 128), w_query.reshape(4 * D, 128),
            w_key.reshape(D, 128), w_value.reshape(D, 128), w_out.reshape(512, D), mlp_gain.reshape(32, 128), w_gate, w_up, w_down,
        )
        x_out, k_new, v_new = pl.pallas_call(
            write_kernel,
            out_shape=(jax.ShapeDtypeStruct((16, D), BF16), jax.ShapeDtypeStruct((W, 128), BF16), jax.ShapeDtypeStruct((W, 128), BF16)),
            in_specs=[vmem_spec] * 3,
            out_specs=(pl.BlockSpec(memory_space=pltpu.HBM),) * 3,
            scratch_shapes=[dma((3,))],
            compiler_params=pltpu.CompilerParams(vmem_limit_bytes=1 << 20),
            name="write",
        )(*[pltpu.with_memory_space_constraint(r, pltpu.VMEM) for r in results])
        return x_out.reshape(x_in.shape), k_new.reshape(k_cache.shape), v_new.reshape(v_cache.shape)

    return jax.shard_map(local_layer, mesh=mesh, in_specs=in_specs, out_specs=out_specs, check_vma=False)
```

```python
import functools

import jax
import numpy as np
import jax.numpy as jnp
from jax import lax
from jax.experimental import pallas as pl
from jax.experimental.pallas import tpu as pltpu
from jax.sharding import PartitionSpec as P

ROPE_BASE = 10000.0
NORM_EPS = 1e-5
BF16 = jnp.bfloat16
F32 = jnp.float32
D = 4096
T = 128
FF = 1792
W = 4096
NP = 8
CW = D // NP
GATHER = [(512 * p, 512) for p in range(7)] + [(3584, 256), (3840, 256)]
SCATTER = [(512 * p, 512) for p in range(8)]
NA = len(GATHER)
NW = 4
NR = len(SCATTER)
LAG = 2
VIA = 6
VMEM_LIMIT = 64000000
KB = 512
NKB = W // KB


def token_of_row(row):
    core = row // 64
    chip = (row // 16) % 4
    return 32 * chip + 16 * core + row % 16


def layer_kernel(start_hbm, x_hbm, freq_hbm, kc_hbm, vc_hbm, g1_hbm, wq_hbm, wk_hbm, wv_hbm, wo_hbm, g2_hbm, wg_hbm, wu_hbm, wd_hbm,
                 xo_ref, kn_ref, vn_ref,
                 start_ref, xv, g1, g2, wg, wu, xg1, xg2, pbuf, ra, sb, rb, tb, hb,
                 lsem, wsem, dsem, gsend_sem, drecv_sem, frecv_sem, asend_sem, arecv_sem, bsend_sem, brecv_sem, trecv_sem):
    me = lax.axis_index("tp")
    core = me % 2
    chip = me // 2
    other = 1 - core
    partner = 2 * chip + other
    flip1 = chip + 1 - 2 * (chip % 2)
    flip2 = chip + 2 - 4 * (chip // 2)
    flip3 = 3 - chip
    chips = (chip, flip1, flip2, flip3)
    my_rows = pl.ds(pl.multiple_of(64 * core + 16 * chip, 16), 16)

    def rows_of(c, q):
        return pl.ds(pl.multiple_of(64 * c + 16 * q, 16), 16)

    def remote(src, dst, ssem, rsem, dev):
        return pltpu.make_async_remote_copy(src_ref=src, dst_ref=dst, send_sem=ssem, recv_sem=rsem, device_id={"tp": dev}, device_id_type=pl.DeviceIdType.MESH)

    def local(src, dst, sem):
        return pltpu.make_async_copy(src, dst, sem)

    def piece(xg, c, r, p):
        return xg.at[rows_of(c, chips[r]), pl.ds(*GATHER[p])]

    def ag_direct(ph, xg, r, p):
        ref = piece(xg, core, 0, p)
        return remote(ref, ref, gsend_sem.at[ph], drecv_sem.at[ph, p], 2 * chips[r] + core)

    def ag_forward(ph, xg, r, p):
        ref = piece(xg, core, r, p)
        return remote(ref, ref, gsend_sem.at[ph], frecv_sem.at[ph, p], partner)

    def ag_start(ph, xg):
        for p in range(NA):
            for r in (3, 1, 2):
                ag_direct(ph, xg, r, p).start()
            ag_forward(ph, xg, 0, p).start()

    def ag_relay(ph, xg, p):
        ref = xg.at[pl.ds(0, 48), pl.ds(*GATHER[p])]
        remote(ref, ref, gsend_sem.at[ph], drecv_sem.at[ph, p], partner).wait_recv()
        for r in (1, 2, 3):
            ag_forward(ph, xg, r, p).start()

    def ag_arrive(ph, xg, p):
        ref = xg.at[pl.ds(0, 64), pl.ds(*GATHER[p])]
        remote(ref, ref, gsend_sem.at[ph], frecv_sem.at[ph, p], partner).wait_recv()

    def ag_finish(ph, xg):
        ref = xg.at[pl.ds(0, 112), :]
        remote(ref, ref, gsend_sem.at[ph], drecv_sem.at[ph, 0], partner).wait_send()

    def rs_a(ph, n):
        cols = pl.ds(*SCATTER[n])
        return remote(pbuf.at[ph, pl.ds(pl.multiple_of(64 * other, 64), 64), cols], ra.at[ph, :, cols], asend_sem.at[ph], arecv_sem.at[ph, n], partner)

    def rs_b(ph, n, r):
        cols = pl.ds(*SCATTER[n])
        return remote(sb.at[ph, pl.ds(pl.multiple_of(16 * chips[r], 16), 16), cols], rb.at[ph, r - 1, :, cols], bsend_sem.at[ph], brecv_sem.at[ph, n], 2 * chips[r] + core)

    def rs_put(ph, n, part):
        pbuf[ph, :, pl.ds(*SCATTER[n])] = part.astype(BF16)
        rs_a(ph, n).start()

    def rs_first(n):
        return 1 + n % 2

    def rs_transit(ph, n):
        cols = pl.ds(*SCATTER[n])
        src = sb.at[ph, pl.ds(pl.multiple_of(16 * chips[3], 16), 16), cols]
        return remote(src, tb.at[ph, :, cols], bsend_sem.at[ph], trecv_sem.at[ph, n], 2 * chips[rs_first(n)] + core)

    def rs_pair(ph, n):
        cols = pl.ds(*SCATTER[n])
        rs_a(ph, n).wait_recv()
        own = pbuf[ph, pl.ds(pl.multiple_of(64 * core, 64), 64), cols].astype(F32)
        sb[ph, :, cols] = (own + ra[ph, :, cols].astype(F32)).astype(BF16)
        if n < VIA:
            rs_transit(ph, n).start()
            rs_b(ph, n, rs_first(n)).start()
        else:
            for r in (3, 1, 2):
                rs_b(ph, n, r).start()

    def rs_cross(ph, n):
        cols = pl.ds(*SCATTER[n])
        second = 3 - rs_first(n)
        rows = pl.ds(pl.multiple_of(16 * chips[second], 16), 16)
        rs_transit(ph, n).wait_recv()
        sb[ph, rows, cols] = (sb[ph, rows, cols].astype(F32) + tb[ph, :, cols].astype(F32)).astype(BF16)
        rs_b(ph, n, second).start()

    def rs_all(ph, product, group):
        for n in range(0, NR, group):
            part = product(n, pl.ds(SCATTER[n][0], group * CW))
            for k in range(group):
                rs_put(ph, n + k, part[:, k * CW:k * CW + CW])
            for k in range(n - LAG, n - LAG + group):
                if k >= 0:
                    rs_pair(ph, k)
        for n in range(NR - LAG, NR):
            rs_pair(ph, n)
        for n in range(VIA):
            rs_cross(ph, n)

    def rs_sum(ph, n):
        cols = pl.ds(*SCATTER[n])
        total = sb[ph, pl.ds(pl.multiple_of(16 * chip, 16), 16), cols].astype(F32)
        count = 2 if n < VIA else 3
        ref = rb.at[ph, pl.ds(0, count), :, cols]
        remote(ref, ref, bsend_sem.at[ph], brecv_sem.at[ph, n], partner).wait_recv()
        for r in range(1, count + 1):
            total = total + rb[ph, r - 1, :, cols].astype(F32)
        return total

    def rs_finish(ph):
        remote(ra.at[ph], ra.at[ph], asend_sem.at[ph], arecv_sem.at[ph, 0], partner).wait_send()
        remote(rb.at[ph], rb.at[ph], bsend_sem.at[ph], brecv_sem.at[ph, 0], partner).wait_send()

    def normed(rows, gain):
        ms = jnp.zeros((16, 128), F32)
        for j in range(32):
            v = rows[:, 128 * j:128 * j + 128].astype(F32)
            ms = ms + v * v
        inv = lax.rsqrt(jnp.sum(ms, axis=-1, keepdims=True) * (1.0 / D) + NORM_EPS)
        return inv

    def store_normed(src, gain, dst):
        inv = normed(src, gain)
        for j in range(32):
            cols = slice(128 * j, 128 * j + 128)
            val = src[:, cols].astype(F32) * inv * gain[j:j + 1, :].astype(F32)
            dst[my_rows, cols] = val.astype(BF16)

    gate_loads = [local(wg_hbm, wg, wsem.at[0]), local(wu_hbm, wu, wsem.at[1])]

    def attention_phase(kc, vc, vt, wo, freqv, qt, kch, vch, bias, o_buf):
        loads = {
            "x": local(x_hbm, xv, lsem.at[0]),
            "g1": local(g1_hbm, g1, lsem.at[1]),
            "freq": local(freq_hbm, freqv, lsem.at[6]),
            "vc": local(vc_hbm, vc, lsem.at[4]),
            "kc": local(kc_hbm, kc, lsem.at[5]),
            "wo": local(wo_hbm, wo, lsem.at[8]),
            "g2": local(g2_hbm, g2, lsem.at[9]),
            "start": local(start_hbm, start_ref, lsem.at[7]),
        }
        loads["x"].start()
        loads["g1"].start()
        barrier = pltpu.get_barrier_semaphore()
        for dev in (partner, 2 * flip1 + core, 2 * flip2 + core, 2 * flip3 + core):
            pl.semaphore_signal(barrier, inc=1, device_id={"tp": dev}, device_id_type=pl.DeviceIdType.MESH)
        tok_lane = token_of_row(lax.broadcasted_iota(jnp.int32, (1, 128), 1))

        def projection_phase(wq4, wqkv):
            wk_load = local(wk_hbm, wqkv.at[:, pl.ds(512, 128)], lsem.at[2])
            wv_load = local(wv_hbm, wqkv.at[:, pl.ds(640, 128)], lsem.at[3])
            wq_loads = [local(wq_hbm.at[pl.ds(p * 4 * (D // NW), 4 * (D // NW)), :], wq4.at[pl.ds(p * 4 * (D // NW), 4 * (D // NW)), :], dsem.at[p]) for p in range(NW)]
            for ld in wq_loads:
                ld.start()
            loads["vc"].start()
            loads["freq"].start()
            loads["start"].start()
            wk_load.start()
            wv_load.start()
            for name in ("kc", "wo", "g2"):
                loads[name].start()

            loads["x"].wait()
            loads["g1"].wait()
            store_normed(xv, g1, xg1)
            pl.semaphore_wait(barrier, 4)
            ag_start(0, xg1)

            ri = lax.broadcasted_iota(jnp.int32, (256, 256), 0)
            ci = lax.broadcasted_iota(jnp.int32, (256, 256), 1)
            perm = (ci == 4 * (ri % 64) + ri // 64).astype(F32).astype(BF16)

            def split_heads(p):
                if p % (NP // NW) == 0:
                    wq_loads[p // (NP // NW)].wait()

                def body(i, carry):
                    base = p * (CW // 64) + 2 * i
                    rows4 = jnp.concatenate([wq4[pl.ds(pl.multiple_of((base + k) * 256, 256), 256), :] for k in range(2)], axis=1)
                    out = jnp.dot(perm, rows4, preferred_element_type=F32).astype(BF16)
                    for k in range(2):
                        for h in range(4):
                            wqkv[pl.ds(pl.multiple_of((base + k) * 64, 64), 64), h * 128:h * 128 + 128] = out[64 * h:64 * h + 64, k * 128:k * 128 + 128]
                    return carry

                for i in range(CW // 128):
                    body(i, 0)

            loads["vc"].wait()

            def flip_values(i, carry):
                ks = pl.ds(pl.multiple_of(i * KB, KB), KB)
                vt[:, ks] = vc[ks, :].astype(F32).T.astype(BF16)
                slot = i * KB + lax.broadcasted_iota(jnp.int32, (KB, 128), 0)
                off = jnp.bitwise_and(slot - start, W - 1)
                keep = jnp.where(off >= W - start, off, -1) > tok_lane
                bias[ks, :] = jnp.where(keep, 0.0, -jnp.inf)
                return carry

            loads["start"].wait()
            start = start_ref[0]
            for p in range(4):
                split_heads(p)
            for p in range(6):
                flip_values(p, 0)
            loads["freq"].wait()
            tok_row = token_of_row(lax.broadcasted_iota(jnp.int32, (T, 128), 0))
            angles = (start + tok_row).astype(F32) * freqv[0:1, :]
            cos_t = jnp.cos(angles)
            lane = lax.broadcasted_iota(jnp.int32, (T, 128), 1)
            even = lane % 2 == 0
            sin_t = jnp.sin(angles)
            sin_t = jnp.where(even, -sin_t, sin_t)
            wk_load.wait()
            wv_load.wait()
            acc = jnp.zeros((T, 768), F32)
            ag_relay(0, xg1, 0)
            ag_relay(0, xg1, 1)
            for p in range(NA):
                if p + 2 < NA:
                    ag_relay(0, xg1, p + 2)
                if p + 4 < NP:
                    split_heads(p + 4)
                if p < 2:
                    flip_values(p + 6, 0)
                ag_arrive(0, xg1, p)
                cols = pl.ds(*GATHER[p])
                acc = acc + jnp.dot(xg1[:, cols], wqkv[cols, :], preferred_element_type=F32)
            for ld in gate_loads:
                ld.start()

            def rotate(v):
                swapped = jnp.where(even, pltpu.roll(v, 127, 1), pltpu.roll(v, 1, 1))
                return v * cos_t + swapped * sin_t

            for h in range(4):
                qt[:, h * 128:h * 128 + 128] = rotate(acc[:, h * 128:h * 128 + 128]).T.astype(BF16)
            kch[...] = rotate(acc[:, 512:640]).astype(BF16)
            v_new = acc[:, 640:768].astype(BF16)
            vch[...] = v_new
            vt[:, W:W + T] = v_new.astype(F32).T.astype(BF16)

        pl.run_scoped(
            projection_phase,
            pltpu.VMEM((4 * D, 128), BF16),
            pltpu.VMEM((D, 768), BF16),
        )
        loads["kc"].wait()
        factor = (128.0 ** -0.5) * 1.4426950408889634

        def softmax_phase(e_buf):
            queries = qt[...]
            tops, masses = [], []
            for b in range(NKB + 1):
                keys = kc[b * KB:b * KB + KB, :] if b < NKB else kch[...]
                scores = jnp.dot(keys, queries, preferred_element_type=F32)
                for i in range(KB // 128 if b < NKB else 1):
                    ks = slice(b * KB + i * 128, b * KB + i * 128 + 128)
                    if b < NKB:
                        shift = bias[ks, :]
                    else:
                        shift = jnp.where(token_of_row(lax.broadcasted_iota(jnp.int32, (T, 128), 0)) <= tok_lane, 0.0, -jnp.inf)
                    top, mass = [], []
                    for g in range(4):
                        gs = slice(g * 128, g * 128 + 128)
                        part = (scores[i * 128:i * 128 + 128, gs] + shift).reshape(16, 8, 128)
                        t = jnp.maximum(jnp.max(part, axis=0), jnp.finfo(F32).min)
                        e = jnp.exp2((part - t[None]) * factor)
                        e_buf[ks, gs] = e.reshape(128, 128)
                        mass.append(jnp.sum(e, axis=0))
                        top.append(t)
                    tops.append(top)
                    masses.append(mass)
            blocks = len(tops)
            weights = []
            for g in range(4):
                best = jnp.max(functools.reduce(jnp.maximum, [tops[b][g] for b in range(blocks)]), axis=0, keepdims=True)
                scales = [jnp.exp2((tops[b][g] - best) * factor) for b in range(blocks)]
                total = functools.reduce(jnp.add, [masses[b][g] * scales[b] for b in range(blocks)])
                inv = 1.0 / jnp.sum(total, axis=0, keepdims=True)
                weights.append([sc * inv for sc in scales])
            out = None
            for b in range(NKB + 1):
                n = KB if b < NKB else T
                ks = slice(b * KB, b * KB + n)
                rows = []
                for i in range(n // 128):
                    r0 = b * KB + i * 128
                    cols = [(e_buf[r0:r0 + 128, g * 128:g * 128 + 128].reshape(16, 8, 128) * weights[g][b * (KB // 128) + i][None]).reshape(128, 128) for g in range(4)]
                    rows.append(jnp.concatenate(cols, axis=1))
                probs = jnp.concatenate(rows, axis=0).astype(BF16)
                part = jnp.dot(vt[:, ks], probs, preferred_element_type=F32)
                out = part if out is None else out + part
            for g in range(4):
                o_buf[:, g * 128:g * 128 + 128] = out[:, g * 128:g * 128 + 128].T.astype(BF16)

        pl.run_scoped(softmax_phase, pltpu.VMEM((W + T, 512), F32))
        loads["wo"].wait()
        rs_all(0, lambda n, cols: jnp.dot(o_buf[...], wo[:, cols], preferred_element_type=F32), 2)
        loads["g2"].wait()

        chunk = jnp.concatenate([kch[...], vch[...]], axis=1)

        def merge(i, carry):
            ks = pl.ds(pl.multiple_of(i * KB, KB), KB)
            slot = i * KB + lax.broadcasted_iota(jnp.int32, (KB, 128), 0)
            off = jnp.bitwise_and(slot - start, W - 1)
            pick = (off == tok_lane).astype(F32).astype(BF16)
            placed = jnp.dot(pick, chunk, preferred_element_type=F32)
            fresh = off < T
            kn_ref[ks, :] = jnp.where(fresh, placed[:, 0:128], kc[ks, :].astype(F32)).astype(BF16)
            vn_ref[ks, :] = jnp.where(fresh, placed[:, 128:256], vc[ks, :].astype(F32)).astype(BF16)
            return carry

        start = start_ref[0]
        lax.fori_loop(0, NKB, merge, 0)

    pl.run_scoped(
        attention_phase,
        pltpu.VMEM((W, 128), BF16),
        pltpu.VMEM((W, 128), BF16),
        pltpu.VMEM((128, W + T), BF16),
        pltpu.VMEM((512, D), BF16),
        pltpu.VMEM((8, 128), F32),
        pltpu.VMEM((128, 512), BF16),
        pltpu.VMEM((T, 128), BF16),
        pltpu.VMEM((T, 128), BF16),
        pltpu.VMEM((W, 128), F32),
        pltpu.VMEM((T, 512), BF16),
    )

    def mlp_phase(wd, acc_g, acc_u, u_buf):
        down_load = local(wd_hbm, wd, wsem.at[2])
        down_load.start()
        for n in range(NR):
            cols = pl.ds(*SCATTER[n])
            hb[:, cols] = (xv[:, cols].astype(F32) + rs_sum(0, n)).astype(BF16)
        store_normed(hb, g2, xg2)
        ag_start(1, xg2)
        ag_finish(0, xg1)
        rs_finish(0)
        ag_relay(1, xg2, 0)
        ag_relay(1, xg2, 1)
        for p in range(NA):
            if p + 2 < NA:
                ag_relay(1, xg2, p + 2)
            if p == 0:
                for ld in gate_loads:
                    ld.wait()
            ag_arrive(1, xg2, p)
            rows = pl.ds(*GATHER[p])
            m = xg2[:, rows]
            gate = jnp.dot(m, wg[rows, :], preferred_element_type=F32)
            up = jnp.dot(m, wu[rows, :], preferred_element_type=F32)
            if p == 0:
                acc_g[...] = gate
                acc_u[...] = up
            elif p + 1 < NA:
                acc_g[...] += gate
                acc_u[...] += up
            else:
                gate = acc_g[...] + gate
                u_buf[...] = (gate / (1.0 + jnp.exp(-gate)) * (acc_u[...] + up)).astype(BF16)
        def down(n, cols):
            if n == 0:
                down_load.wait()
            return jnp.dot(u_buf[...], wd[:, cols], preferred_element_type=F32)

        rs_all(1, down, 1)
        ag_finish(1, xg2)
        for n in range(NR):
            cols = pl.ds(*SCATTER[n])
            xo_ref[:, cols] = (hb[:, cols].astype(F32) + rs_sum(1, n)).astype(BF16)
        rs_finish(1)

    pl.run_scoped(
        mlp_phase,
        pltpu.VMEM((FF, D), BF16),
        pltpu.VMEM((T, FF), F32),
        pltpu.VMEM((T, FF), F32),
        pltpu.VMEM((T, FF), BF16),
    )


def write_kernel(x_ref, k_ref, v_ref, xo_hbm, ko_hbm, vo_hbm, sem):
    copies = [pltpu.make_async_copy(src, dst, sem.at[i]) for i, (src, dst) in enumerate(((k_ref, ko_hbm), (v_ref, vo_hbm), (x_ref, xo_hbm)))]
    for copy in copies:
        copy.start()
    for copy in copies:
        copy.wait()


def solution(mesh):
    row_spec = P('dp', 'tp', None)
    cache_spec = P('dp', None, 'tp', None)
    head_cols = P(None, 'tp', None)
    in_specs = (row_spec, P('dp'), cache_spec, cache_spec, P(), head_cols, head_cols, head_cols, P('tp', None, None), P(), P(None, 'tp'), P(None, 'tp'), P('tp', None))
    out_specs = (row_spec, cache_spec, cache_spec)

    def local_layer(x_in, start_pos, k_cache, v_cache, attn_gain, w_query, w_key, w_value, w_out, mlp_gain, w_gate, w_up, w_down):
        freq = np.repeat(ROPE_BASE ** (-np.arange(0, 128, 2) / 128.0), 2).astype(np.float32)
        freq = jnp.asarray(np.tile(freq[None, :], (8, 1)))
        any_spec = pl.BlockSpec(memory_space=pl.ANY)
        vmem_spec = pl.BlockSpec(memory_space=pltpu.VMEM)
        dma = pltpu.SemaphoreType.DMA
        kc2 = k_cache.reshape(W, 128)
        vc2 = v_cache.reshape(W, 128)
        results = pl.pallas_call(
            layer_kernel,
            out_shape=(pltpu.VMEM((16, D), BF16), pltpu.VMEM((W, 128), BF16), pltpu.VMEM((W, 128), BF16)),
            in_specs=[any_spec] * 14,
            out_specs=(vmem_spec, vmem_spec, vmem_spec),
            scratch_shapes=[
                pltpu.SMEM((1,), jnp.int32),
                pltpu.VMEM((16, D), BF16),
                pltpu.VMEM((32, 128), BF16),
                pltpu.VMEM((32, 128), BF16),
                pltpu.VMEM((D, FF), BF16),
                pltpu.VMEM((D, FF), BF16),
                pltpu.VMEM((T, D), BF16),
                pltpu.VMEM((T, D), BF16),
                pltpu.VMEM((2, T, D), BF16),
                pltpu.VMEM((2, 64, D), BF16),
                pltpu.VMEM((2, 64, D), BF16),
                pltpu.VMEM((2, 3, 16, D), BF16),
                pltpu.VMEM((2, 16, VIA * CW), BF16),
                pltpu.VMEM((16, D), BF16),
                dma((10,)),
                dma((3,)),
                dma((NW,)),
                dma((2,)),
                dma((2, NA)),
                dma((2, NA)),
                dma((2,)),
                dma((2, NR)),
                dma((2,)),
                dma((2, NR)),
                dma((2, VIA)),
            ],
            compiler_params=pltpu.CompilerParams(collective_id=0, has_side_effects=True, vmem_limit_bytes=VMEM_LIMIT),
            name="layer",
        )(
            start_pos, x_in.reshape(16, D), freq, kc2, vc2, attn_gain.reshape(32, 128), w_query.reshape(4 * D, 128),
            w_key.reshape(D, 128), w_value.reshape(D, 128), w_out.reshape(512, D), mlp_gain.reshape(32, 128), w_gate, w_up, w_down,
        )
        x_out, k_new, v_new = pl.pallas_call(
            write_kernel,
            out_shape=(jax.ShapeDtypeStruct((16, D), BF16), jax.ShapeDtypeStruct((W, 128), BF16), jax.ShapeDtypeStruct((W, 128), BF16)),
            in_specs=[vmem_spec] * 3,
            out_specs=(pl.BlockSpec(memory_space=pltpu.HBM),) * 3,
            scratch_shapes=[dma((3,))],
            compiler_params=pltpu.CompilerParams(vmem_limit_bytes=1 << 20),
            name="write",
        )(*[pltpu.with_memory_space_constraint(r, pltpu.VMEM) for r in results])
        return x_out.reshape(x_in.shape), k_new.reshape(k_cache.shape), v_new.reshape(v_cache.shape)

    return jax.shard_map(local_layer, mesh=mesh, in_specs=in_specs, out_specs=out_specs, check_vma=False)
```

```python
import functools

import jax
import numpy as np
import jax.numpy as jnp
from jax import lax
from jax.experimental import pallas as pl
from jax.experimental.pallas import tpu as pltpu
from jax.sharding import PartitionSpec as P

ROPE_BASE = 10000.0
NORM_EPS = 1e-5
BF16 = jnp.bfloat16
F32 = jnp.float32
D = 4096
T = 128
FF = 1792
W = 4096
NP = 8
CW = D // NP
GATHER = [(0, 256), (256, 256)] + [(512 * p, 512) for p in range(1, 7)] + [(3584, 256), (3840, 256)]
SCATTER = [(512 * p, 512) for p in range(8)]
NA = len(GATHER)
NW = 2
NR = len(SCATTER)
LAG = 2
VIA = 6
VMEM_LIMIT = 64000000
KB = 512
NKB = W // KB


def token_of_row(row):
    core = row // 64
    chip = (row // 16) % 4
    return 32 * chip + 16 * core + row % 16


def layer_kernel(start_hbm, x_hbm, freq_hbm, kc_hbm, vc_hbm, g1_hbm, wq_hbm, wk_hbm, wv_hbm, wo_hbm, g2_hbm, wg_hbm, wu_hbm, wd_hbm,
                 xo_ref, kn_ref, vn_ref,
                 start_ref, xv, g1, g2, wg, wu, xg1, xg2, pbuf, ra, sb, rb, tb, hb,
                 lsem, wsem, dsem, gsend_sem, drecv_sem, frecv_sem, asend_sem, arecv_sem, bsend_sem, brecv_sem, trecv_sem):
    me = lax.axis_index("tp")
    core = me % 2
    chip = me // 2
    other = 1 - core
    partner = 2 * chip + other
    flip1 = chip + 1 - 2 * (chip % 2)
    flip2 = chip + 2 - 4 * (chip // 2)
    flip3 = 3 - chip
    chips = (chip, flip1, flip2, flip3)
    my_rows = pl.ds(pl.multiple_of(64 * core + 16 * chip, 16), 16)

    def rows_of(c, q):
        return pl.ds(pl.multiple_of(64 * c + 16 * q, 16), 16)

    def remote(src, dst, ssem, rsem, dev):
        return pltpu.make_async_remote_copy(src_ref=src, dst_ref=dst, send_sem=ssem, recv_sem=rsem, device_id={"tp": dev}, device_id_type=pl.DeviceIdType.MESH)

    def local(src, dst, sem):
        return pltpu.make_async_copy(src, dst, sem)

    def piece(xg, c, r, p):
        return xg.at[rows_of(c, chips[r]), pl.ds(*GATHER[p])]

    def ag_direct(ph, xg, r, p):
        ref = piece(xg, core, 0, p)
        return remote(ref, ref, gsend_sem.at[ph], drecv_sem.at[p], 2 * chips[r] + core)

    def ag_forward(ph, xg, r, p):
        ref = piece(xg, core, r, p)
        return remote(ref, ref, gsend_sem.at[ph], frecv_sem.at[p], partner)

    def ag_start(ph, xg):
        for p in range(NA):
            for r in (3, 1, 2):
                ag_direct(ph, xg, r, p).start()
            ag_forward(ph, xg, 0, p).start()

    def ag_relay(ph, xg, p):
        ref = xg.at[pl.ds(0, 48), pl.ds(*GATHER[p])]
        remote(ref, ref, gsend_sem.at[ph], drecv_sem.at[p], partner).wait_recv()
        for r in (1, 2, 3):
            ag_forward(ph, xg, r, p).start()

    def ag_arrive(ph, xg, p):
        ref = xg.at[pl.ds(0, 64), pl.ds(*GATHER[p])]
        remote(ref, ref, gsend_sem.at[ph], frecv_sem.at[p], partner).wait_recv()

    def ag_finish(ph, xg):
        ref = xg.at[pl.ds(0, 112), :]
        remote(ref, ref, gsend_sem.at[ph], drecv_sem.at[0], partner).wait_send()

    def rs_a(ph, n):
        cols = pl.ds(*SCATTER[n])
        return remote(pbuf.at[ph, pl.ds(pl.multiple_of(64 * other, 64), 64), cols], ra.at[ph, :, cols], asend_sem.at[ph], arecv_sem.at[n], partner)

    def rs_b(ph, n, r):
        cols = pl.ds(*SCATTER[n])
        return remote(sb.at[ph, pl.ds(pl.multiple_of(16 * chips[r], 16), 16), cols], rb.at[ph, r - 1, :, cols], bsend_sem.at[ph], brecv_sem.at[n], 2 * chips[r] + core)

    def rs_put(ph, n, part):
        pbuf[ph, :, pl.ds(*SCATTER[n])] = part.astype(BF16)
        rs_a(ph, n).start()

    def rs_first(n):
        return 1 + n % 2

    def rs_transit(ph, n):
        cols = pl.ds(*SCATTER[n])
        src = sb.at[ph, pl.ds(pl.multiple_of(16 * chips[3], 16), 16), cols]
        return remote(src, tb.at[ph, :, cols], bsend_sem.at[ph], trecv_sem.at[n], 2 * chips[rs_first(n)] + core)

    def rs_pair(ph, n):
        cols = pl.ds(*SCATTER[n])
        rs_a(ph, n).wait_recv()
        own = pbuf[ph, pl.ds(pl.multiple_of(64 * core, 64), 64), cols].astype(F32)
        sb[ph, :, cols] = (own + ra[ph, :, cols].astype(F32)).astype(BF16)
        if n < VIA:
            rs_transit(ph, n).start()
            rs_b(ph, n, rs_first(n)).start()
        else:
            for r in (3, 1, 2):
                rs_b(ph, n, r).start()

    def rs_cross(ph, n):
        cols = pl.ds(*SCATTER[n])
        second = 3 - rs_first(n)
        rows = pl.ds(pl.multiple_of(16 * chips[second], 16), 16)
        rs_transit(ph, n).wait_recv()
        sb[ph, rows, cols] = (sb[ph, rows, cols].astype(F32) + tb[ph, :, cols].astype(F32)).astype(BF16)
        rs_b(ph, n, second).start()

    def rs_all(ph, product, group):
        for n in range(0, NR, group):
            part = product(n, pl.ds(SCATTER[n][0], group * CW))
            for k in range(group):
                rs_put(ph, n + k, part[:, k * CW:k * CW + CW])
            for k in range(n - LAG, n - LAG + group):
                if k >= 0:
                    rs_pair(ph, k)
        for n in range(NR - LAG, NR):
            rs_pair(ph, n)
        for n in range(VIA):
            rs_cross(ph, n)

    def rs_sum(ph, n):
        cols = pl.ds(*SCATTER[n])
        total = sb[ph, pl.ds(pl.multiple_of(16 * chip, 16), 16), cols].astype(F32)
        count = 2 if n < VIA else 3
        ref = rb.at[ph, pl.ds(0, count), :, cols]
        remote(ref, ref, bsend_sem.at[ph], brecv_sem.at[n], partner).wait_recv()
        for r in range(1, count + 1):
            total = total + rb[ph, r - 1, :, cols].astype(F32)
        return total

    def rs_finish(ph):
        remote(ra.at[ph], ra.at[ph], asend_sem.at[ph], arecv_sem.at[0], partner).wait_send()
        remote(rb.at[ph], rb.at[ph], bsend_sem.at[ph], brecv_sem.at[0], partner).wait_send()

    def normed(rows, gain):
        ms = jnp.zeros((16, 128), F32)
        for j in range(32):
            v = rows[:, 128 * j:128 * j + 128].astype(F32)
            ms = ms + v * v
        inv = lax.rsqrt(jnp.sum(ms, axis=-1, keepdims=True) * (1.0 / D) + NORM_EPS)
        return inv

    def store_normed(src, gain, dst):
        inv = normed(src, gain)
        for j in range(32):
            cols = slice(128 * j, 128 * j + 128)
            val = src[:, cols].astype(F32) * inv * gain[j:j + 1, :].astype(F32)
            dst[my_rows, cols] = val.astype(BF16)

    gate_loads = [local(wg_hbm, wg, wsem.at[0]), local(wu_hbm, wu, wsem.at[1])]

    def attention_phase(kc, vc, vt, wo, freqv, qt, kch, vch, bias, o_buf):
        loads = {
            "x": local(x_hbm, xv, lsem.at[0]),
            "g1": local(g1_hbm, g1, lsem.at[1]),
            "freq": local(freq_hbm, freqv, lsem.at[6]),
            "vc": local(vc_hbm, vc, lsem.at[4]),
            "kc": local(kc_hbm, kc, lsem.at[5]),
            "wo": local(wo_hbm, wo, lsem.at[8]),
            "g2": local(g2_hbm, g2, lsem.at[9]),
            "start": local(start_hbm, start_ref, lsem.at[7]),
        }
        loads["x"].start()
        loads["g1"].start()
        barrier = pltpu.get_barrier_semaphore()
        for dev in (partner, 2 * flip1 + core, 2 * flip2 + core, 2 * flip3 + core):
            pl.semaphore_signal(barrier, inc=1, device_id={"tp": dev}, device_id_type=pl.DeviceIdType.MESH)
        tok_lane = token_of_row(lax.broadcasted_iota(jnp.int32, (1, 128), 1))

        def projection_phase(wq4, wqkv):
            wk_load = local(wk_hbm, wqkv.at[:, pl.ds(512, 128)], lsem.at[2])
            wv_load = local(wv_hbm, wqkv.at[:, pl.ds(640, 128)], lsem.at[3])
            wq_loads = [local(wq_hbm.at[pl.ds(p * 4 * (D // NW), 4 * (D // NW)), :], wq4.at[pl.ds(p * 4 * (D // NW), 4 * (D // NW)), :], dsem.at[p]) for p in range(NW)]
            for ld in wq_loads:
                ld.start()
            loads["vc"].start()
            loads["freq"].start()
            loads["start"].start()
            wk_load.start()
            wv_load.start()
            for name in ("kc", "wo", "g2"):
                loads[name].start()

            loads["x"].wait()
            loads["g1"].wait()
            store_normed(xv, g1, xg1)
            pl.semaphore_wait(barrier, 4)
            ag_start(0, xg1)

            ri = lax.broadcasted_iota(jnp.int32, (256, 256), 0)
            ci = lax.broadcasted_iota(jnp.int32, (256, 256), 1)
            perm = (ci == 4 * (ri % 64) + ri // 64).astype(F32).astype(BF16)

            def split_heads(p):
                if p % (NP // NW) == 0:
                    wq_loads[p // (NP // NW)].wait()

                def body(i, carry):
                    base = p * (CW // 64) + 2 * i
                    rows4 = jnp.concatenate([wq4[pl.ds(pl.multiple_of((base + k) * 256, 256), 256), :] for k in range(2)], axis=1)
                    out = jnp.dot(perm, rows4, preferred_element_type=F32).astype(BF16)
                    for k in range(2):
                        for h in range(4):
                            wqkv[pl.ds(pl.multiple_of((base + k) * 64, 64), 64), h * 128:h * 128 + 128] = out[64 * h:64 * h + 64, k * 128:k * 128 + 128]
                    return carry

                for i in range(CW // 128):
                    body(i, 0)

            loads["vc"].wait()

            def flip_values(i, carry):
                ks = pl.ds(pl.multiple_of(i * KB, KB), KB)
                vt[:, ks] = vc[ks, :].astype(F32).T.astype(BF16)
                slot = i * KB + lax.broadcasted_iota(jnp.int32, (KB, 128), 0)
                off = jnp.bitwise_and(slot - start, W - 1)
                keep = jnp.where(off >= W - start, off, -1) > tok_lane
                bias[ks, :] = jnp.where(keep, 0.0, -jnp.inf)
                return carry

            loads["start"].wait()
            start = start_ref[0]
            for p in range(4):
                split_heads(p)
            for p in range(6):
                flip_values(p, 0)
            loads["freq"].wait()
            tok_row = token_of_row(lax.broadcasted_iota(jnp.int32, (T, 128), 0))
            angles = (start + tok_row).astype(F32) * freqv[0:1, :]
            cos_t = jnp.cos(angles)
            lane = lax.broadcasted_iota(jnp.int32, (T, 128), 1)
            even = lane % 2 == 0
            sin_t = jnp.sin(angles)
            sin_t = jnp.where(even, -sin_t, sin_t)
            wk_load.wait()
            wv_load.wait()
            acc = jnp.zeros((T, 768), F32)
            ag_relay(0, xg1, 0)
            ag_relay(0, xg1, 1)
            for p in range(NA):
                if p + 2 < NA:
                    ag_relay(0, xg1, p + 2)
                if p + 4 < NP:
                    split_heads(p + 4)
                if p < 2:
                    flip_values(p + 6, 0)
                ag_arrive(0, xg1, p)
                cols = pl.ds(*GATHER[p])
                acc = acc + jnp.dot(xg1[:, cols], wqkv[cols, :], preferred_element_type=F32)
            for ld in gate_loads:
                ld.start()

            def rotate(v):
                swapped = jnp.where(even, pltpu.roll(v, 127, 1), pltpu.roll(v, 1, 1))
                return v * cos_t + swapped * sin_t

            for h in range(4):
                qt[:, h * 128:h * 128 + 128] = rotate(acc[:, h * 128:h * 128 + 128]).T.astype(BF16)
            kch[...] = rotate(acc[:, 512:640]).astype(BF16)
            v_new = acc[:, 640:768].astype(BF16)
            vch[...] = v_new
            vt[:, W:W + T] = v_new.astype(F32).T.astype(BF16)

        pl.run_scoped(
            projection_phase,
            pltpu.VMEM((4 * D, 128), BF16),
            pltpu.VMEM((D, 768), BF16),
        )
        loads["kc"].wait()
        factor = (128.0 ** -0.5) * 1.4426950408889634

        def softmax_phase(e_buf):
            queries = qt[...]
            tops, masses = [], []
            for b in range(NKB + 1):
                keys = kc[b * KB:b * KB + KB, :] if b < NKB else kch[...]
                scores = jnp.dot(keys, queries, preferred_element_type=F32)
                for i in range(KB // 128 if b < NKB else 1):
                    ks = slice(b * KB + i * 128, b * KB + i * 128 + 128)
                    if b < NKB:
                        shift = bias[ks, :]
                    else:
                        shift = jnp.where(token_of_row(lax.broadcasted_iota(jnp.int32, (T, 128), 0)) <= tok_lane, 0.0, -jnp.inf)
                    top, mass = [], []
                    for g in range(4):
                        gs = slice(g * 128, g * 128 + 128)
                        part = (scores[i * 128:i * 128 + 128, gs] + shift).reshape(16, 8, 128)
                        t = jnp.maximum(jnp.max(part, axis=0), jnp.finfo(F32).min)
                        e = jnp.exp2((part - t[None]) * factor)
                        e_buf[ks, gs] = e.reshape(128, 128)
                        mass.append(jnp.sum(e, axis=0))
                        top.append(t)
                    tops.append(top)
                    masses.append(mass)
            blocks = len(tops)
            weights = []
            for g in range(4):
                best = jnp.max(functools.reduce(jnp.maximum, [tops[b][g] for b in range(blocks)]), axis=0, keepdims=True)
                scales = [jnp.exp2((tops[b][g] - best) * factor) for b in range(blocks)]
                total = functools.reduce(jnp.add, [masses[b][g] * scales[b] for b in range(blocks)])
                inv = 1.0 / jnp.sum(total, axis=0, keepdims=True)
                weights.append([sc * inv for sc in scales])
            out = None
            for b in range(NKB + 1):
                n = KB if b < NKB else T
                ks = slice(b * KB, b * KB + n)
                rows = []
                for i in range(n // 128):
                    r0 = b * KB + i * 128
                    cols = [(e_buf[r0:r0 + 128, g * 128:g * 128 + 128].reshape(16, 8, 128) * weights[g][b * (KB // 128) + i][None]).reshape(128, 128) for g in range(4)]
                    rows.append(jnp.concatenate(cols, axis=1))
                probs = jnp.concatenate(rows, axis=0).astype(BF16)
                part = jnp.dot(vt[:, ks], probs, preferred_element_type=F32)
                out = part if out is None else out + part
            for g in range(4):
                o_buf[:, g * 128:g * 128 + 128] = out[:, g * 128:g * 128 + 128].T.astype(BF16)

        pl.run_scoped(softmax_phase, pltpu.VMEM((W + T, 512), F32))
        loads["wo"].wait()
        rs_all(0, lambda n, cols: jnp.dot(o_buf[...], wo[:, cols], preferred_element_type=F32), 2)
        loads["g2"].wait()

        chunk = jnp.concatenate([kch[...], vch[...]], axis=1)

        def merge(i, carry):
            ks = pl.ds(pl.multiple_of(i * KB, KB), KB)
            slot = i * KB + lax.broadcasted_iota(jnp.int32, (KB, 128), 0)
            off = jnp.bitwise_and(slot - start, W - 1)
            pick = (off == tok_lane).astype(F32).astype(BF16)
            placed = jnp.dot(pick, chunk, preferred_element_type=F32)
            fresh = off < T
            kn_ref[ks, :] = jnp.where(fresh, placed[:, 0:128], kc[ks, :].astype(F32)).astype(BF16)
            vn_ref[ks, :] = jnp.where(fresh, placed[:, 128:256], vc[ks, :].astype(F32)).astype(BF16)
            return carry

        start = start_ref[0]
        lax.fori_loop(0, NKB, merge, 0)

    pl.run_scoped(
        attention_phase,
        pltpu.VMEM((W, 128), BF16),
        pltpu.VMEM((W, 128), BF16),
        pltpu.VMEM((128, W + T), BF16),
        pltpu.VMEM((512, D), BF16),
        pltpu.VMEM((8, 128), F32),
        pltpu.VMEM((128, 512), BF16),
        pltpu.VMEM((T, 128), BF16),
        pltpu.VMEM((T, 128), BF16),
        pltpu.VMEM((W, 128), F32),
        pltpu.VMEM((T, 512), BF16),
    )

    def mlp_phase(wd, acc_g, acc_u, u_buf):
        down_load = local(wd_hbm, wd, wsem.at[2])
        down_load.start()
        for n in range(NR):
            cols = pl.ds(*SCATTER[n])
            hb[:, cols] = (xv[:, cols].astype(F32) + rs_sum(0, n)).astype(BF16)
        store_normed(hb, g2, xg2)
        ag_start(1, xg2)
        ag_finish(0, xg1)
        rs_finish(0)
        ag_relay(1, xg2, 0)
        ag_relay(1, xg2, 1)
        for p in range(NA):
            if p + 2 < NA:
                ag_relay(1, xg2, p + 2)
            if p == 0:
                for ld in gate_loads:
                    ld.wait()
            ag_arrive(1, xg2, p)
            rows = pl.ds(*GATHER[p])
            m = xg2[:, rows]
            gate = jnp.dot(m, wg[rows, :], preferred_element_type=F32)
            up = jnp.dot(m, wu[rows, :], preferred_element_type=F32)
            if p == 0:
                acc_g[...] = gate
                acc_u[...] = up
            elif p + 1 < NA:
                acc_g[...] += gate
                acc_u[...] += up
            else:
                gate = acc_g[...] + gate
                u_buf[...] = (gate / (1.0 + jnp.exp(-gate)) * (acc_u[...] + up)).astype(BF16)
        def down(n, cols):
            if n == 0:
                down_load.wait()
            return jnp.dot(u_buf[...], wd[:, cols], preferred_element_type=F32)

        rs_all(1, down, 1)
        ag_finish(1, xg2)
        for n in range(NR):
            cols = pl.ds(*SCATTER[n])
            xo_ref[:, cols] = (hb[:, cols].astype(F32) + rs_sum(1, n)).astype(BF16)
        rs_finish(1)

    pl.run_scoped(
        mlp_phase,
        pltpu.VMEM((FF, D), BF16),
        pltpu.VMEM((T, FF), F32),
        pltpu.VMEM((T, FF), F32),
        pltpu.VMEM((T, FF), BF16),
    )


def write_kernel(x_ref, k_ref, v_ref, xo_hbm, ko_hbm, vo_hbm, sem):
    copies = [pltpu.make_async_copy(src, dst, sem.at[i]) for i, (src, dst) in enumerate(((k_ref, ko_hbm), (v_ref, vo_hbm), (x_ref, xo_hbm)))]
    for copy in copies:
        copy.start()
    for copy in copies:
        copy.wait()


def solution(mesh):
    row_spec = P('dp', 'tp', None)
    cache_spec = P('dp', None, 'tp', None)
    head_cols = P(None, 'tp', None)
    in_specs = (row_spec, P('dp'), cache_spec, cache_spec, P(), head_cols, head_cols, head_cols, P('tp', None, None), P(), P(None, 'tp'), P(None, 'tp'), P('tp', None))
    out_specs = (row_spec, cache_spec, cache_spec)

    def local_layer(x_in, start_pos, k_cache, v_cache, attn_gain, w_query, w_key, w_value, w_out, mlp_gain, w_gate, w_up, w_down):
        freq = np.repeat(ROPE_BASE ** (-np.arange(0, 128, 2) / 128.0), 2).astype(np.float32)
        freq = jnp.asarray(np.tile(freq[None, :], (8, 1)))
        any_spec = pl.BlockSpec(memory_space=pl.ANY)
        vmem_spec = pl.BlockSpec(memory_space=pltpu.VMEM)
        dma = pltpu.SemaphoreType.DMA
        kc2 = k_cache.reshape(W, 128)
        vc2 = v_cache.reshape(W, 128)
        results = pl.pallas_call(
            layer_kernel,
            out_shape=(pltpu.VMEM((16, D), BF16), pltpu.VMEM((W, 128), BF16), pltpu.VMEM((W, 128), BF16)),
            in_specs=[any_spec] * 14,
            out_specs=(vmem_spec, vmem_spec, vmem_spec),
            scratch_shapes=[
                pltpu.SMEM((1,), jnp.int32),
                pltpu.VMEM((16, D), BF16),
                pltpu.VMEM((32, 128), BF16),
                pltpu.VMEM((32, 128), BF16),
                pltpu.VMEM((D, FF), BF16),
                pltpu.VMEM((D, FF), BF16),
                pltpu.VMEM((T, D), BF16),
                pltpu.VMEM((T, D), BF16),
                pltpu.VMEM((2, T, D), BF16),
                pltpu.VMEM((2, 64, D), BF16),
                pltpu.VMEM((2, 64, D), BF16),
                pltpu.VMEM((2, 3, 16, D), BF16),
                pltpu.VMEM((2, 16, VIA * CW), BF16),
                pltpu.VMEM((16, D), BF16),
                dma((10,)),
                dma((3,)),
                dma((NW,)),
                dma((2,)),
                dma((NA,)),
                dma((NA,)),
                dma((2,)),
                dma((NR,)),
                dma((2,)),
                dma((NR,)),
                dma((VIA,)),
            ],
            compiler_params=pltpu.CompilerParams(collective_id=0, has_side_effects=True, vmem_limit_bytes=VMEM_LIMIT),
            name="layer",
        )(
            start_pos, x_in.reshape(16, D), freq, kc2, vc2, attn_gain.reshape(32, 128), w_query.reshape(4 * D, 128),
            w_key.reshape(D, 128), w_value.reshape(D, 128), w_out.reshape(512, D), mlp_gain.reshape(32, 128), w_gate, w_up, w_down,
        )
        x_out, k_new, v_new = pl.pallas_call(
            write_kernel,
            out_shape=(jax.ShapeDtypeStruct((16, D), BF16), jax.ShapeDtypeStruct((W, 128), BF16), jax.ShapeDtypeStruct((W, 128), BF16)),
            in_specs=[vmem_spec] * 3,
            out_specs=(pl.BlockSpec(memory_space=pltpu.HBM),) * 3,
            scratch_shapes=[dma((3,))],
            compiler_params=pltpu.CompilerParams(vmem_limit_bytes=1 << 20),
            name="write",
        )(*[pltpu.with_memory_space_constraint(r, pltpu.VMEM) for r in results])
        return x_out.reshape(x_in.shape), k_new.reshape(k_cache.shape), v_new.reshape(v_cache.shape)

    return jax.shard_map(local_layer, mesh=mesh, in_specs=in_specs, out_specs=out_specs, check_vma=False)
```

```python
import functools

import jax
import numpy as np
import jax.numpy as jnp
from jax import lax
from jax.experimental import pallas as pl
from jax.experimental.pallas import tpu as pltpu
from jax.sharding import PartitionSpec as P

ROPE_BASE = 10000.0
NORM_EPS = 1e-5
BF16 = jnp.bfloat16
F32 = jnp.float32
D = 4096
T = 128
FF = 1792
W = 4096
NP = 8
CW = D // NP
GATHER = [(0, 256), (256, 256)] + [(512 * p, 512) for p in range(1, 7)] + [(3584, 256), (3840, 256)]
SCATTER = [(512 * p, 512) for p in range(8)]
NA = len(GATHER)
NW = 2
NR = len(SCATTER)
LAG = 2
VIA = 6
VMEM_LIMIT = 64000000
KB = 512
NKB = W // KB


def token_of_row(row):
    core = row // 64
    chip = (row // 16) % 4
    return 32 * chip + 16 * core + row % 16


def layer_kernel(start_hbm, x_hbm, freq_hbm, kc_hbm, vc_hbm, g1_hbm, wq_hbm, wk_hbm, wv_hbm, wo_hbm, g2_hbm, wg_hbm, wu_hbm, wd_hbm,
                 xo_ref, kn_ref, vn_ref,
                 start_ref, xv, g1, g2, wg, wu, xg1, xg2, pbuf, ra, sb, rb, tb, hb,
                 lsem, wsem, dsem, gsend_sem, drecv_sem, frecv_sem, asend_sem, arecv_sem, bsend_sem, brecv_sem, trecv_sem):
    me = lax.axis_index("tp")
    core = me % 2
    chip = me // 2
    other = 1 - core
    partner = 2 * chip + other
    flip1 = chip + 1 - 2 * (chip % 2)
    flip2 = chip + 2 - 4 * (chip // 2)
    flip3 = 3 - chip
    chips = (chip, flip1, flip2, flip3)
    my_rows = pl.ds(pl.multiple_of(64 * core + 16 * chip, 16), 16)

    def rows_of(c, q):
        return pl.ds(pl.multiple_of(64 * c + 16 * q, 16), 16)

    def remote(src, dst, ssem, rsem, dev):
        return pltpu.make_async_remote_copy(src_ref=src, dst_ref=dst, send_sem=ssem, recv_sem=rsem, device_id={"tp": dev}, device_id_type=pl.DeviceIdType.MESH)

    def local(src, dst, sem):
        return pltpu.make_async_copy(src, dst, sem)

    def piece(xg, c, r, p):
        return xg.at[rows_of(c, chips[r]), pl.ds(*GATHER[p])]

    def ag_direct(ph, xg, r, p):
        ref = piece(xg, core, 0, p)
        return remote(ref, ref, gsend_sem.at[ph], drecv_sem.at[p], 2 * chips[r] + core)

    def ag_forward(ph, xg, r, p):
        ref = piece(xg, core, r, p)
        return remote(ref, ref, gsend_sem.at[ph], frecv_sem.at[p], partner)

    def ag_start(ph, xg):
        for p in range(NA):
            for r in (3, 1, 2):
                ag_direct(ph, xg, r, p).start()
            ag_forward(ph, xg, 0, p).start()

    def ag_relay(ph, xg, p):
        ref = xg.at[pl.ds(0, 48), pl.ds(*GATHER[p])]
        remote(ref, ref, gsend_sem.at[ph], drecv_sem.at[p], partner).wait_recv()
        for r in (1, 2, 3):
            ag_forward(ph, xg, r, p).start()

    def ag_arrive(ph, xg, p):
        ref = xg.at[pl.ds(0, 64), pl.ds(*GATHER[p])]
        remote(ref, ref, gsend_sem.at[ph], frecv_sem.at[p], partner).wait_recv()

    def ag_finish(ph, xg):
        ref = xg.at[pl.ds(0, 112), :]
        remote(ref, ref, gsend_sem.at[ph], drecv_sem.at[0], partner).wait_send()

    def rs_a(ph, n):
        cols = pl.ds(*SCATTER[n])
        return remote(pbuf.at[ph, pl.ds(pl.multiple_of(64 * other, 64), 64), cols], ra.at[ph, :, cols], asend_sem.at[ph], arecv_sem.at[n], partner)

    def rs_b(ph, n, r):
        cols = pl.ds(*SCATTER[n])
        return remote(sb.at[ph, pl.ds(pl.multiple_of(16 * chips[r], 16), 16), cols], rb.at[ph, r - 1, :, cols], bsend_sem.at[ph], brecv_sem.at[n], 2 * chips[r] + core)

    def rs_put(ph, n, part):
        pbuf[ph, :, pl.ds(*SCATTER[n])] = part.astype(BF16)
        rs_a(ph, n).start()

    def rs_first(n):
        return 1 + n % 2

    def rs_transit(ph, n):
        cols = pl.ds(*SCATTER[n])
        src = sb.at[ph, pl.ds(pl.multiple_of(16 * chips[3], 16), 16), cols]
        return remote(src, tb.at[ph, :, cols], bsend_sem.at[ph], trecv_sem.at[n], 2 * chips[rs_first(n)] + core)

    def rs_pair(ph, n):
        cols = pl.ds(*SCATTER[n])
        rs_a(ph, n).wait_recv()
        own = pbuf[ph, pl.ds(pl.multiple_of(64 * core, 64), 64), cols].astype(F32)
        sb[ph, :, cols] = (own + ra[ph, :, cols].astype(F32)).astype(BF16)
        if n < VIA:
            rs_transit(ph, n).start()
            rs_b(ph, n, rs_first(n)).start()
        else:
            for r in (3, 1, 2):
                rs_b(ph, n, r).start()

    def rs_cross(ph, n):
        cols = pl.ds(*SCATTER[n])
        second = 3 - rs_first(n)
        rows = pl.ds(pl.multiple_of(16 * chips[second], 16), 16)
        rs_transit(ph, n).wait_recv()
        sb[ph, rows, cols] = (sb[ph, rows, cols].astype(F32) + tb[ph, :, cols].astype(F32)).astype(BF16)
        rs_b(ph, n, second).start()

    def rs_all(ph, product, group):
        for n in range(0, NR, group):
            part = product(n, pl.ds(SCATTER[n][0], group * CW))
            for k in range(group):
                rs_put(ph, n + k, part[:, k * CW:k * CW + CW])
            for k in range(n - LAG, n - LAG + group):
                if k >= 0:
                    rs_pair(ph, k)
        for n in range(NR - LAG, NR):
            rs_pair(ph, n)
        for n in range(VIA):
            rs_cross(ph, n)

    def rs_sum(ph, n):
        cols = pl.ds(*SCATTER[n])
        total = sb[ph, pl.ds(pl.multiple_of(16 * chip, 16), 16), cols].astype(F32)
        count = 2 if n < VIA else 3
        ref = rb.at[ph, pl.ds(0, count), :, cols]
        remote(ref, ref, bsend_sem.at[ph], brecv_sem.at[n], partner).wait_recv()
        for r in range(1, count + 1):
            total = total + rb[ph, r - 1, :, cols].astype(F32)
        return total

    def rs_finish(ph):
        remote(ra.at[ph], ra.at[ph], asend_sem.at[ph], arecv_sem.at[0], partner).wait_send()
        remote(rb.at[ph], rb.at[ph], bsend_sem.at[ph], brecv_sem.at[0], partner).wait_send()

    def normed(rows, gain):
        ms = jnp.zeros((16, 128), F32)
        for j in range(32):
            v = rows[:, 128 * j:128 * j + 128].astype(F32)
            ms = ms + v * v
        inv = lax.rsqrt(jnp.sum(ms, axis=-1, keepdims=True) * (1.0 / D) + NORM_EPS)
        return inv

    def store_normed(src, gain, dst):
        inv = normed(src, gain)
        for j in range(32):
            cols = slice(128 * j, 128 * j + 128)
            val = src[:, cols].astype(F32) * inv * gain[j:j + 1, :].astype(F32)
            dst[my_rows, cols] = val.astype(BF16)

    gate_loads = [local(wg_hbm, wg, wsem.at[0]), local(wu_hbm, wu, wsem.at[1])]

    def attention_phase(kc, vc, vt, wo, freqv, qt, kch, vch, bias, o_buf):
        loads = {
            "x": local(x_hbm, xv, lsem.at[0]),
            "g1": local(g1_hbm, g1, lsem.at[1]),
            "freq": local(freq_hbm, freqv, lsem.at[6]),
            "vc": local(vc_hbm, vc, lsem.at[4]),
            "kc": local(kc_hbm, kc, lsem.at[5]),
            "wo": local(wo_hbm, wo, lsem.at[8]),
            "g2": local(g2_hbm, g2, lsem.at[9]),
            "start": local(start_hbm, start_ref, lsem.at[7]),
        }
        loads["x"].start()
        loads["g1"].start()
        barrier = pltpu.get_barrier_semaphore()
        for dev in (partner, 2 * flip1 + core, 2 * flip2 + core, 2 * flip3 + core):
            pl.semaphore_signal(barrier, inc=1, device_id={"tp": dev}, device_id_type=pl.DeviceIdType.MESH)
        tok_lane = token_of_row(lax.broadcasted_iota(jnp.int32, (1, 128), 1))

        def projection_phase(wq4, wqkv):
            wk_load = local(wk_hbm, wqkv.at[:, pl.ds(512, 128)], lsem.at[2])
            wv_load = local(wv_hbm, wqkv.at[:, pl.ds(640, 128)], lsem.at[3])
            wq_loads = [local(wq_hbm.at[pl.ds(p * 4 * (D // NW), 4 * (D // NW)), :], wq4.at[pl.ds(p * 4 * (D // NW), 4 * (D // NW)), :], dsem.at[p]) for p in range(NW)]
            for ld in wq_loads:
                ld.start()
            loads["vc"].start()
            loads["freq"].start()
            loads["start"].start()
            wk_load.start()
            wv_load.start()
            for name in ("kc", "wo", "g2"):
                loads[name].start()

            loads["x"].wait()
            loads["g1"].wait()
            store_normed(xv, g1, xg1)
            pl.semaphore_wait(barrier, 4)
            ag_start(0, xg1)

            ri = lax.broadcasted_iota(jnp.int32, (256, 256), 0)
            ci = lax.broadcasted_iota(jnp.int32, (256, 256), 1)
            perm = (ci == 4 * (ri % 64) + ri // 64).astype(F32).astype(BF16)

            def split_heads(p):
                if p % (NP // NW) == 0:
                    wq_loads[p // (NP // NW)].wait()

                def body(i, carry):
                    base = p * (CW // 64) + 2 * i
                    rows4 = jnp.concatenate([wq4[pl.ds(pl.multiple_of((base + k) * 256, 256), 256), :] for k in range(2)], axis=1)
                    out = jnp.dot(perm, rows4, preferred_element_type=F32).astype(BF16)
                    for k in range(2):
                        for h in range(4):
                            wqkv[pl.ds(pl.multiple_of((base + k) * 64, 64), 64), h * 128:h * 128 + 128] = out[64 * h:64 * h + 64, k * 128:k * 128 + 128]
                    return carry

                for i in range(CW // 128):
                    body(i, 0)

            loads["vc"].wait()

            def flip_values(i, carry):
                ks = pl.ds(pl.multiple_of(i * KB, KB), KB)
                vt[:, ks] = vc[ks, :].astype(F32).T.astype(BF16)
                slot = i * KB + lax.broadcasted_iota(jnp.int32, (KB, 128), 0)
                off = jnp.bitwise_and(slot - start, W - 1)
                keep = jnp.where(off >= W - start, off, -1) > tok_lane
                bias[ks, :] = jnp.where(keep, 0.0, -jnp.inf)
                return carry

            loads["start"].wait()
            start = start_ref[0]
            for p in range(4):
                split_heads(p)
            for p in range(6):
                flip_values(p, 0)
            loads["freq"].wait()
            tok_row = token_of_row(lax.broadcasted_iota(jnp.int32, (T, 128), 0))
            angles = (start + tok_row).astype(F32) * freqv[0:1, :]
            cos_t = jnp.cos(angles)
            lane = lax.broadcasted_iota(jnp.int32, (T, 128), 1)
            even = lane % 2 == 0
            sin_t = jnp.sin(angles)
            sin_t = jnp.where(even, -sin_t, sin_t)
            wk_load.wait()
            wv_load.wait()
            acc = jnp.zeros((T, 768), F32)
            ag_relay(0, xg1, 0)
            ag_relay(0, xg1, 1)
            for p in range(NA):
                if p + 2 < NA:
                    ag_relay(0, xg1, p + 2)
                if p + 4 < NP:
                    split_heads(p + 4)
                if p < 2:
                    flip_values(p + 6, 0)
                if p == NA - 2:
                    for name in ("kc", "wo", "g2"):
                        loads[name].wait()
                    for ld in gate_loads:
                        ld.start()
                ag_arrive(0, xg1, p)
                cols = pl.ds(*GATHER[p])
                acc = acc + jnp.dot(xg1[:, cols], wqkv[cols, :], preferred_element_type=F32)

            def rotate(v):
                swapped = jnp.where(even, pltpu.roll(v, 127, 1), pltpu.roll(v, 1, 1))
                return v * cos_t + swapped * sin_t

            for h in range(4):
                qt[:, h * 128:h * 128 + 128] = rotate(acc[:, h * 128:h * 128 + 128]).T.astype(BF16)
            kch[...] = rotate(acc[:, 512:640]).astype(BF16)
            v_new = acc[:, 640:768].astype(BF16)
            vch[...] = v_new
            vt[:, W:W + T] = v_new.astype(F32).T.astype(BF16)

        pl.run_scoped(
            projection_phase,
            pltpu.VMEM((4 * D, 128), BF16),
            pltpu.VMEM((D, 768), BF16),
        )
        factor = (128.0 ** -0.5) * 1.4426950408889634

        def softmax_phase(e_buf):
            queries = qt[...]
            tops, masses = [], []
            for b in range(NKB + 1):
                keys = kc[b * KB:b * KB + KB, :] if b < NKB else kch[...]
                scores = jnp.dot(keys, queries, preferred_element_type=F32)
                for i in range(KB // 128 if b < NKB else 1):
                    ks = slice(b * KB + i * 128, b * KB + i * 128 + 128)
                    if b < NKB:
                        shift = bias[ks, :]
                    else:
                        shift = jnp.where(token_of_row(lax.broadcasted_iota(jnp.int32, (T, 128), 0)) <= tok_lane, 0.0, -jnp.inf)
                    top, mass = [], []
                    for g in range(4):
                        gs = slice(g * 128, g * 128 + 128)
                        part = (scores[i * 128:i * 128 + 128, gs] + shift).reshape(16, 8, 128)
                        t = jnp.maximum(jnp.max(part, axis=0), jnp.finfo(F32).min)
                        e = jnp.exp2((part - t[None]) * factor)
                        e_buf[ks, gs] = e.reshape(128, 128)
                        mass.append(jnp.sum(e, axis=0))
                        top.append(t)
                    tops.append(top)
                    masses.append(mass)
            blocks = len(tops)
            weights = []
            for g in range(4):
                best = jnp.max(functools.reduce(jnp.maximum, [tops[b][g] for b in range(blocks)]), axis=0, keepdims=True)
                scales = [jnp.exp2((tops[b][g] - best) * factor) for b in range(blocks)]
                total = functools.reduce(jnp.add, [masses[b][g] * scales[b] for b in range(blocks)])
                inv = 1.0 / jnp.sum(total, axis=0, keepdims=True)
                weights.append([sc * inv for sc in scales])
            out = None
            for b in range(NKB + 1):
                n = KB if b < NKB else T
                ks = slice(b * KB, b * KB + n)
                rows = []
                for i in range(n // 128):
                    r0 = b * KB + i * 128
                    cols = [(e_buf[r0:r0 + 128, g * 128:g * 128 + 128].reshape(16, 8, 128) * weights[g][b * (KB // 128) + i][None]).reshape(128, 128) for g in range(4)]
                    rows.append(jnp.concatenate(cols, axis=1))
                probs = jnp.concatenate(rows, axis=0).astype(BF16)
                part = jnp.dot(vt[:, ks], probs, preferred_element_type=F32)
                out = part if out is None else out + part
            for g in range(4):
                o_buf[:, g * 128:g * 128 + 128] = out[:, g * 128:g * 128 + 128].T.astype(BF16)

        pl.run_scoped(softmax_phase, pltpu.VMEM((W + T, 512), F32))
        rs_all(0, lambda n, cols: jnp.dot(o_buf[...], wo[:, cols], preferred_element_type=F32), 2)

        chunk = jnp.concatenate([kch[...], vch[...]], axis=1)

        def merge(i, carry):
            ks = pl.ds(pl.multiple_of(i * KB, KB), KB)
            slot = i * KB + lax.broadcasted_iota(jnp.int32, (KB, 128), 0)
            off = jnp.bitwise_and(slot - start, W - 1)
            pick = (off == tok_lane).astype(F32).astype(BF16)
            placed = jnp.dot(pick, chunk, preferred_element_type=F32)
            fresh = off < T
            kn_ref[ks, :] = jnp.where(fresh, placed[:, 0:128], kc[ks, :].astype(F32)).astype(BF16)
            vn_ref[ks, :] = jnp.where(fresh, placed[:, 128:256], vc[ks, :].astype(F32)).astype(BF16)
            return carry

        start = start_ref[0]
        lax.fori_loop(0, NKB, merge, 0)

    pl.run_scoped(
        attention_phase,
        pltpu.VMEM((W, 128), BF16),
        pltpu.VMEM((W, 128), BF16),
        pltpu.VMEM((128, W + T), BF16),
        pltpu.VMEM((512, D), BF16),
        pltpu.VMEM((8, 128), F32),
        pltpu.VMEM((128, 512), BF16),
        pltpu.VMEM((T, 128), BF16),
        pltpu.VMEM((T, 128), BF16),
        pltpu.VMEM((W, 128), F32),
        pltpu.VMEM((T, 512), BF16),
    )

    def mlp_phase(wd, acc_g, acc_u, u_buf):
        down_load = local(wd_hbm, wd, wsem.at[2])
        down_load.start()
        for n in range(NR):
            cols = pl.ds(*SCATTER[n])
            hb[:, cols] = (xv[:, cols].astype(F32) + rs_sum(0, n)).astype(BF16)
        store_normed(hb, g2, xg2)
        ag_start(1, xg2)
        ag_finish(0, xg1)
        rs_finish(0)
        ag_relay(1, xg2, 0)
        ag_relay(1, xg2, 1)
        for p in range(NA):
            if p + 2 < NA:
                ag_relay(1, xg2, p + 2)
            if p == 0:
                for ld in gate_loads:
                    ld.wait()
            ag_arrive(1, xg2, p)
            rows = pl.ds(*GATHER[p])
            m = xg2[:, rows]
            gate = jnp.dot(m, wg[rows, :], preferred_element_type=F32)
            up = jnp.dot(m, wu[rows, :], preferred_element_type=F32)
            if p == 0:
                acc_g[...] = gate
                acc_u[...] = up
            elif p + 1 < NA:
                acc_g[...] += gate
                acc_u[...] += up
            else:
                gate = acc_g[...] + gate
                u_buf[...] = (gate / (1.0 + jnp.exp(-gate)) * (acc_u[...] + up)).astype(BF16)
        def down(n, cols):
            if n == 0:
                down_load.wait()
            return jnp.dot(u_buf[...], wd[:, cols], preferred_element_type=F32)

        rs_all(1, down, 1)
        ag_finish(1, xg2)
        for n in range(NR):
            cols = pl.ds(*SCATTER[n])
            xo_ref[:, cols] = (hb[:, cols].astype(F32) + rs_sum(1, n)).astype(BF16)
        rs_finish(1)

    pl.run_scoped(
        mlp_phase,
        pltpu.VMEM((FF, D), BF16),
        pltpu.VMEM((T, FF), F32),
        pltpu.VMEM((T, FF), F32),
        pltpu.VMEM((T, FF), BF16),
    )


def write_kernel(x_ref, k_ref, v_ref, xo_hbm, ko_hbm, vo_hbm, sem):
    parts = [(x_ref, xo_hbm)]
    for i in range(4):
        rows = pl.ds(i * (W // 4), W // 4)
        parts += [(k_ref.at[rows, :], ko_hbm.at[rows, :]), (v_ref.at[rows, :], vo_hbm.at[rows, :])]
    copies = [pltpu.make_async_copy(src, dst, sem.at[i]) for i, (src, dst) in enumerate(parts)]
    for copy in copies:
        copy.start()
    for copy in copies:
        copy.wait()


def solution(mesh):
    row_spec = P('dp', 'tp', None)
    cache_spec = P('dp', None, 'tp', None)
    head_cols = P(None, 'tp', None)
    in_specs = (row_spec, P('dp'), cache_spec, cache_spec, P(), head_cols, head_cols, head_cols, P('tp', None, None), P(), P(None, 'tp'), P(None, 'tp'), P('tp', None))
    out_specs = (row_spec, cache_spec, cache_spec)

    def local_layer(x_in, start_pos, k_cache, v_cache, attn_gain, w_query, w_key, w_value, w_out, mlp_gain, w_gate, w_up, w_down):
        freq = np.repeat(ROPE_BASE ** (-np.arange(0, 128, 2) / 128.0), 2).astype(np.float32)
        freq = jnp.asarray(np.tile(freq[None, :], (8, 1)))
        any_spec = pl.BlockSpec(memory_space=pl.ANY)
        vmem_spec = pl.BlockSpec(memory_space=pltpu.VMEM)
        dma = pltpu.SemaphoreType.DMA
        kc2 = k_cache.reshape(W, 128)
        vc2 = v_cache.reshape(W, 128)
        results = pl.pallas_call(
            layer_kernel,
            out_shape=(pltpu.VMEM((16, D), BF16), pltpu.VMEM((W, 128), BF16), pltpu.VMEM((W, 128), BF16)),
            in_specs=[any_spec] * 14,
            out_specs=(vmem_spec, vmem_spec, vmem_spec),
            scratch_shapes=[
                pltpu.SMEM((1,), jnp.int32),
                pltpu.VMEM((16, D), BF16),
                pltpu.VMEM((32, 128), BF16),
                pltpu.VMEM((32, 128), BF16),
                pltpu.VMEM((D, FF), BF16),
                pltpu.VMEM((D, FF), BF16),
                pltpu.VMEM((T, D), BF16),
                pltpu.VMEM((T, D), BF16),
                pltpu.VMEM((2, T, D), BF16),
                pltpu.VMEM((2, 64, D), BF16),
                pltpu.VMEM((2, 64, D), BF16),
                pltpu.VMEM((2, 3, 16, D), BF16),
                pltpu.VMEM((2, 16, VIA * CW), BF16),
                pltpu.VMEM((16, D), BF16),
                dma((10,)),
                dma((3,)),
                dma((NW,)),
                dma((2,)),
                dma((NA,)),
                dma((NA,)),
                dma((2,)),
                dma((NR,)),
                dma((2,)),
                dma((NR,)),
                dma((VIA,)),
            ],
            compiler_params=pltpu.CompilerParams(collective_id=0, has_side_effects=True, vmem_limit_bytes=VMEM_LIMIT),
            name="layer",
        )(
            start_pos, x_in.reshape(16, D), freq, kc2, vc2, attn_gain.reshape(32, 128), w_query.reshape(4 * D, 128),
            w_key.reshape(D, 128), w_value.reshape(D, 128), w_out.reshape(512, D), mlp_gain.reshape(32, 128), w_gate, w_up, w_down,
        )
        x_out, k_new, v_new = pl.pallas_call(
            write_kernel,
            out_shape=(jax.ShapeDtypeStruct((16, D), BF16), jax.ShapeDtypeStruct((W, 128), BF16), jax.ShapeDtypeStruct((W, 128), BF16)),
            in_specs=[vmem_spec] * 3,
            out_specs=(pl.BlockSpec(memory_space=pltpu.HBM),) * 3,
            scratch_shapes=[dma((9,))],
            compiler_params=pltpu.CompilerParams(vmem_limit_bytes=1 << 20),
            name="write",
        )(*[pltpu.with_memory_space_constraint(r, pltpu.VMEM) for r in results])
        return x_out.reshape(x_in.shape), k_new.reshape(k_cache.shape), v_new.reshape(v_cache.shape)

    return jax.shard_map(local_layer, mesh=mesh, in_specs=in_specs, out_specs=out_specs, check_vma=False)
```

```python
import functools

import jax
import numpy as np
import jax.numpy as jnp
from jax import lax
from jax.experimental import pallas as pl
from jax.experimental.pallas import tpu as pltpu
from jax.sharding import PartitionSpec as P

ROPE_BASE = 10000.0
NORM_EPS = 1e-5
BF16 = jnp.bfloat16
F32 = jnp.float32
D = 4096
T = 128
FF = 1792
W = 4096
NP = 8
CW = D // NP
GATHER = [(0, 256), (256, 256)] + [(512 * p, 512) for p in range(1, 7)] + [(3584, 256), (3840, 256)]
SCATTER = [(512 * p, 512) for p in range(8)]
NA = len(GATHER)
NW = 2
NR = len(SCATTER)
LAG = 2
VIA = 6
VMEM_LIMIT = 64000000
KB = 512
NKB = W // KB


def token_of_row(row):
    core = row // 64
    chip = (row // 16) % 4
    return 32 * chip + 16 * core + row % 16


def layer_kernel(start_hbm, x_hbm, freq_hbm, kc_hbm, vc_hbm, g1_hbm, wq_hbm, wk_hbm, wv_hbm, wo_hbm, g2_hbm, wg_hbm, wu_hbm, wd_hbm,
                 xo_ref, kn_ref, vn_ref,
                 start_ref, xv, g1, g2, wg, wu, xg1, xg2, pbuf, ra, sb, rb, tb, hb,
                 lsem, wsem, dsem, gsend_sem, drecv_sem, frecv_sem, asend_sem, arecv_sem, bsend_sem, brecv_sem, trecv_sem):
    me = lax.axis_index("tp")
    core = me % 2
    chip = me // 2
    other = 1 - core
    partner = 2 * chip + other
    flip1 = chip + 1 - 2 * (chip % 2)
    flip2 = chip + 2 - 4 * (chip // 2)
    flip3 = 3 - chip
    chips = (chip, flip1, flip2, flip3)
    my_rows = pl.ds(pl.multiple_of(64 * core + 16 * chip, 16), 16)

    def rows_of(c, q):
        return pl.ds(pl.multiple_of(64 * c + 16 * q, 16), 16)

    def remote(src, dst, ssem, rsem, dev):
        return pltpu.make_async_remote_copy(src_ref=src, dst_ref=dst, send_sem=ssem, recv_sem=rsem, device_id={"tp": dev}, device_id_type=pl.DeviceIdType.MESH)

    def local(src, dst, sem):
        return pltpu.make_async_copy(src, dst, sem)

    def piece(xg, c, r, p):
        return xg.at[rows_of(c, chips[r]), pl.ds(*GATHER[p])]

    def ag_direct(ph, xg, r, p):
        ref = piece(xg, core, 0, p)
        return remote(ref, ref, gsend_sem.at[ph], drecv_sem.at[p], 2 * chips[r] + core)

    def ag_forward(ph, xg, r, p):
        ref = piece(xg, core, r, p)
        return remote(ref, ref, gsend_sem.at[ph], frecv_sem.at[p], partner)

    def ag_start(ph, xg):
        for p in range(NA):
            for r in (3, 1, 2):
                ag_direct(ph, xg, r, p).start()
            ag_forward(ph, xg, 0, p).start()

    def ag_relay(ph, xg, p):
        ref = xg.at[pl.ds(0, 48), pl.ds(*GATHER[p])]
        remote(ref, ref, gsend_sem.at[ph], drecv_sem.at[p], partner).wait_recv()
        for r in (1, 2, 3):
            ag_forward(ph, xg, r, p).start()

    def ag_arrive(ph, xg, p):
        ref = xg.at[pl.ds(0, 64), pl.ds(*GATHER[p])]
        remote(ref, ref, gsend_sem.at[ph], frecv_sem.at[p], partner).wait_recv()

    def ag_finish(ph, xg):
        ref = xg.at[pl.ds(0, 112), :]
        remote(ref, ref, gsend_sem.at[ph], drecv_sem.at[0], partner).wait_send()

    def rs_a(ph, n):
        cols = pl.ds(*SCATTER[n])
        return remote(pbuf.at[ph, pl.ds(pl.multiple_of(64 * other, 64), 64), cols], ra.at[ph, :, cols], asend_sem.at[ph], arecv_sem.at[n], partner)

    def rs_b(ph, n, r):
        cols = pl.ds(*SCATTER[n])
        return remote(sb.at[ph, pl.ds(pl.multiple_of(16 * chips[r], 16), 16), cols], rb.at[ph, r - 1, :, cols], bsend_sem.at[ph], brecv_sem.at[n], 2 * chips[r] + core)

    def rs_put(ph, n, part):
        pbuf[ph, :, pl.ds(*SCATTER[n])] = part.astype(BF16)
        rs_a(ph, n).start()

    def rs_first(n):
        return 1 + n % 2

    def rs_transit(ph, n):
        cols = pl.ds(*SCATTER[n])
        src = sb.at[ph, pl.ds(pl.multiple_of(16 * chips[3], 16), 16), cols]
        return remote(src, tb.at[ph, :, cols], bsend_sem.at[ph], trecv_sem.at[n], 2 * chips[rs_first(n)] + core)

    def rs_pair(ph, n):
        cols = pl.ds(*SCATTER[n])
        rs_a(ph, n).wait_recv()
        own = pbuf[ph, pl.ds(pl.multiple_of(64 * core, 64), 64), cols].astype(F32)
        sb[ph, :, cols] = (own + ra[ph, :, cols].astype(F32)).astype(BF16)
        if n < VIA:
            rs_transit(ph, n).start()
            rs_b(ph, n, rs_first(n)).start()
        else:
            for r in (3, 1, 2):
                rs_b(ph, n, r).start()

    def rs_cross(ph, n):
        cols = pl.ds(*SCATTER[n])
        second = 3 - rs_first(n)
        rows = pl.ds(pl.multiple_of(16 * chips[second], 16), 16)
        rs_transit(ph, n).wait_recv()
        sb[ph, rows, cols] = (sb[ph, rows, cols].astype(F32) + tb[ph, :, cols].astype(F32)).astype(BF16)
        rs_b(ph, n, second).start()

    def rs_all(ph, product, group):
        for n in range(0, NR, group):
            part = product(n, pl.ds(SCATTER[n][0], group * CW))
            for k in range(group):
                rs_put(ph, n + k, part[:, k * CW:k * CW + CW])
            for k in range(n - LAG, n - LAG + group):
                if k >= 0:
                    rs_pair(ph, k)
        for n in range(NR - LAG, NR):
            rs_pair(ph, n)
        for n in range(VIA):
            rs_cross(ph, n)

    def rs_sum(ph, n):
        cols = pl.ds(*SCATTER[n])
        total = sb[ph, pl.ds(pl.multiple_of(16 * chip, 16), 16), cols].astype(F32)
        count = 2 if n < VIA else 3
        ref = rb.at[ph, pl.ds(0, count), :, cols]
        remote(ref, ref, bsend_sem.at[ph], brecv_sem.at[n], partner).wait_recv()
        for r in range(1, count + 1):
            total = total + rb[ph, r - 1, :, cols].astype(F32)
        return total

    def rs_finish(ph):
        remote(ra.at[ph], ra.at[ph], asend_sem.at[ph], arecv_sem.at[0], partner).wait_send()
        remote(rb.at[ph], rb.at[ph], bsend_sem.at[ph], brecv_sem.at[0], partner).wait_send()

    def normed(rows, gain):
        ms = jnp.zeros((16, 128), F32)
        for j in range(32):
            v = rows[:, 128 * j:128 * j + 128].astype(F32)
            ms = ms + v * v
        inv = lax.rsqrt(jnp.sum(ms, axis=-1, keepdims=True) * (1.0 / D) + NORM_EPS)
        return inv

    def store_normed(src, gain, dst):
        inv = normed(src, gain)
        for j in range(32):
            cols = slice(128 * j, 128 * j + 128)
            val = src[:, cols].astype(F32) * inv * gain[j:j + 1, :].astype(F32)
            dst[my_rows, cols] = val.astype(BF16)

    gate_loads = [local(wg_hbm, wg, wsem.at[0]), local(wu_hbm, wu, wsem.at[1])]

    def attention_phase(kc, vc, vt, wo, freqv, qt, kch, vch, bias, o_buf):
        loads = {
            "x": local(x_hbm, xv, lsem.at[0]),
            "g1": local(g1_hbm, g1, lsem.at[1]),
            "freq": local(freq_hbm, freqv, lsem.at[6]),
            "vc": local(vc_hbm, vc, lsem.at[4]),
            "kc": local(kc_hbm, kc, lsem.at[5]),
            "wo": local(wo_hbm, wo, lsem.at[8]),
            "g2": local(g2_hbm, g2, lsem.at[9]),
            "start": local(start_hbm, start_ref, lsem.at[7]),
        }
        loads["x"].start()
        loads["g1"].start()
        barrier = pltpu.get_barrier_semaphore()
        for dev in (partner, 2 * flip1 + core, 2 * flip2 + core, 2 * flip3 + core):
            pl.semaphore_signal(barrier, inc=1, device_id={"tp": dev}, device_id_type=pl.DeviceIdType.MESH)
        tok_lane = token_of_row(lax.broadcasted_iota(jnp.int32, (1, 128), 1))

        def projection_phase(wq4, wqkv):
            wk_load = local(wk_hbm, wqkv.at[:, pl.ds(512, 128)], lsem.at[2])
            wv_load = local(wv_hbm, wqkv.at[:, pl.ds(640, 128)], lsem.at[3])
            wq_loads = [local(wq_hbm.at[pl.ds(p * 4 * (D // NW), 4 * (D // NW)), :], wq4.at[pl.ds(p * 4 * (D // NW), 4 * (D // NW)), :], dsem.at[p]) for p in range(NW)]
            for ld in wq_loads:
                ld.start()
            loads["vc"].start()
            loads["freq"].start()
            loads["start"].start()
            wk_load.start()
            wv_load.start()
            for name in ("kc", "wo", "g2"):
                loads[name].start()

            loads["x"].wait()
            loads["g1"].wait()
            store_normed(xv, g1, xg1)
            pl.semaphore_wait(barrier, 4)
            ag_start(0, xg1)

            ri = lax.broadcasted_iota(jnp.int32, (256, 256), 0)
            ci = lax.broadcasted_iota(jnp.int32, (256, 256), 1)
            perm = (ci == 4 * (ri % 64) + ri // 64).astype(F32).astype(BF16)

            def split_heads(p):
                if p % (NP // NW) == 0:
                    wq_loads[p // (NP // NW)].wait()

                def body(i, carry):
                    base = p * (CW // 64) + 2 * i
                    rows4 = jnp.concatenate([wq4[pl.ds(pl.multiple_of((base + k) * 256, 256), 256), :] for k in range(2)], axis=1)
                    out = jnp.dot(perm, rows4, preferred_element_type=F32).astype(BF16)
                    for k in range(2):
                        for h in range(4):
                            wqkv[pl.ds(pl.multiple_of((base + k) * 64, 64), 64), h * 128:h * 128 + 128] = out[64 * h:64 * h + 64, k * 128:k * 128 + 128]
                    return carry

                for i in range(CW // 128):
                    body(i, 0)

            loads["vc"].wait()

            def flip_values(i, carry):
                ks = pl.ds(pl.multiple_of(i * KB, KB), KB)
                vt[:, ks] = vc[ks, :].astype(F32).T.astype(BF16)
                slot = i * KB + lax.broadcasted_iota(jnp.int32, (KB, 128), 0)
                off = jnp.bitwise_and(slot - start, W - 1)
                keep = jnp.where(off >= W - start, off, -1) > tok_lane
                bias[ks, :] = jnp.where(keep, 0.0, -jnp.inf)
                return carry

            loads["start"].wait()
            start = start_ref[0]
            for p in range(4):
                split_heads(p)
            for p in range(6):
                flip_values(p, 0)
            loads["freq"].wait()
            tok_row = token_of_row(lax.broadcasted_iota(jnp.int32, (T, 128), 0))
            angles = (start + tok_row).astype(F32) * freqv[0:1, :]
            cos_t = jnp.cos(angles)
            lane = lax.broadcasted_iota(jnp.int32, (T, 128), 1)
            even = lane % 2 == 0
            sin_t = jnp.sin(angles)
            sin_t = jnp.where(even, -sin_t, sin_t)
            wk_load.wait()
            wv_load.wait()
            acc = jnp.zeros((T, 768), F32)
            ag_relay(0, xg1, 0)
            ag_relay(0, xg1, 1)
            for p in range(NA):
                if p + 2 < NA:
                    ag_relay(0, xg1, p + 2)
                if p + 4 < NP:
                    split_heads(p + 4)
                if p < 2:
                    flip_values(p + 6, 0)
                if p == NA - 2:
                    for name in ("kc", "wo", "g2"):
                        loads[name].wait()
                    for ld in gate_loads:
                        ld.start()
                ag_arrive(0, xg1, p)
                cols = pl.ds(*GATHER[p])
                acc = acc + jnp.dot(xg1[:, cols], wqkv[cols, :], preferred_element_type=F32)

            def rotate(v):
                swapped = jnp.where(even, pltpu.roll(v, 127, 1), pltpu.roll(v, 1, 1))
                return v * cos_t + swapped * sin_t

            for h in range(4):
                qt[:, h * 128:h * 128 + 128] = rotate(acc[:, h * 128:h * 128 + 128]).T.astype(BF16)
            kch[...] = rotate(acc[:, 512:640]).astype(BF16)
            v_new = acc[:, 640:768].astype(BF16)
            vch[...] = v_new
            vt[:, W:W + T] = v_new.astype(F32).T.astype(BF16)

        pl.run_scoped(
            projection_phase,
            pltpu.VMEM((4 * D, 128), BF16),
            pltpu.VMEM((D, 768), BF16),
        )
        factor = (128.0 ** -0.5) * 1.4426950408889634

        def softmax_phase(e_buf):
            queries = qt[...]
            tops, masses = [], []
            for b in range(NKB + 1):
                keys = kc[b * KB:b * KB + KB, :] if b < NKB else kch[...]
                scores = jnp.dot(keys, queries, preferred_element_type=F32)
                for i in range(KB // 128 if b < NKB else 1):
                    ks = slice(b * KB + i * 128, b * KB + i * 128 + 128)
                    if b < NKB:
                        shift = bias[ks, :]
                    else:
                        shift = jnp.where(token_of_row(lax.broadcasted_iota(jnp.int32, (T, 128), 0)) <= tok_lane, 0.0, -jnp.inf)
                    top, mass = [], []
                    for g in range(4):
                        gs = slice(g * 128, g * 128 + 128)
                        part = (scores[i * 128:i * 128 + 128, gs] + shift).reshape(16, 8, 128)
                        t = jnp.maximum(jnp.max(part, axis=0), jnp.finfo(F32).min)
                        e = jnp.exp2((part - t[None]) * factor)
                        e_buf[ks, gs] = e.reshape(128, 128)
                        mass.append(jnp.sum(e, axis=0))
                        top.append(t)
                    tops.append(top)
                    masses.append(mass)
            blocks = len(tops)
            weights = []
            for g in range(4):
                best = jnp.max(functools.reduce(jnp.maximum, [tops[b][g] for b in range(blocks)]), axis=0, keepdims=True)
                scales = [jnp.exp2((tops[b][g] - best) * factor) for b in range(blocks)]
                total = functools.reduce(jnp.add, [masses[b][g] * scales[b] for b in range(blocks)])
                inv = 1.0 / jnp.sum(total, axis=0, keepdims=True)
                weights.append([sc * inv for sc in scales])
            out = None
            for b in range(NKB + 1):
                n = KB if b < NKB else T
                ks = slice(b * KB, b * KB + n)
                rows = []
                for i in range(n // 128):
                    r0 = b * KB + i * 128
                    cols = [(e_buf[r0:r0 + 128, g * 128:g * 128 + 128].reshape(16, 8, 128) * weights[g][b * (KB // 128) + i][None]).reshape(128, 128) for g in range(4)]
                    rows.append(jnp.concatenate(cols, axis=1))
                probs = jnp.concatenate(rows, axis=0).astype(BF16)
                part = jnp.dot(vt[:, ks], probs, preferred_element_type=F32)
                out = part if out is None else out + part
            for g in range(4):
                o_buf[:, g * 128:g * 128 + 128] = out[:, g * 128:g * 128 + 128].T.astype(BF16)

        pl.run_scoped(softmax_phase, pltpu.VMEM((W + T, 512), F32))
        rs_all(0, lambda n, cols: jnp.dot(o_buf[...], wo[:, cols], preferred_element_type=F32), 2)

        chunk = jnp.concatenate([kch[...], vch[...]], axis=1)

        def merge(i, carry):
            ks = pl.ds(pl.multiple_of(i * KB, KB), KB)
            slot = i * KB + lax.broadcasted_iota(jnp.int32, (KB, 128), 0)
            off = jnp.bitwise_and(slot - start, W - 1)
            pick = (off == tok_lane).astype(F32).astype(BF16)
            placed = jnp.dot(pick, chunk, preferred_element_type=F32)
            fresh = off < T
            kn_ref[ks, :] = jnp.where(fresh, placed[:, 0:128], kc[ks, :].astype(F32)).astype(BF16)
            vn_ref[ks, :] = jnp.where(fresh, placed[:, 128:256], vc[ks, :].astype(F32)).astype(BF16)
            return carry

        start = start_ref[0]
        lax.fori_loop(0, NKB, merge, 0)

    pl.run_scoped(
        attention_phase,
        pltpu.VMEM((W, 128), BF16),
        pltpu.VMEM((W, 128), BF16),
        pltpu.VMEM((128, W + T), BF16),
        pltpu.VMEM((512, D), BF16),
        pltpu.VMEM((8, 128), F32),
        pltpu.VMEM((128, 512), BF16),
        pltpu.VMEM((T, 128), BF16),
        pltpu.VMEM((T, 128), BF16),
        pltpu.VMEM((W, 128), F32),
        pltpu.VMEM((T, 512), BF16),
    )

    def mlp_phase(wd, acc_g, acc_u, u_buf):
        down_load = local(wd_hbm, wd, wsem.at[2])
        down_load.start()
        for n in range(NR):
            cols = pl.ds(*SCATTER[n])
            hb[:, cols] = (xv[:, cols].astype(F32) + rs_sum(0, n)).astype(BF16)
        store_normed(hb, g2, xg2)
        ag_start(1, xg2)
        ag_finish(0, xg1)
        rs_finish(0)
        ag_relay(1, xg2, 0)
        ag_relay(1, xg2, 1)
        for p in range(NA):
            if p + 2 < NA:
                ag_relay(1, xg2, p + 2)
            if p == 0:
                for ld in gate_loads:
                    ld.wait()
            if p == NA - 2:
                down_load.wait()
            ag_arrive(1, xg2, p)
            rows = pl.ds(*GATHER[p])
            m = xg2[:, rows]
            gate = jnp.dot(m, wg[rows, :], preferred_element_type=F32)
            up = jnp.dot(m, wu[rows, :], preferred_element_type=F32)
            if p == 0:
                acc_g[...] = gate
                acc_u[...] = up
            elif p + 1 < NA:
                acc_g[...] += gate
                acc_u[...] += up
            else:
                gate = acc_g[...] + gate
                u_buf[...] = (gate / (1.0 + jnp.exp(-gate)) * (acc_u[...] + up)).astype(BF16)
        def down(n, cols):
            return jnp.dot(u_buf[...], wd[:, cols], preferred_element_type=F32)

        rs_all(1, down, 1)
        ag_finish(1, xg2)
        for n in range(NR):
            cols = pl.ds(*SCATTER[n])
            xo_ref[:, cols] = (hb[:, cols].astype(F32) + rs_sum(1, n)).astype(BF16)
        rs_finish(1)

    pl.run_scoped(
        mlp_phase,
        pltpu.VMEM((FF, D), BF16),
        pltpu.VMEM((T, FF), F32),
        pltpu.VMEM((T, FF), F32),
        pltpu.VMEM((T, FF), BF16),
    )


def write_kernel(x_ref, k_ref, v_ref, xo_hbm, ko_hbm, vo_hbm, sem):
    copies = [pltpu.make_async_copy(src, dst, sem.at[i]) for i, (src, dst) in enumerate(((k_ref, ko_hbm), (v_ref, vo_hbm), (x_ref, xo_hbm)))]
    for copy in copies:
        copy.start()
    for copy in copies:
        copy.wait()


def solution(mesh):
    row_spec = P('dp', 'tp', None)
    cache_spec = P('dp', None, 'tp', None)
    head_cols = P(None, 'tp', None)
    in_specs = (row_spec, P('dp'), cache_spec, cache_spec, P(), head_cols, head_cols, head_cols, P('tp', None, None), P(), P(None, 'tp'), P(None, 'tp'), P('tp', None))
    out_specs = (row_spec, cache_spec, cache_spec)

    def local_layer(x_in, start_pos, k_cache, v_cache, attn_gain, w_query, w_key, w_value, w_out, mlp_gain, w_gate, w_up, w_down):
        freq = np.repeat(ROPE_BASE ** (-np.arange(0, 128, 2) / 128.0), 2).astype(np.float32)
        freq = jnp.asarray(np.tile(freq[None, :], (8, 1)))
        any_spec = pl.BlockSpec(memory_space=pl.ANY)
        vmem_spec = pl.BlockSpec(memory_space=pltpu.VMEM)
        dma = pltpu.SemaphoreType.DMA
        kc2 = k_cache.reshape(W, 128)
        vc2 = v_cache.reshape(W, 128)
        results = pl.pallas_call(
            layer_kernel,
            out_shape=(pltpu.VMEM((16, D), BF16), pltpu.VMEM((W, 128), BF16), pltpu.VMEM((W, 128), BF16)),
            in_specs=[any_spec] * 14,
            out_specs=(vmem_spec, vmem_spec, vmem_spec),
            scratch_shapes=[
                pltpu.SMEM((1,), jnp.int32),
                pltpu.VMEM((16, D), BF16),
                pltpu.VMEM((32, 128), BF16),
                pltpu.VMEM((32, 128), BF16),
                pltpu.VMEM((D, FF), BF16),
                pltpu.VMEM((D, FF), BF16),
                pltpu.VMEM((T, D), BF16),
                pltpu.VMEM((T, D), BF16),
                pltpu.VMEM((2, T, D), BF16),
                pltpu.VMEM((2, 64, D), BF16),
                pltpu.VMEM((2, 64, D), BF16),
                pltpu.VMEM((2, 3, 16, D), BF16),
                pltpu.VMEM((2, 16, VIA * CW), BF16),
                pltpu.VMEM((16, D), BF16),
                dma((10,)),
                dma((3,)),
                dma((NW,)),
                dma((2,)),
                dma((NA,)),
                dma((NA,)),
                dma((2,)),
                dma((NR,)),
                dma((2,)),
                dma((NR,)),
                dma((VIA,)),
            ],
            compiler_params=pltpu.CompilerParams(collective_id=0, has_side_effects=True, vmem_limit_bytes=VMEM_LIMIT),
            name="layer",
        )(
            start_pos, x_in.reshape(16, D), freq, kc2, vc2, attn_gain.reshape(32, 128), w_query.reshape(4 * D, 128),
            w_key.reshape(D, 128), w_value.reshape(D, 128), w_out.reshape(512, D), mlp_gain.reshape(32, 128), w_gate, w_up, w_down,
        )
        x_out, k_new, v_new = pl.pallas_call(
            write_kernel,
            out_shape=(jax.ShapeDtypeStruct((16, D), BF16), jax.ShapeDtypeStruct((W, 128), BF16), jax.ShapeDtypeStruct((W, 128), BF16)),
            in_specs=[vmem_spec] * 3,
            out_specs=(pl.BlockSpec(memory_space=pltpu.HBM),) * 3,
            scratch_shapes=[dma((3,))],
            compiler_params=pltpu.CompilerParams(vmem_limit_bytes=1 << 20),
            name="write",
        )(*[pltpu.with_memory_space_constraint(r, pltpu.VMEM) for r in results])
        return x_out.reshape(x_in.shape), k_new.reshape(k_cache.shape), v_new.reshape(v_cache.shape)

    return jax.shard_map(local_layer, mesh=mesh, in_specs=in_specs, out_specs=out_specs, check_vma=False)
```
